16 devices in a mesh: dp: 2 (over y, z), sp: 8 (over x, core).
Axes of the slice: x: 4, y: 2, z: 1, core: 2. Of those that a mesh axis runs over, the one named last changes fastest.
The devices are a block of a 4x4x8 slice.
Arguments:
- patches: bfloat16 [16384, 1280], P(('dp', 'sp')), parts along dimension 0
- embeds: bfloat16 [8192, 2560], P(('dp', 'sp')), parts along dimension 0
- dest_slot: int32 [4096], P(('dp', 'sp')), parts along dimension 0
- rope_pos: int32 [3, 8192], P(None, ('dp', 'sp')), parts along dimension 1
- cu_doc: int32 [6], P('dp'), parts along dimension 0
- ln_w: bfloat16 [1280], replicated
- ln_b: bfloat16 [1280], replicated
- w_one: bfloat16 [5120, 5120], replicated
- b_one: bfloat16 [5120], replicated
- w_two: bfloat16 [5120, 2560], replicated
- b_two: bfloat16 [2560], replicated
- norm_attn: bfloat16 [2560], replicated
- w_q: bfloat16 [2560, 2560], replicated
- b_q: bfloat16 [2560], replicated
- w_k: bfloat16 [2560, 2560], replicated
- b_k: bfloat16 [2560], replicated
- w_v: bfloat16 [2560, 2560], replicated
- b_v: bfloat16 [2560], replicated
- w_o: bfloat16 [2560, 2560], replicated
- norm_mlp: bfloat16 [2560], replicated
- w_gate: bfloat16 [2560, 6912], replicated
- w_up: bfloat16 [2560, 6912], replicated
- w_down: bfloat16 [6912, 2560], replicated
Outputs:
- output: bfloat16 [8192, 2560], P(('dp', 'sp')), parts along dimension 0
There are 2 independent parts. The reference program is written for one: setup_inputs(seed, part) draws one part's arguments, and reference() takes and returns one part's arrays. A program takes and returns all parts, laid end to end along the dimension named above; an argument that names none is the same for every part.
All inputs are finite; a program needn't handle non-finite values.
Results may differ from the reference program's by a relative error of at most 0.0106714.
Values are sent between devices in bfloat16 or wider.
A program may use at most 768 MiB of HBM per device.

```python
import jax
import jax.numpy as jnp
from jax import lax

GROUP_SIZE = 8
TOK_DEV = 512
MERGED_DEV = 256
HIDDEN = 2560
FFN_DIM = 6912
NUM_HEADS = 20
KV_HEADS = 20
HEAD_DIM = 128
VIT_DIM = 1280
NUM_DOCS = 2

SEQ_LEN = GROUP_SIZE * TOK_DEV
MERGE_DIM = 4 * VIT_DIM
Q_WIDTH = NUM_HEADS * HEAD_DIM
KV_WIDTH = KV_HEADS * HEAD_DIM
NORM_EPS = 1e-6
ROPE_THETA = 1000000.0
MROPE_SPLIT = (16, 40)


def layout_draw(layout_key):
    sub_keys = jax.random.split(layout_key, 7)
    totals = jax.random.randint(sub_keys[0], (GROUP_SIZE,), MERGED_DEV // 4, MERGED_DEV + 1)
    full_dev = jax.random.randint(sub_keys[1], (), 0, GROUP_SIZE)
    totals = jnp.where(jnp.arange(GROUP_SIZE) == full_dev, MERGED_DEV, totals)
    first_len = jax.random.randint(sub_keys[2], (GROUP_SIZE,), 1, totals)
    img_sizes = jnp.stack([first_len, totals - first_len], axis=1).reshape(2 * GROUP_SIZE)
    img_order = jax.random.permutation(sub_keys[3], 2 * GROUP_SIZE)
    text_total = SEQ_LEN - jnp.sum(img_sizes)
    gap_weights = jax.random.randint(sub_keys[4], (2 * GROUP_SIZE + 1,), 1, 17)
    cum_weights = jnp.cumsum(gap_weights)
    text_before = text_total * cum_weights // cum_weights[-1]
    sizes_seq = img_sizes[img_order]
    start_seq = text_before[:-1] + jnp.cumsum(sizes_seq) - sizes_seq
    start_img = jnp.zeros((2 * GROUP_SIZE,), jnp.int32).at[img_order].set(start_seq.astype(jnp.int32))
    row_ids = jnp.arange(GROUP_SIZE * MERGED_DEV)
    dev_of = row_ids // MERGED_DEV
    local_row = row_ids % MERGED_DEV
    first_of = first_len[dev_of]
    second_img = local_row >= first_of
    img_id = 2 * dev_of + second_img.astype(jnp.int32)
    offset = local_row - jnp.where(second_img, first_of, 0)
    dest_slot = jnp.where(local_row < totals[dev_of], start_img[img_id] + offset, -1).astype(jnp.int32)
    doc_cuts = jnp.sort(jax.random.permutation(sub_keys[5], SEQ_LEN - 1)[:NUM_DOCS - 1] + 1).astype(jnp.int32)
    cu_doc = jnp.concatenate([jnp.zeros((1,), jnp.int32), doc_cuts, jnp.full((1,), SEQ_LEN, jnp.int32)])
    tokens = jnp.arange(SEQ_LEN)
    doc_id = jnp.sum(tokens[:, None] >= doc_cuts[None, :], axis=1)
    within = tokens - cu_doc[doc_id]
    is_image = jnp.zeros((SEQ_LEN,), jnp.bool_).at[jnp.where(dest_slot >= 0, dest_slot, SEQ_LEN)].set(True, mode='drop')
    grid_off = jax.random.randint(sub_keys[6], (2, SEQ_LEN), 0, 32)
    rope_pos = jnp.stack([within, within + jnp.where(is_image, grid_off[0], 0), within + jnp.where(is_image, grid_off[1], 0)]).astype(jnp.int32)
    return dest_slot, rope_pos, cu_doc


def gauss_draw(draw_key, shape, scale):
    return jax.random.normal(draw_key, shape, jnp.float32) * scale


def setup_inputs(seed: int = 0, part: int = 0) -> dict:
    root = jax.random.key(seed)
    part_key = jax.random.fold_in(root, part)
    layout_key, patch_key, embed_key = jax.random.split(part_key, 3)
    dest_slot, rope_pos, cu_doc = layout_draw(layout_key)
    wkeys = jax.random.split(jax.random.fold_in(root, 100003), 18)
    bf_type = jnp.bfloat16
    return dict(
        patches=gauss_draw(patch_key, (GROUP_SIZE * 4 * MERGED_DEV, VIT_DIM), 1.0).astype(bf_type),
        embeds=gauss_draw(embed_key, (SEQ_LEN, HIDDEN), 1.0).astype(bf_type),
        dest_slot=dest_slot,
        rope_pos=rope_pos,
        cu_doc=cu_doc,
        ln_w=(1.0 + gauss_draw(wkeys[0], (VIT_DIM,), 0.3)).astype(bf_type),
        ln_b=gauss_draw(wkeys[1], (VIT_DIM,), 0.3).astype(bf_type),
        w_one=gauss_draw(wkeys[2], (MERGE_DIM, MERGE_DIM), MERGE_DIM ** -0.5).astype(bf_type),
        b_one=gauss_draw(wkeys[3], (MERGE_DIM,), 0.5).astype(bf_type),
        w_two=gauss_draw(wkeys[4], (MERGE_DIM, HIDDEN), MERGE_DIM ** -0.5).astype(bf_type),
        b_two=gauss_draw(wkeys[5], (HIDDEN,), 0.5).astype(bf_type),
        norm_attn=(1.0 + gauss_draw(wkeys[6], (HIDDEN,), 0.3)).astype(bf_type),
        w_q=gauss_draw(wkeys[7], (HIDDEN, Q_WIDTH), 1.6 * HIDDEN ** -0.5).astype(bf_type),
        b_q=gauss_draw(wkeys[8], (Q_WIDTH,), 0.5).astype(bf_type),
        w_k=gauss_draw(wkeys[9], (HIDDEN, KV_WIDTH), 1.6 * HIDDEN ** -0.5).astype(bf_type),
        b_k=gauss_draw(wkeys[10], (KV_WIDTH,), 0.5).astype(bf_type),
        w_v=gauss_draw(wkeys[11], (HIDDEN, KV_WIDTH), HIDDEN ** -0.5).astype(bf_type),
        b_v=gauss_draw(wkeys[12], (KV_WIDTH,), 0.5).astype(bf_type),
        w_o=gauss_draw(wkeys[13], (Q_WIDTH, HIDDEN), Q_WIDTH ** -0.5).astype(bf_type),
        norm_mlp=(1.0 + gauss_draw(wkeys[14], (HIDDEN,), 0.3)).astype(bf_type),
        w_gate=gauss_draw(wkeys[15], (HIDDEN, FFN_DIM), HIDDEN ** -0.5).astype(bf_type),
        w_up=gauss_draw(wkeys[16], (HIDDEN, FFN_DIM), HIDDEN ** -0.5).astype(bf_type),
        w_down=gauss_draw(wkeys[17], (FFN_DIM, HIDDEN), FFN_DIM ** -0.5).astype(bf_type),
    )


def layer_norm(values_in, gain_vec, shift_vec):
    widened = values_in.astype(jnp.float32)
    centered = widened - jnp.mean(widened, axis=-1, keepdims=True)
    spread = jnp.mean(centered * centered, axis=-1, keepdims=True)
    return (centered * lax.rsqrt(spread + NORM_EPS) * gain_vec.astype(jnp.float32) + shift_vec.astype(jnp.float32)).astype(jnp.bfloat16)


def rms_norm(values_in, gain_vec):
    widened = values_in.astype(jnp.float32)
    return (widened * lax.rsqrt(jnp.mean(widened * widened, axis=-1, keepdims=True) + NORM_EPS) * gain_vec.astype(jnp.float32)).astype(jnp.bfloat16)


def merger_mlp(grouped, w_one, b_one, w_two, b_two):
    inner = jax.nn.gelu(jnp.dot(grouped, w_one, preferred_element_type=jnp.float32) + b_one.astype(jnp.float32), approximate=False).astype(jnp.bfloat16)
    return (jnp.dot(inner, w_two, preferred_element_type=jnp.float32) + b_two.astype(jnp.float32)).astype(jnp.bfloat16)


def rope_tables(rope_pos):
    inv_freq = ROPE_THETA ** (-jnp.arange(0, HEAD_DIM, 2, dtype=jnp.float32) / HEAD_DIM)
    freq_idx = jnp.arange(HEAD_DIM // 2)[None, :]
    chosen = jnp.where(freq_idx < MROPE_SPLIT[0], rope_pos[0][:, None], jnp.where(freq_idx < MROPE_SPLIT[1], rope_pos[1][:, None], rope_pos[2][:, None]))
    angles = chosen.astype(jnp.float32) * inv_freq[None, :]
    angles = jnp.concatenate([angles, angles], axis=-1)
    return jnp.cos(angles), jnp.sin(angles)


def apply_rope(heads_in, cos_t, sin_t):
    half_dim = HEAD_DIM // 2
    rotated = jnp.concatenate([-heads_in[..., half_dim:], heads_in[..., :half_dim]], axis=-1)
    return heads_in * cos_t[:, None, :] + rotated * sin_t[:, None, :]


def reference(patches, embeds, dest_slot, rope_pos, cu_doc, ln_w, ln_b, w_one, b_one, w_two, b_two, norm_attn, w_q, b_q, w_k, b_k, w_v, b_v, w_o, norm_mlp, w_gate, w_up, w_down):
    normed = layer_norm(patches, ln_w, ln_b).reshape(GROUP_SIZE * MERGED_DEV, MERGE_DIM)
    merged = merger_mlp(normed, w_one, b_one, w_two, b_two)
    target = jnp.where(dest_slot >= 0, dest_slot, SEQ_LEN)
    h_zero = embeds.at[target].set(merged, mode='drop')
    normed_a = rms_norm(h_zero, norm_attn)
    cos_t, sin_t = rope_tables(rope_pos)
    q_lin = jnp.dot(normed_a, w_q, preferred_element_type=jnp.float32) + b_q.astype(jnp.float32)
    k_lin = jnp.dot(normed_a, w_k, preferred_element_type=jnp.float32) + b_k.astype(jnp.float32)
    queries = apply_rope(q_lin.reshape(SEQ_LEN, NUM_HEADS, HEAD_DIM), cos_t, sin_t).astype(jnp.bfloat16)
    keys_rot = apply_rope(k_lin.reshape(SEQ_LEN, KV_HEADS, HEAD_DIM), cos_t, sin_t).astype(jnp.bfloat16)
    values_bf = (jnp.dot(normed_a, w_v, preferred_element_type=jnp.float32) + b_v.astype(jnp.float32)).astype(jnp.bfloat16).reshape(SEQ_LEN, KV_HEADS, HEAD_DIM)
    key_pos = jnp.arange(SEQ_LEN)
    doc_id = jnp.sum(key_pos[:, None] >= cu_doc[None, 1:NUM_DOCS], axis=1)
    keys_wide = keys_rot.astype(jnp.float32)
    values_wide = values_bf.astype(jnp.float32)
    q_blocks = queries.reshape(GROUP_SIZE, TOK_DEV, KV_HEADS, NUM_HEADS // KV_HEADS, HEAD_DIM)

    def attend(block_args):
        block_idx, q_block = block_args
        query_pos = block_idx * TOK_DEV + jnp.arange(TOK_DEV)
        query_doc = lax.dynamic_slice(doc_id, (block_idx * TOK_DEV,), (TOK_DEV,))
        allowed = (key_pos[None, :] <= query_pos[:, None]) & (query_doc[:, None] == doc_id[None, :])
        scores = jnp.einsum('qkgd,tkd->kgqt', q_block.astype(jnp.float32), keys_wide) * HEAD_DIM ** -0.5
        probs_bf = jax.nn.softmax(jnp.where(allowed, scores, -1e30), axis=-1).astype(jnp.bfloat16)
        return jnp.einsum('kgqt,tkd->qkgd', probs_bf.astype(jnp.float32), values_wide).astype(jnp.bfloat16)

    attn_out = lax.map(attend, (jnp.arange(GROUP_SIZE), q_blocks)).reshape(SEQ_LEN, Q_WIDTH)
    h_one = (h_zero.astype(jnp.float32) + jnp.dot(attn_out, w_o, preferred_element_type=jnp.float32)).astype(jnp.bfloat16)
    normed_m = rms_norm(h_one, norm_mlp)
    gate_pre = jnp.dot(normed_m, w_gate, preferred_element_type=jnp.float32)
    up_pre = jnp.dot(normed_m, w_up, preferred_element_type=jnp.float32)
    activated = (jax.nn.silu(gate_pre) * up_pre).astype(jnp.bfloat16)
    return (h_one.astype(jnp.float32) + jnp.dot(activated, w_down, preferred_element_type=jnp.float32)).astype(jnp.bfloat16)
```

```python
import functools

import jax
import jax.numpy as jnp
from jax import lax
from jax.experimental import pallas as pl
from jax.experimental.pallas import tpu as pltpu
from jax.sharding import PartitionSpec as P

HEAD_DIM = 128
NORM_EPS = 1e-6
ROPE_THETA = 1000000.0
MROPE_SPLIT = (16, 40)
CORES = 2
NEG_BIG = -1e30
LOG2_E = 1.4426950408889634
F32 = jnp.float32
BF16 = jnp.bfloat16
VMEM_LIMIT = 60 * 1024 * 1024


def cost(flops, nbytes, trans=0):
    return pl.CostEstimate(flops=int(flops), bytes_accessed=int(nbytes), transcendentals=int(trans))


def params(limit=VMEM_LIMIT):
    return pltpu.CompilerParams(vmem_limit_bytes=limit)


def dot32(lhs, rhs):
    return jnp.dot(lhs, rhs, preferred_element_type=F32)


def merger_kernel(x_ref, lnw_ref, lnb_ref, w1_ref, b1_ref, w2_ref, b2_ref, out_ref, wide_ref, z_ref, acc_ref):
    step = pl.program_id(0)
    rows, feat = out_ref.shape[0], x_ref.shape[1]

    @pl.when(step == 0)
    def _():
        x = x_ref[...].astype(F32)
        cent = x - jnp.mean(x, axis=-1, keepdims=True)
        var = jnp.mean(cent * cent, axis=-1, keepdims=True)
        normed = cent * lax.rsqrt(var + NORM_EPS) * lnw_ref[...].astype(F32) + lnb_ref[...].astype(F32)
        for j in range(feat // 128):
            wide_ref[j] = normed[:, j * 128:(j + 1) * 128]
        for i in range(4):
            for j in range(feat // 128):
                col = i * feat + j * 128
                z_ref[:, col:col + 128] = wide_ref[j, pl.ds(i, rows, stride=4), :].astype(BF16)
        acc_ref[...] = jnp.zeros_like(acc_ref)

    pre = dot32(z_ref[...], w1_ref[...]) + b1_ref[...].astype(F32)
    inner = (0.5 * pre * (1.0 + lax.erf(pre * 2.0 ** -0.5))).astype(BF16)
    acc_ref[...] += dot32(inner, w2_ref[...])

    @pl.when(step == pl.num_programs(0) - 1)
    def _():
        out_ref[...] = (acc_ref[...] + b2_ref[...].astype(F32)).astype(BF16)


def merger(patches, ln_w, ln_b, w_one, b_one, w_two, b_two):
    total, feat = patches.shape
    rows = total // 4
    depth, mid = w_one.shape
    hid = w_two.shape[1]
    tile = 512
    whole = lambda i: (0, 0)
    return pl.pallas_call(
        merger_kernel,
        grid=(mid // tile,),
        in_specs=[
            pl.BlockSpec((total, feat), whole),
            pl.BlockSpec((1, feat), whole),
            pl.BlockSpec((1, feat), whole),
            pl.BlockSpec((depth, tile), lambda i: (0, i)),
            pl.BlockSpec((1, tile), lambda i: (0, i)),
            pl.BlockSpec((tile, hid), lambda i: (i, 0)),
            pl.BlockSpec((1, hid), whole),
        ],
        out_specs=pl.BlockSpec((rows, hid), whole),
        out_shape=jax.ShapeDtypeStruct((rows, hid), BF16),
        scratch_shapes=[
            pltpu.VMEM((feat // 128, total, 128), F32),
            pltpu.VMEM((rows, depth), BF16),
            pltpu.VMEM((rows, hid), F32),
        ],
        compiler_params=params(),
        cost_estimate=cost(2 * rows * mid * (depth + hid), 2 * mid * (depth + hid)),
        name="merger",
    )(patches, ln_w[None], ln_b[None], w_one, b_one[None], w_two, b_two[None])


def place_kernel(info_ref, slots_ref, m_ref, placed_ref, mask_ref):
    step = pl.program_id(0)
    rows = placed_ref.shape[1]
    per_shard = info_ref[2] // rows
    base = info_ref[2] * (CORES * (step // per_shard) + info_ref[1]) + rows * (step % per_shard)
    pos = base + lax.broadcasted_iota(jnp.int32, (rows, slots_ref.shape[1]), 0)
    hit = (slots_ref[...] == pos).astype(F32)
    placed_ref[0] = dot32(hit.astype(BF16), m_ref[...]).astype(BF16)
    any_hit = jnp.max(hit, axis=1, keepdims=True)
    mask_ref[0] = jnp.broadcast_to(any_hit, mask_ref.shape[1:]).astype(BF16)


def place(info, slots, m_all, chips, tok):
    rows = 256
    hid = m_all.shape[1]
    per = tok // rows
    grid_spec = pltpu.PrefetchScalarGridSpec(
        num_scalar_prefetch=1,
        grid=(chips * per,),
        in_specs=[
            pl.BlockSpec((1, slots.shape[0]), lambda i, s: (0, 0)),
            pl.BlockSpec(m_all.shape, lambda i, s: (0, 0)),
        ],
        out_specs=[
            pl.BlockSpec((1, rows, hid), lambda i, s: (i // per, i % per, 0)),
            pl.BlockSpec((1, rows, 128), lambda i, s: (i // per, i % per, 0)),
        ],
    )
    return pl.pallas_call(
        place_kernel,
        grid_spec=grid_spec,
        out_shape=[jax.ShapeDtypeStruct((chips, tok, hid), BF16), jax.ShapeDtypeStruct((chips, tok, 128), BF16)],
        compiler_params=params(),
        cost_estimate=cost(2 * chips * tok * m_all.shape[0] * hid, 2 * m_all.size + 2 * chips * tok * hid),
        name="place",
    )(info, slots[None], m_all)


def qkv_kernel(info_ref, e_ref, p_ref, mask_ref, g_ref, cos_ref, sin_ref, bq_ref, bk_ref, bv_ref, wq_ref, wk_ref, wv_ref,
               q_ref, kv_ref, wq_buf, wk_buf, wv_buf, sems):
    width = wq_buf.shape[1]
    col = pl.multiple_of(info_ref[0] * width, width)
    first = pl.program_id(0) == 0
    pairs = ((wq_ref, wq_buf), (wk_ref, wk_buf), (wv_ref, wv_buf))

    def copy(i):
        src, dst = pairs[i]
        return pltpu.make_async_copy(src.at[:, pl.ds(col, width)], dst, sems.at[i])

    @pl.when(first)
    def _():
        for i in range(3):
            copy(i).start()

    chips, rows, hid = e_ref.shape
    flat = chips * rows
    hit = mask_ref[...].reshape(flat, 128)[:, :1].astype(F32) > 0.5
    h = jnp.where(hit, p_ref[...].reshape(flat, hid).astype(F32), e_ref[...].reshape(flat, hid).astype(F32))
    a = (h * lax.rsqrt(jnp.mean(h * h, axis=-1, keepdims=True) + NORM_EPS) * g_ref[...].astype(F32)).astype(BF16)
    cos_t = cos_ref[...].reshape(flat, HEAD_DIM)
    sin_t = sin_ref[...].reshape(flat, HEAD_DIM)

    def rope_to(lin, out_ref):
        for j in range(width // HEAD_DIM):
            cols = slice(j * HEAD_DIM, (j + 1) * HEAD_DIM)
            part = lin[:, cols]
            turned = part * cos_t + pltpu.roll(part, HEAD_DIM // 2, 1) * sin_t
            out_ref[:, :, cols] = turned.astype(BF16).reshape(chips, rows, HEAD_DIM)

    for i in range(3):
        @pl.when(first)
        def _():
            copy(i).wait()

        lin = dot32(a, pairs[i][1][...])
        if i == 0:
            rope_to(lin + bq_ref[...].astype(F32), q_ref)
        elif i == 1:
            rope_to(lin + bk_ref[...].astype(F32), kv_ref)
        else:
            v = (lin + bv_ref[...].astype(F32)).astype(BF16)
            kv_ref[:, :, width:] = v.reshape(chips, rows, width)


def qkv(info, e, placed, mask, cos_t, sin_t, norm, w_q, b_q, w_k, b_k, w_v, b_v, row0, width):
    chips, total, hid = e.shape
    rows = 128
    b0 = row0 // rows
    slab = lambda i, s: (0, i, 0)
    off = lambda i, s: (0, i + b0, 0)
    bias = pl.BlockSpec((1, width), lambda i, s: (0, s[0]))
    anyspec = pl.BlockSpec(memory_space=pl.ANY)
    grid_spec = pltpu.PrefetchScalarGridSpec(
        num_scalar_prefetch=1,
        grid=(total // rows,),
        in_specs=[
            pl.BlockSpec((chips, rows, hid), slab),
            pl.BlockSpec((chips, rows, hid), off),
            pl.BlockSpec((chips, rows, 128), off),
            pl.BlockSpec((1, hid), lambda i, s: (0, 0)),
            pl.BlockSpec((chips, rows, HEAD_DIM), off),
            pl.BlockSpec((chips, rows, HEAD_DIM), off),
            bias, bias, bias, anyspec, anyspec, anyspec,
        ],
        out_specs=[
            pl.BlockSpec((chips, rows, width), slab),
            pl.BlockSpec((chips, rows, 2 * width), slab),
        ],
        scratch_shapes=[pltpu.VMEM((hid, width), BF16)] * 3 + [pltpu.SemaphoreType.DMA((3,))],
    )
    return pl.pallas_call(
        qkv_kernel,
        grid_spec=grid_spec,
        out_shape=[jax.ShapeDtypeStruct((chips, total, width), BF16), jax.ShapeDtypeStruct((chips, total, 2 * width), BF16)],
        compiler_params=params(),
        cost_estimate=cost(2 * chips * total * hid * 3 * width, 2 * hid * 3 * width + 4 * chips * total * hid),
        name="qkv",
    )(info, e, placed, mask, norm[None], cos_t, sin_t, b_q[None], b_k[None], b_v[None], w_q, w_k, w_v)


def attn_kernel(num_docs, n_slab, *refs):
    info_ref = refs[0]
    q_refs = refs[1:1 + n_slab]
    groups = [refs[1 + n_slab * (1 + g):1 + n_slab * (2 + g)] for g in range(4)]
    k_own, v_own, k_sib, v_sib = groups
    o_ref, m_ref, l_ref, acc_ref = refs[1 + 5 * n_slab:]
    shard_chip, core = info_ref[0], info_ref[1]
    queries = o_ref.shape[0]
    q_base = queries * (CORES * shard_chip + core)
    q = jnp.concatenate([r[0] for r in q_refs], axis=0)
    q_pos = q_base + lax.broadcasted_iota(jnp.int32, (1, queries), 1)

    def doc_start(pos):
        start = jnp.zeros_like(pos)
        for d in range(1, num_docs):
            cut = info_ref[2 + d]
            start = jnp.where(pos >= cut, cut, start)
        return start

    starts = doc_start(q_pos)
    lo_start = doc_start(q_base)
    hi_start = doc_start(q_base + queries - 1)
    factor = HEAD_DIM ** -0.5 * LOG2_E
    halves = 2
    half = queries // halves

    def block(k_refs, v_refs, idx, k_base, masked, fresh):
        k = jnp.concatenate([r[idx] for r in k_refs], axis=0)
        v = jnp.concatenate([r[idx] for r in v_refs], axis=0)
        for i in range(halves):
            lanes = slice(i * half, (i + 1) * half)
            s = lax.dot_general(k, q[lanes], (((1,), (1,)), ((), ())), preferred_element_type=F32)
            if masked:
                k_pos = k_base + lax.broadcasted_iota(jnp.int32, s.shape, 0)
                s = jnp.where((k_pos <= q_pos[:, lanes]) & (k_pos >= starts[:, lanes]), s, NEG_BIG)
            top = jnp.max(s, axis=0, keepdims=True)
            if not fresh:
                old = m_ref[:, lanes]
                top = jnp.maximum(top, old)
            p = jnp.exp2((s - top) * factor)
            total = jnp.sum(p, axis=0, keepdims=True)
            out = lax.dot_general(v, p.astype(BF16), (((0,), (0,)), ((), ())), preferred_element_type=F32)
            if not fresh:
                alpha = jnp.exp2((old - top) * factor)
                total = total + l_ref[:, lanes] * alpha
                out = out + acc_ref[:, lanes] * alpha
            m_ref[:, lanes] = top
            l_ref[:, lanes] = total
            acc_ref[:, lanes] = out

    block(k_own, v_own, shard_chip, q_base, True, True)

    def sweep(k_refs, v_refs, parity, end):
        begin = (lo_start // queries - parity + 1) // CORES

        def body(j, carry):
            k_base = queries * (CORES * j + parity)

            @pl.when(k_base >= hi_start)
            def _():
                block(k_refs, v_refs, j, k_base, False, False)

            @pl.when(k_base < hi_start)
            def _():
                block(k_refs, v_refs, j, k_base, True, False)

            return carry

        lax.fori_loop(begin, end, body, 0)

    sweep(k_own, v_own, core, shard_chip)
    sweep(k_sib, v_sib, 1 - core, shard_chip + core)
    o_ref[...] = jnp.transpose(acc_ref[...] / l_ref[...]).astype(BF16)


def attention(info, qs, kvs, sibs, num_docs, tok, width):
    heads = width // HEAD_DIM
    chips = qs[0].shape[0]
    n_slab = len(qs)
    q_specs = [pl.BlockSpec((1, a.shape[1], HEAD_DIM), lambda h, s: (s[0], 0, h)) for a in qs]
    k_specs = [pl.BlockSpec((chips, a.shape[1], HEAD_DIM), lambda h, s: (0, 0, h)) for a in kvs]
    v_specs = [pl.BlockSpec((chips, a.shape[1], HEAD_DIM), lambda h, s: (0, 0, heads + h)) for a in kvs]
    grid_spec = pltpu.PrefetchScalarGridSpec(
        num_scalar_prefetch=1,
        grid=(heads,),
        in_specs=q_specs + k_specs + v_specs + k_specs + v_specs,
        out_specs=pl.BlockSpec((tok, HEAD_DIM), lambda h, s: (0, h)),
        scratch_shapes=[pltpu.VMEM((1, tok), F32), pltpu.VMEM((1, tok), F32), pltpu.VMEM((HEAD_DIM, tok), F32)],
    )
    return pl.pallas_call(
        functools.partial(attn_kernel, num_docs, n_slab),
        grid_spec=grid_spec,
        out_shape=jax.ShapeDtypeStruct((tok, width), BF16),
        compiler_params=params(),
        cost_estimate=cost(2 * 2 * tok * 5 * tok * width, 4 * chips * tok * 2 * width),
        name="attend",
    )(info, *qs, *kvs, *kvs, *sibs, *sibs)


def oproj_kernel(order, info_ref, *refs):
    chips = len(order)
    o_refs = refs[:chips]
    h_ref, g_ref, w_ref, h1_ref, b_ref, w_buf, sems = refs[chips:]
    width = w_buf.shape[1]

    def copy(i):
        src = lax.rem(info_ref[0] + chips - order[i], chips)
        return pltpu.make_async_copy(w_ref.at[pl.ds(pl.multiple_of(src * width, width), width), :], w_buf.at[i], sems.at[i])

    for i in range(chips):
        copy(i).start()
    acc = h_ref[...].astype(F32)
    total = None
    for i in range(chips):
        copy(i).wait()
        part = dot32(o_refs[i][...], w_buf[i])
        total = part if total is None else total + part
    h1 = (acc + total).astype(BF16)
    h1_ref[...] = h1
    wide = h1.astype(F32)
    b_ref[...] = (wide * lax.rsqrt(jnp.mean(wide * wide, axis=-1, keepdims=True) + NORM_EPS) * g_ref[...].astype(F32)).astype(BF16)


def oproj(info, outs, order, h_zero, norm, w_o):
    tok, hid = h_zero.shape
    width = outs[0].shape[1]
    chips = len(outs)
    vm = pl.BlockSpec(memory_space=pltpu.VMEM)
    return pl.pallas_call(
        functools.partial(oproj_kernel, order),
        in_specs=[pl.BlockSpec(memory_space=pltpu.SMEM)] + [vm] * (chips + 2) + [pl.BlockSpec(memory_space=pl.ANY)],
        out_specs=[vm, vm],
        out_shape=[jax.ShapeDtypeStruct((tok, hid), BF16)] * 2,
        scratch_shapes=[pltpu.VMEM((chips, width, hid), BF16), pltpu.SemaphoreType.DMA((chips,))],
        compiler_params=params(),
        cost_estimate=cost(2 * tok * hid * chips * width, 2 * chips * width * hid),
        name="oproj",
    )(info, *outs, h_zero, norm[None], w_o)


def mlp_kernel(h_ref, b_ref, wg_ref, wu_ref, wd_ref, out_ref, acc_ref):
    step = pl.program_id(0)

    @pl.when(step == 0)
    def _():
        acc_ref[...] = h_ref[...].astype(F32)

    b = b_ref[...]
    gate = dot32(b, wg_ref[...])
    up = dot32(b, wu_ref[...])
    act = (jax.nn.silu(gate) * up).astype(BF16)
    acc_ref[...] += dot32(act, wd_ref[...])

    @pl.when(step == pl.num_programs(0) - 1)
    def _():
        out_ref[...] = acc_ref[...].astype(BF16)


def mlp(h_one, normed, w_gate, w_up, w_down):
    tok, hid = h_one.shape
    ffn = w_gate.shape[1]
    tile = 768
    whole = lambda i: (0, 0)
    return pl.pallas_call(
        mlp_kernel,
        grid=(ffn // tile,),
        in_specs=[
            pl.BlockSpec((tok, hid), whole),
            pl.BlockSpec((tok, hid), whole),
            pl.BlockSpec((hid, tile), lambda i: (0, i)),
            pl.BlockSpec((hid, tile), lambda i: (0, i)),
            pl.BlockSpec((tile, hid), lambda i: (i, 0)),
        ],
        out_specs=pl.BlockSpec((tok, hid), whole),
        out_shape=jax.ShapeDtypeStruct((tok, hid), BF16),
        scratch_shapes=[pltpu.VMEM((tok, hid), F32)],
        compiler_params=params(),
        cost_estimate=cost(6 * tok * hid * ffn, 6 * hid * ffn),
        name="mlp",
    )(h_one, normed, w_gate, w_up, w_down)


def rope_tables(rope_pos):
    half = HEAD_DIM // 2
    inv_freq = ROPE_THETA ** (-jnp.arange(0, HEAD_DIM, 2, dtype=F32) / HEAD_DIM)
    idx = jnp.arange(half)
    lo, hi = MROPE_SPLIT
    chosen = jnp.where(idx < lo, rope_pos[:, 0, :, None], jnp.where(idx < hi, rope_pos[:, 1, :, None], rope_pos[:, 2, :, None]))
    angles = chosen.astype(F32) * inv_freq
    cos_h, sin_h = jnp.cos(angles), jnp.sin(angles)
    return jnp.concatenate([cos_h, cos_h], axis=-1), jnp.concatenate([-sin_h, sin_h], axis=-1)


def solution(mesh):
    group = mesh.shape['sp']
    chips = group // CORES
    row_spec = P(('dp', 'sp'), None)
    same_core = [[CORES * j + c for j in range(chips)] for c in range(CORES)]
    sibling = [(i, CORES * (i // CORES) + (i + 1) % CORES) for i in range(group)]

    def local_step(patches, embeds, dest_slot, rope_pos, cu_doc, ln_w, ln_b, w_one, b_one, w_two, b_two, norm_attn, w_q, b_q, w_k, b_k, w_v, b_v, w_o, norm_mlp, w_gate, w_up, w_down):
        tok, hid = embeds.shape
        merged_dev = dest_slot.shape[0]
        num_docs = cu_doc.shape[0] - 1
        me = lax.axis_index('sp')
        chip, core = me // CORES, me % CORES
        width = w_q.shape[1] // chips

        ints = jnp.concatenate([rope_pos, jnp.pad(dest_slot, (0, tok - merged_dev))[None]], axis=0)
        ints_all = lax.all_gather(ints, 'sp')
        slots = ints_all[:, 3, :merged_dev].reshape(-1)
        pos_own = lax.dynamic_index_in_dim(ints_all.reshape(chips, CORES, 4, tok), core, 1, keepdims=False)[:, :3]
        cos_t, sin_t = rope_tables(pos_own)

        cuts = ((0, tok // 2), (tok // 2, 3 * tok // 4), (3 * tok // 4, tok))
        gathered = []
        merged = None
        for n, (r0, r1) in enumerate(cuts):
            gathered.append(lax.all_gather(embeds[r0:r1], 'sp', axis_index_groups=same_core))
            if n == 0:
                merged = merger(patches, ln_w, ln_b, w_one, b_one, w_two, b_two)
                m_all = lax.all_gather(merged, 'sp', tiled=True)

        info = jnp.stack([chip, core, jnp.int32(tok)]).astype(jnp.int32)
        placed, mask = place(info, slots, m_all, chips, tok)
        h_zero = jnp.where(lax.dynamic_index_in_dim(mask, chip, 0, keepdims=False)[:, :1] > 0.5,
                           lax.dynamic_index_in_dim(placed, chip, 0, keepdims=False), embeds)

        qs, kvs, sibs = [], [], []
        for (r0, r1), e in zip(cuts, gathered):
            q, kv = qkv(info, e, placed, mask, cos_t, sin_t, norm_attn, w_q, b_q, w_k, b_k, w_v, b_v, r0, width)
            qs.append(q)
            kvs.append(kv)
            sibs.append(lax.ppermute(kv, 'sp', sibling))

        order = sorted(range(chips), key=lambda s: -min(s, chips - s))
        outs = []
        for s in order:
            target = (chip + s) % chips
            att_info = jnp.concatenate([jnp.stack([target, core]), cu_doc]).astype(jnp.int32)
            o = attention(att_info, qs, kvs, sibs, num_docs, tok, width)
            if s:
                o = lax.ppermute(o, 'sp', [(i, (i + CORES * s) % group) for i in range(group)])
            outs.append(o)
        h_one, normed = oproj(info, outs, tuple(order), h_zero, norm_mlp, w_o)
        return mlp(h_one, normed, w_gate, w_up, w_down)

    in_specs = (row_spec, row_spec, P(('dp', 'sp')), P(None, ('dp', 'sp')), P('dp')) + (P(),) * 18
    return jax.shard_map(local_step, mesh=mesh, in_specs=in_specs, out_specs=row_spec, check_vma=False)
```

```python
import functools

import jax
import jax.numpy as jnp
from jax import lax
from jax.experimental import pallas as pl
from jax.experimental.pallas import tpu as pltpu
from jax.sharding import PartitionSpec as P


HEAD_DIM = 128
NORM_EPS = 1e-6
ROPE_THETA = 1000000.0
MROPE_SPLIT = (16, 40)
CORES = 2
NEG_BIG = -1e30
LOG2_E = 1.4426950408889634
F32 = jnp.float32
BF16 = jnp.bfloat16
VMEM_LIMIT = 60 * 1024 * 1024


def cost(flops, nbytes, trans=0):
    return pl.CostEstimate(flops=int(flops), bytes_accessed=int(nbytes), transcendentals=int(trans))


def params(limit=VMEM_LIMIT):
    return pltpu.CompilerParams(vmem_limit_bytes=limit)


def dot32(lhs, rhs):
    return jnp.dot(lhs, rhs, preferred_element_type=F32)


def merger_kernel(x_ref, lnw_ref, lnb_ref, w1_ref, b1_ref, w2_ref, b2_ref, out_ref, wide_ref, z_ref, acc_ref):
    step = pl.program_id(0)
    rows, feat = out_ref.shape[0], x_ref.shape[1]

    @pl.when(step == 0)
    def _():
        x = x_ref[...].astype(F32)
        cent = x - jnp.mean(x, axis=-1, keepdims=True)
        var = jnp.mean(cent * cent, axis=-1, keepdims=True)
        normed = cent * lax.rsqrt(var + NORM_EPS) * lnw_ref[...].astype(F32) + lnb_ref[...].astype(F32)
        for j in range(feat // 128):
            wide_ref[j] = normed[:, j * 128:(j + 1) * 128]
        for i in range(4):
            for j in range(feat // 128):
                col = i * feat + j * 128
                z_ref[:, col:col + 128] = wide_ref[j, pl.ds(i, rows, stride=4), :].astype(BF16)
        acc_ref[...] = jnp.zeros_like(acc_ref)

    pre = dot32(z_ref[...], w1_ref[...]) + b1_ref[...].astype(F32)
    inner = (0.5 * pre * (1.0 + lax.erf(pre * 2.0 ** -0.5))).astype(BF16)
    acc_ref[...] += dot32(inner, w2_ref[...])

    @pl.when(step == pl.num_programs(0) - 1)
    def _():
        out_ref[...] = (acc_ref[...] + b2_ref[...].astype(F32)).astype(BF16)


def merger(patches, ln_w, ln_b, w_one, b_one, w_two, b_two):
    total, feat = patches.shape
    rows = total // 4
    depth, mid = w_one.shape
    hid = w_two.shape[1]
    tile = 512
    whole = lambda i: (0, 0)
    return pl.pallas_call(
        merger_kernel,
        grid=(mid // tile,),
        in_specs=[
            pl.BlockSpec((total, feat), whole),
            pl.BlockSpec((1, feat), whole),
            pl.BlockSpec((1, feat), whole),
            pl.BlockSpec((depth, tile), lambda i: (0, i)),
            pl.BlockSpec((1, tile), lambda i: (0, i)),
            pl.BlockSpec((tile, hid), lambda i: (i, 0)),
            pl.BlockSpec((1, hid), whole),
        ],
        out_specs=pl.BlockSpec((rows, hid), whole),
        out_shape=jax.ShapeDtypeStruct((rows, hid), BF16),
        scratch_shapes=[
            pltpu.VMEM((feat // 128, total, 128), F32),
            pltpu.VMEM((rows, depth), BF16),
            pltpu.VMEM((rows, hid), F32),
        ],
        compiler_params=params(),
        cost_estimate=cost(2 * rows * mid * (depth + hid), 2 * mid * (depth + hid)),
        name="merger",
    )(patches, ln_w[None], ln_b[None], w_one, b_one[None], w_two, b_two[None])


def stack_delta(i, chips):
    return jnp.where(i == chips - 1, chips // 2, jnp.where(i == chips - 2, chips - 1, i))


def place_kernel(sizes, chips, tok, info_ref, slots_ref, *refs):
    n = len(sizes)
    m_refs = refs[:n]
    placed_ref, mask_ref, m_buf, sems = refs[n:]
    step = pl.program_id(0)
    rows = placed_ref.shape[1]
    per_shard = tok // rows
    starts = [sum(sizes[:i]) for i in range(n)]

    def copy(i):
        return pltpu.make_async_copy(m_refs[i], m_buf.at[pl.ds(starts[i], sizes[i]), :], sems.at[i])

    @pl.when(step == 0)
    def _():
        for i in range(n):
            copy(i).start()
        for i in range(n):
            copy(i).wait()

    chip = lax.rem(info_ref[0] + stack_delta(step // per_shard, chips), chips)
    base = tok * (CORES * chip + info_ref[1]) + rows * (step % per_shard)
    pos = base + lax.broadcasted_iota(jnp.int32, (rows, slots_ref.shape[1]), 0)
    hit = (slots_ref[...] == pos).astype(F32)
    placed_ref[0] = dot32(hit.astype(BF16), m_buf[...]).astype(BF16)
    any_hit = jnp.max(hit, axis=1, keepdims=True)
    mask_ref[0] = jnp.broadcast_to(any_hit, mask_ref.shape[1:]).astype(BF16)


def place(info, slots, parts, chips, tok):
    rows = 256
    hid = parts[0].shape[1]
    per = tok // rows
    sizes = tuple(a.shape[0] for a in parts)
    grid_spec = pltpu.PrefetchScalarGridSpec(
        num_scalar_prefetch=1,
        grid=(chips * per,),
        in_specs=[pl.BlockSpec((1, slots.shape[0]), lambda i, s: (0, 0))] + [pl.BlockSpec(memory_space=pl.ANY)] * len(parts),
        out_specs=[
            pl.BlockSpec((1, rows, hid), lambda i, s: (i // per, i % per, 0)),
            pl.BlockSpec((1, rows, 128), lambda i, s: (i // per, i % per, 0)),
        ],
        scratch_shapes=[pltpu.VMEM((sum(sizes), hid), BF16), pltpu.SemaphoreType.DMA((len(sizes),))],
    )
    return pl.pallas_call(
        functools.partial(place_kernel, sizes, chips, tok),
        grid_spec=grid_spec,
        out_shape=[jax.ShapeDtypeStruct((chips, tok, hid), BF16), jax.ShapeDtypeStruct((chips, tok, 128), BF16)],
        compiler_params=params(),
        cost_estimate=cost(2 * chips * tok * sum(sizes) * hid, 2 * sum(sizes) * hid + 2 * chips * tok * hid),
        name="place",
    )(info, slots[None], *parts)


def qkv_kernel(first, piece_rows, want_h, info_ref, g_ref, mask_ref, cos_ref, sin_ref, bq_ref, bk_ref, bv_ref, placed_ref, wq_ref, wk_ref, wv_ref, *refs):
    n = len(piece_rows)
    total = sum(len(r) for r in piece_rows)
    e_refs = refs[:total]
    outs = refs[total:total + 3 + want_h]
    q_ref, k_ref, v_ref = outs[:3]
    e_buf, p_buf, a_buf, wq_buf, wk_buf, wv_buf, e_sems, p_sems, w_sems = refs[total + 3 + want_h:]
    width = wq_buf.shape[1]
    col = pl.multiple_of(info_ref[0] * width, width)
    weights = ((wq_ref, wq_buf), (wk_ref, wk_buf), (wv_ref, wv_buf))

    def load_weight(i):
        src, dst = weights[i]
        return pltpu.make_async_copy(src.at[:, pl.ds(col, width)], dst, w_sems.at[i])

    def loads(i):
        at = sum(len(r) for r in piece_rows[:i])
        row = 0
        out = [pltpu.make_async_copy(placed_ref.at[first + i], p_buf.at[i % 2], p_sems.at[i % 2])]
        for j, rows in enumerate(piece_rows[i]):
            out.append(pltpu.make_async_copy(e_refs[at + j], e_buf.at[i % 2, pl.ds(row, rows), :], e_sems.at[i % 2, j]))
            row += rows
        return out

    def prologue(i):
        for c in loads(i):
            c.wait()
        hit = mask_ref[first + i][:, :1].astype(F32) > 0.5
        h = jnp.where(hit, p_buf[i % 2].astype(F32), e_buf[i % 2].astype(F32))
        if want_h and i == 0:
            outs[3][...] = h.astype(BF16)
        a_buf[i % 2] = (h * lax.rsqrt(jnp.mean(h * h, axis=-1, keepdims=True) + NORM_EPS) * g_ref[...].astype(F32)).astype(BF16)

    for c in loads(0):
        c.start()
    for i in range(3):
        load_weight(i).start()
    prologue(0)
    for i in range(n):
        if i + 1 < n:
            for c in loads(i + 1):
                c.start()
        a = a_buf[i % 2]
        cos_t, sin_t = cos_ref[first + i], sin_ref[first + i]
        for j, (bias, out_ref) in enumerate(((bq_ref, q_ref), (bk_ref, k_ref), (bv_ref, v_ref))):
            if i == 0:
                load_weight(j).wait()
            lin = dot32(a, weights[j][1][...]) + bias[...].astype(F32)
            for h in range(width // HEAD_DIM):
                cols = slice(h * HEAD_DIM, (h + 1) * HEAD_DIM)
                part = lin[:, cols]
                if j < 2:
                    out_ref[i, :, cols] = (part * cos_t + pltpu.roll(part, HEAD_DIM // 2, 1) * sin_t).astype(BF16)
                else:
                    out_ref[i, cols, :] = jnp.transpose(part).astype(BF16)
        if i + 1 < n:
            prologue(i + 1)


def qkv(info, first, pieces, placed, mask, cos_t, sin_t, norm, w_q, b_q, w_k, b_k, w_v, b_v, width, want_h):
    tok, hid = placed.shape[1:]
    n = len(pieces)
    rows = tuple(tuple(a.shape[0] for a in p) for p in pieces)
    flat = [a for p in pieces for a in p]
    whole2 = lambda i, s: (0, 0)
    whole3 = lambda i, s: (0, 0, 0)
    bias = pl.BlockSpec((1, width), lambda i, s: (0, s[0]))
    anyspec = pl.BlockSpec(memory_space=pl.ANY)
    out_shape = [jax.ShapeDtypeStruct((n, tok, width), BF16)] * 2 + [jax.ShapeDtypeStruct((n, width, tok), BF16)]
    out_specs = [pl.BlockSpec((n, tok, width), whole3)] * 2 + [pl.BlockSpec((n, width, tok), whole3)]
    if want_h:
        out_shape.append(jax.ShapeDtypeStruct((tok, hid), BF16))
        out_specs.append(pl.BlockSpec((tok, hid), whole2))
    most = max(len(r) for r in rows)
    grid_spec = pltpu.PrefetchScalarGridSpec(
        num_scalar_prefetch=1,
        grid=(1,),
        in_specs=[
            pl.BlockSpec((1, hid), whole2),
            pl.BlockSpec(mask.shape, whole3),
            pl.BlockSpec(cos_t.shape, whole3),
            pl.BlockSpec(sin_t.shape, whole3),
            bias, bias, bias,
        ] + [anyspec] * (4 + len(flat)),
        out_specs=out_specs,
        scratch_shapes=[
            pltpu.VMEM((2, tok, hid), BF16),
            pltpu.VMEM((2, tok, hid), BF16),
            pltpu.VMEM((2, tok, hid), BF16),
            pltpu.VMEM((hid, width), BF16),
            pltpu.VMEM((hid, width), BF16),
            pltpu.VMEM((hid, width), BF16),
            pltpu.SemaphoreType.DMA((2, most)),
            pltpu.SemaphoreType.DMA((2,)),
            pltpu.SemaphoreType.DMA((3,)),
        ],
    )
    return pl.pallas_call(
        functools.partial(qkv_kernel, first, rows, int(want_h)),
        grid_spec=grid_spec,
        out_shape=out_shape,
        compiler_params=params(),
        cost_estimate=cost(2 * n * tok * hid * 3 * width, 2 * hid * 3 * width + 4 * n * tok * hid),
        name="qkv",
    )(info, norm[None], mask, cos_t, sin_t, b_q[None], b_k[None], b_v[None], placed, w_q, w_k, w_v, *flat)


def attn_kernel(num_docs, chips, head0, info_ref, *refs):
    q_in, k_own_in, k_sib_in, v_own_in, v_sib_in = (refs[2 * g:2 * g + 2] for g in range(5))
    o_ref, q_buf, k_buf, v_buf, sems, m_ref, l_ref, acc_ref = refs[10:]
    head = pl.program_id(0)
    slot = lax.rem(head, 2)
    my_chip, core = info_ref[0], info_ref[1]
    tok = o_ref.shape[1]

    def copies(h, s):
        col = pl.multiple_of((head0 + h) * HEAD_DIM, HEAD_DIM)
        out = []
        lo = 0
        for g in range(2):
            n = q_in[g].shape[0]
            span = pl.ds(lo, n)
            lo += n
            cols = pl.ds(col, HEAD_DIM)
            out.append(pltpu.make_async_copy(q_in[g].at[:, :, cols], q_buf.at[s, span], sems.at[s, 5 * g]))
            out.append(pltpu.make_async_copy(k_own_in[g].at[:, :, cols], k_buf.at[s, 0, span], sems.at[s, 5 * g + 1]))
            out.append(pltpu.make_async_copy(k_sib_in[g].at[:, :, cols], k_buf.at[s, 1, span], sems.at[s, 5 * g + 2]))
            out.append(pltpu.make_async_copy(v_own_in[g].at[:, cols, :], v_buf.at[s, 0, span], sems.at[s, 5 * g + 3]))
            out.append(pltpu.make_async_copy(v_sib_in[g].at[:, cols, :], v_buf.at[s, 1, span], sems.at[s, 5 * g + 4]))
        return out

    @pl.when(head == 0)
    def _():
        for c in copies(0, 0):
            c.start()

    @pl.when(head + 1 < pl.num_programs(0))
    def _():
        for c in copies(head + 1, 1 - slot):
            c.start()

    for c in copies(head, slot):
        c.wait()

    def place_of(chip):
        delta = lax.rem(chip - my_chip + chips, chips)
        return jnp.where(delta == chips // 2, chips - 1, jnp.where(delta == chips - 1, chips - 2, delta))

    def doc_start(pos):
        start = jnp.zeros_like(pos)
        for d in range(1, num_docs):
            cut = info_ref[2 + d]
            start = jnp.where(pos >= cut, cut, start)
        return start

    factor = HEAD_DIM ** -0.5 * LOG2_E
    halves = 2
    half = tok // halves

    def queries(q_chip, carry):
        q_at = place_of(q_chip)
        q_base = tok * (CORES * q_chip + core)
        q = q_buf[slot, q_at]
        q_pos = q_base + lax.broadcasted_iota(jnp.int32, (1, tok), 1)
        starts = doc_start(q_pos)
        lo_start = doc_start(q_base)
        hi_start = doc_start(q_base + tok - 1)

        def block(j, masked, fresh):
            at = place_of(j)
            bases = (tok * (CORES * j + core), tok * (CORES * j + 1 - core))
            ks = [k_buf[slot, b, at] for b in range(2)]
            vs = jnp.concatenate([v_buf[slot, b, at] for b in range(2)], axis=1)
            scores = [[lax.dot_general(k, q[i * half:(i + 1) * half], (((1,), (1,)), ((), ())), preferred_element_type=F32) for k in ks] for i in range(halves)]
            for i in range(halves):
                lanes = slice(i * half, (i + 1) * half)
                pair = scores[i]
                if masked:
                    for b in range(2):
                        k_pos = bases[b] + lax.broadcasted_iota(jnp.int32, pair[b].shape, 0)
                        pair[b] = jnp.where((k_pos <= q_pos[:, lanes]) & (k_pos >= starts[:, lanes]), pair[b], NEG_BIG)
                top = jnp.maximum(jnp.max(pair[0], axis=0, keepdims=True), jnp.max(pair[1], axis=0, keepdims=True))
                if not fresh:
                    old = m_ref[:, lanes]
                    top = jnp.maximum(top, old)
                probs = [jnp.exp2((s - top) * factor) for s in pair]
                total = jnp.sum(probs[0], axis=0, keepdims=True) + jnp.sum(probs[1], axis=0, keepdims=True)
                out = dot32(vs, jnp.concatenate([p.astype(BF16) for p in probs], axis=0))
                if not fresh:
                    alpha = jnp.exp2((old - top) * factor)
                    total = total + l_ref[:, lanes] * alpha
                    out = out + acc_ref[:, lanes] * alpha
                m_ref[:, lanes] = top
                l_ref[:, lanes] = total
                acc_ref[:, lanes] = out

        block(q_chip, True, True)

        def body(t, inner):
            j = q_chip - 1 - t
            clear = tok * CORES * j >= hi_start

            @pl.when(clear)
            def _():
                block(j, False, False)

            @pl.when(jnp.logical_not(clear))
            def _():
                block(j, True, False)

            return inner

        lax.fori_loop(0, q_chip - lo_start // (tok * CORES), body, 0)
        o_ref[q_at] = jnp.transpose(acc_ref[...] / l_ref[...]).astype(BF16)
        return carry

    lax.fori_loop(0, chips, queries, 0)


def attention(info, qs, ks, k_sibs, vs, v_sibs, num_docs, chips, tok, head0, heads):
    grid_spec = pltpu.PrefetchScalarGridSpec(
        num_scalar_prefetch=1,
        grid=(heads,),
        in_specs=[pl.BlockSpec(memory_space=pl.ANY)] * 10,
        out_specs=pl.BlockSpec((chips, tok, HEAD_DIM), lambda h, s: (0, 0, h)),
        scratch_shapes=[
            pltpu.VMEM((2, chips, tok, HEAD_DIM), BF16),
            pltpu.VMEM((2, 2, chips, tok, HEAD_DIM), BF16),
            pltpu.VMEM((2, 2, chips, HEAD_DIM, tok), BF16),
            pltpu.SemaphoreType.DMA((2, 10)),
            pltpu.VMEM((1, tok), F32),
            pltpu.VMEM((1, tok), F32),
            pltpu.VMEM((HEAD_DIM, tok), F32),
        ],
    )
    width = heads * HEAD_DIM
    return pl.pallas_call(
        functools.partial(attn_kernel, num_docs, chips, head0),
        grid_spec=grid_spec,
        out_shape=jax.ShapeDtypeStruct((chips, tok, width), BF16),
        compiler_params=params(),
        cost_estimate=cost(2 * 2 * 20 * tok * tok * width, 2 * 5 * chips * tok * width),
        name="attend",
    )(info, *qs, *ks, *k_sibs, *vs, *v_sibs)


def oproj_kernel(shifts, info_ref, *refs):
    chips = len(shifts)
    n = 2 * chips
    o_refs = refs[:n]
    h_ref, g_ref, w_ref, h1_ref, b_ref, w_bufs, o_bufs, sems = refs[n], refs[n + 1], refs[n + 2], refs[n + 3], refs[n + 4], refs[n + 5:n + 7], refs[n + 7:n + 9], refs[n + 9]
    widths = [o_refs[0].shape[1], o_refs[chips].shape[1]]

    def copies(g, i):
        wide = widths[g]
        src = lax.rem(info_ref[0] + 2 * chips - shifts[i], chips)
        row = pl.multiple_of(src * sum(widths) + g * widths[0], HEAD_DIM)
        return (
            pltpu.make_async_copy(w_ref.at[pl.ds(row, wide), :], w_bufs[g].at[pl.ds(i * wide, wide), :], sems.at[g, i]),
            pltpu.make_async_copy(o_refs[g * chips + i], o_bufs[g].at[:, pl.ds(i * wide, wide)], sems.at[g, chips + i]),
        )

    for g in range(2):
        for i in range(chips):
            for c in copies(g, i):
                c.start()
    parts = []
    for g in range(2):
        for i in range(chips):
            for c in copies(g, i):
                c.wait()
        parts.append(dot32(o_bufs[g][...], w_bufs[g][...]))
    h1 = (h_ref[...].astype(F32) + (parts[0] + parts[1])).astype(BF16)
    h1_ref[...] = h1
    wide = h1.astype(F32)
    b_ref[...] = (wide * lax.rsqrt(jnp.mean(wide * wide, axis=-1, keepdims=True) + NORM_EPS) * g_ref[...].astype(F32)).astype(BF16)


def oproj(info, outs_a, outs_b, shifts, h_zero, norm, w_o):
    tok, hid = h_zero.shape
    wide_a, wide_b = outs_a[0].shape[1], outs_b[0].shape[1]
    chips = len(shifts)
    vm = pl.BlockSpec(memory_space=pltpu.VMEM)
    anyspec = pl.BlockSpec(memory_space=pl.ANY)
    return pl.pallas_call(
        functools.partial(oproj_kernel, shifts),
        in_specs=[pl.BlockSpec(memory_space=pltpu.SMEM)] + [anyspec] * (2 * chips) + [vm] * 2 + [anyspec],
        out_specs=[vm, vm],
        out_shape=[jax.ShapeDtypeStruct((tok, hid), BF16)] * 2,
        scratch_shapes=[
            pltpu.VMEM((chips * wide_a, hid), BF16),
            pltpu.VMEM((chips * wide_b, hid), BF16),
            pltpu.VMEM((tok, chips * wide_a), BF16),
            pltpu.VMEM((tok, chips * wide_b), BF16),
            pltpu.SemaphoreType.DMA((2, 2 * chips)),
        ],
        compiler_params=params(),
        cost_estimate=cost(2 * tok * hid * chips * (wide_a + wide_b), 2 * chips * (wide_a + wide_b) * hid),
        name="oproj",
    )(info, *outs_a, *outs_b, h_zero, norm[None], w_o)


def mlp_kernel(h_ref, b_ref, wg_ref, wu_ref, wd_ref, out_ref, acc_ref):
    step = pl.program_id(0)

    @pl.when(step == 0)
    def _():
        acc_ref[...] = h_ref[...].astype(F32)

    b = b_ref[...]
    gate = dot32(b, wg_ref[...])
    up = dot32(b, wu_ref[...])
    act = (jax.nn.silu(gate) * up).astype(BF16)
    acc_ref[...] += dot32(act, wd_ref[...])

    @pl.when(step == pl.num_programs(0) - 1)
    def _():
        out_ref[...] = acc_ref[...].astype(BF16)


def mlp(h_one, normed, w_gate, w_up, w_down):
    tok, hid = h_one.shape
    ffn = w_gate.shape[1]
    tile = 768
    whole = lambda i: (0, 0)
    return pl.pallas_call(
        mlp_kernel,
        grid=(ffn // tile,),
        in_specs=[
            pl.BlockSpec((tok, hid), whole),
            pl.BlockSpec((tok, hid), whole),
            pl.BlockSpec((hid, tile), lambda i: (0, i)),
            pl.BlockSpec((hid, tile), lambda i: (0, i)),
            pl.BlockSpec((tile, hid), lambda i: (i, 0)),
        ],
        out_specs=pl.BlockSpec((tok, hid), whole),
        out_shape=jax.ShapeDtypeStruct((tok, hid), BF16),
        scratch_shapes=[pltpu.VMEM((tok, hid), F32)],
        compiler_params=params(),
        cost_estimate=cost(6 * tok * hid * ffn, 6 * hid * ffn),
        name="mlp",
    )(h_one, normed, w_gate, w_up, w_down)


def rope_tables(rope_pos):
    half = HEAD_DIM // 2
    inv_freq = ROPE_THETA ** (-jnp.arange(0, HEAD_DIM, 2, dtype=F32) / HEAD_DIM)
    idx = jnp.arange(half)
    lo, hi = MROPE_SPLIT
    chosen = jnp.where(idx < lo, rope_pos[:, 0, :, None], jnp.where(idx < hi, rope_pos[:, 1, :, None], rope_pos[:, 2, :, None]))
    angles = chosen.astype(F32) * inv_freq
    cos_h, sin_h = jnp.cos(angles), jnp.sin(angles)
    return jnp.concatenate([cos_h, cos_h], axis=-1), jnp.concatenate([-sin_h, sin_h], axis=-1)


def solution(mesh):
    group = mesh.shape['sp']
    chips = group // CORES
    row_spec = P(('dp', 'sp'), None)
    sibling = [(i, CORES * (i // CORES) + (i + 1) % CORES) for i in range(group)]

    def hop(x, steps):
        return lax.ppermute(x, 'sp', [(i, (i + CORES * steps) % group) for i in range(group)])

    def swap(x):
        return lax.ppermute(x, 'sp', sibling)

    def step(patches, embeds, dest_slot, rope_pos, cu_doc, ln_w, ln_b, w_one, b_one, w_two, b_two, norm_attn, w_q, b_q, w_k, b_k, w_v, b_v, w_o, norm_mlp, w_gate, w_up, w_down):
        tok, _ = embeds.shape
        merged_dev = dest_slot.shape[0]
        num_docs = cu_doc.shape[0] - 1
        me = lax.axis_index('sp')
        chip, core = me // CORES, me % CORES
        width = w_q.shape[1] // chips
        mid = tok // 2
        quarter = mid // 2
        half_m = merged_dev // 2
        info = jnp.stack([chip, core]).astype(jnp.int32)

        ints = jnp.concatenate([rope_pos, jnp.pad(dest_slot, (0, tok - merged_dev))[None]], axis=0)
        ints_all = lax.all_gather(ints, 'sp').reshape(chips, CORES, 4, tok)
        rolled = lax.dynamic_slice_in_dim(jnp.concatenate([ints_all, ints_all], axis=0), chip, chips, 0)
        rolled = jnp.stack([rolled[0], rolled[1], rolled[3], rolled[2]])
        own = lax.dynamic_index_in_dim(rolled, core, 1, keepdims=False)
        sib = lax.dynamic_index_in_dim(rolled, 1 - core, 1, keepdims=False)
        slots = jnp.concatenate([own[:, 3, :merged_dev], sib[:, 3, :merged_dev]]).reshape(-1)
        cos_t, sin_t = rope_tables(own[:, :3])
        embeds, ints_all = lax.optimization_barrier((embeds, ints_all))

        e_a, e_b = embeds[:mid], embeds[mid:]
        a_prev = hop(e_a, 1)
        a_next = hop(e_a, -1)
        merged = merger(patches, ln_w, ln_b, w_one, b_one, w_two, b_two)
        m_prev = hop(merged, 1)
        m_next = hop(merged, -1)
        m_far_lo = hop(m_prev[:half_m], 1)
        m_far_hi = hop(m_next[half_m:], -1)
        mine = [merged, m_next, m_prev, m_far_lo, m_far_hi]
        theirs = [swap(m) for m in mine]
        b_prev = hop(e_b, 1)
        b_next = hop(e_b, -1)
        a_far_lo = hop(a_prev[:quarter], 1)
        a_far_hi = hop(a_next[quarter:], -1)
        b_far_lo = hop(b_prev[:quarter], 1)
        b_far_hi = hop(b_next[quarter:], -1)

        placed, mask = place(info, slots, mine + theirs, chips, tok)
        common = (placed, mask, cos_t, sin_t, norm_attn, w_q, b_q, w_k, b_k, w_v, b_v, width)
        near = [[embeds], [a_next, b_next], [a_prev, b_prev]]
        q_n, k_n, v_n, h_zero = qkv(info, 0, near, *common, True)
        far = [[a_far_lo, a_far_hi, b_far_lo, b_far_hi]]
        k_sib_n, v_sib_n = swap(k_n), swap(v_n)
        q_f, k_f, v_f = qkv(info, len(near), far, *common, False)
        k_sibs = [k_sib_n, swap(k_f)]
        v_sibs = [v_sib_n, swap(v_f)]

        att_info = jnp.concatenate([info, cu_doc]).astype(jnp.int32)
        heads = width // HEAD_DIM
        split = (heads + 1) // 2
        shifts = (0, 1, -1, chips // 2)
        parts = []
        for head0, n in ((0, split), (split, heads - split)):
            o = attention(att_info, (q_n, q_f), (k_n, k_f), k_sibs, (v_n, v_f), v_sibs, num_docs, chips, tok, head0, n)
            parts.append([o[0]] + [hop(o[i], shifts[i]) for i in range(1, chips)])
        h_one, normed = oproj(info, parts[0], parts[1], shifts, h_zero, norm_mlp, w_o)
        return mlp(h_one, normed, w_gate, w_up, w_down)

    in_specs = (row_spec, row_spec, P(('dp', 'sp')), P(None, ('dp', 'sp')), P('dp')) + (P(),) * 18
    return jax.shard_map(step, mesh=mesh, in_specs=in_specs, out_specs=row_spec, check_vma=False)
```

```python
import functools

import jax
import jax.numpy as jnp
from jax import lax
from jax.experimental import pallas as pl
from jax.experimental.pallas import tpu as pltpu
from jax.sharding import PartitionSpec as P


HEAD_DIM = 128
NORM_EPS = 1e-6
ROPE_THETA = 1000000.0
MROPE_SPLIT = (16, 40)
CORES = 2
NEG_BIG = -1e30
LOG2_E = 1.4426950408889634
F32 = jnp.float32
BF16 = jnp.bfloat16
VMEM_LIMIT = 60 * 1024 * 1024


def cost(flops, nbytes, trans=0):
    return pl.CostEstimate(flops=int(flops), bytes_accessed=int(nbytes), transcendentals=int(trans))


def params(limit=VMEM_LIMIT):
    return pltpu.CompilerParams(vmem_limit_bytes=limit)


def dot32(lhs, rhs):
    return jnp.dot(lhs, rhs, preferred_element_type=F32)


def merger_kernel(x_ref, lnw_ref, lnb_ref, w1_ref, b1_ref, w2_ref, b2_ref, out_ref, wide_ref, z_ref, pre_ref, acc_ref):
    step = pl.program_id(0)
    last = pl.num_programs(0) - 1
    rows, feat = out_ref.shape[0], x_ref.shape[1]

    @pl.when(step == 0)
    def _():
        chunk = 32

        def norm_rows(n, carry):
            at = pl.ds(pl.multiple_of(n * chunk, chunk), chunk)
            x = x_ref[at, :].astype(F32)
            cent = x - jnp.mean(x, axis=-1, keepdims=True)
            var = jnp.mean(cent * cent, axis=-1, keepdims=True)
            normed = cent * lax.rsqrt(var + NORM_EPS) * lnw_ref[...].astype(F32) + lnb_ref[...].astype(F32)
            for j in range(feat // 128):
                wide_ref[j, at, :] = normed[:, j * 128:(j + 1) * 128]
            return carry

        lax.fori_loop(0, x_ref.shape[0] // chunk, norm_rows, 0)
        for i in range(4):
            for j in range(feat // 128):
                col = i * feat + j * 128
                z_ref[:, col:col + 128] = wide_ref[j, pl.ds(i, rows, stride=4), :].astype(BF16)
        acc_ref[...] = jnp.zeros_like(acc_ref)
        pre_ref[...] = jnp.zeros_like(pre_ref)

    def second(pre):
        inner = (0.5 * pre * (1.0 + lax.erf(pre * 2.0 ** -0.5))).astype(BF16)
        return dot32(inner, w2_ref[...])

    @pl.when(step < last)
    def _():
        before = pre_ref[...]
        pre_ref[...] = dot32(z_ref[...], w1_ref[...]) + b1_ref[...].astype(F32)
        acc_ref[...] += second(before)

    @pl.when(step == last)
    def _():
        out_ref[...] = (acc_ref[...] + second(pre_ref[...]) + b2_ref[...].astype(F32)).astype(BF16)


def merger(patches, ln_w, ln_b, w_one, b_one, w_two, b_two):
    total, feat = patches.shape
    rows = total // 4
    depth, mid = w_one.shape
    hid = w_two.shape[1]
    tile = 512
    whole = lambda i: (0, 0)
    return pl.pallas_call(
        merger_kernel,
        grid=(mid // tile + 1,),
        in_specs=[
            pl.BlockSpec((total, feat), whole),
            pl.BlockSpec((1, feat), whole),
            pl.BlockSpec((1, feat), whole),
            pl.BlockSpec((depth, tile), lambda i: (0, jnp.minimum(i, mid // tile - 1))),
            pl.BlockSpec((1, tile), lambda i: (0, jnp.minimum(i, mid // tile - 1))),
            pl.BlockSpec((tile, hid), lambda i: (jnp.maximum(i - 1, 0), 0)),
            pl.BlockSpec((1, hid), whole),
        ],
        out_specs=pl.BlockSpec((rows, hid), whole),
        out_shape=jax.ShapeDtypeStruct((rows, hid), BF16),
        scratch_shapes=[
            pltpu.VMEM((feat // 128, total, 128), F32),
            pltpu.VMEM((rows, depth), BF16),
            pltpu.VMEM((rows, tile), F32),
            pltpu.VMEM((rows, hid), F32),
        ],
        compiler_params=params(),
        cost_estimate=cost(2 * rows * mid * (depth + hid), 2 * mid * (depth + hid)),
        name="merger",
    )(patches, ln_w[None], ln_b[None], w_one, b_one[None], w_two, b_two[None])


def qkv_kernel(near, n_parts, e_counts, chips, info_ref, *refs):
    g_ref, cos_ref, sin_ref, bq_ref, bk_ref, bv_ref, wq_ref, wk_ref, wv_ref = refs[:9]
    n = len(e_counts)
    pos = 9
    e_refs = refs[pos:pos + sum(e_counts)]
    pos += len(e_refs)
    if near:
        slots_ref = refs[pos]
        m_refs = refs[pos + 1:pos + 1 + n_parts]
        pos += 1 + n_parts
        q_ref, k_ref, v_ref, h_ref, far_ref, far_mask_ref, e_buf, a_buf, w_buf, e_sems, w_sems, m_buf, acc_ref, any_ref, m_sems = refs[pos:]
    else:
        far_ref, far_mask_ref = refs[pos:pos + 2]
        q_ref, k_ref, v_ref, e_buf, a_buf, w_buf, e_sems, w_sems = refs[pos + 2:]
    first = 0 if near else chips - 1
    width = w_buf.shape[1] // 3
    heads = width // HEAD_DIM
    col = pl.multiple_of(info_ref[0] * width, width)
    tok, _ = a_buf.shape[1:]
    block = 256
    w_refs = (wq_ref, wk_ref, wv_ref)

    def load_weight(i):
        return pltpu.make_async_copy(w_refs[i].at[:, pl.ds(col, width)], w_buf.at[:, pl.ds(i * width, width)], w_sems.at[i])

    def loads(i):
        at = sum(e_counts[:i])
        row = 0
        out = []
        for j in range(e_counts[i]):
            rows = e_refs[at + j].shape[0]
            out.append(pltpu.make_async_copy(e_refs[at + j], e_buf.at[i % 2, pl.ds(row, rows), :], e_sems.at[i % 2, j]))
            row += rows
        return out

    if near:
        m_copies = []
        row = 0
        for j, m in enumerate(m_refs):
            m_copies.append(pltpu.make_async_copy(m, m_buf.at[pl.ds(row, m.shape[0]), :], m_sems.at[j]))
            row += m.shape[0]
        for c in m_copies:
            c.start()
    for c in loads(0):
        c.start()
    for i in range(3):
        load_weight(i).start()
    if near:
        for c in m_copies:
            c.wait()

    def gather_rows(shard, part):
        blocks = m_buf.shape[0] // block
        delta = chips // 2 if shard == chips - 1 else chips - 1 if shard == chips - 2 else shard
        chip = lax.rem(info_ref[0] + delta, chips)
        base = tok * (CORES * chip + info_ref[1]) + block * part
        acc_ref[...] = jnp.zeros_like(acc_ref)
        any_ref[...] = jnp.zeros_like(any_ref)

        def visit(j, carry):
            @pl.when(info_ref[2 + (shard * (tok // block) + part) * blocks + j] > 0)
            def _():
                token = base + lax.broadcasted_iota(jnp.int32, (block, block), 0)
                hit = (slots_ref[pl.ds(j, 1), :] == token).astype(F32)
                at = pl.ds(pl.multiple_of(j * block, block), block)
                acc_ref[...] += dot32(hit.astype(BF16), m_buf[at, :])
                any_ref[...] = jnp.maximum(any_ref[...], jnp.max(hit, axis=1, keepdims=True))

            return carry

        lax.fori_loop(0, blocks, visit, 0)

    chunk = 32

    def place_rows(i):
        for c in loads(i):
            c.wait()
        for part in range(tok // block):
            if near:
                gather_rows(i, part)
            for r in range(0, block, chunk):
                at = slice(part * block + r, part * block + r + chunk)
                if near:
                    hit, rows = any_ref[r:r + chunk, :1] > 0.5, acc_ref[r:r + chunk, :]
                else:
                    hit, rows = far_mask_ref[at, :1].astype(F32) > 0.5, far_ref[at, :].astype(F32)
                e_buf[i % 2, at, :] = jnp.where(hit, rows, e_buf[i % 2, at, :].astype(F32)).astype(BF16)
        if near and i == 0:
            h_ref[...] = e_buf[0]

    def norm_rows(i):
        for r in range(0, tok, chunk):
            h = e_buf[i % 2, r:r + chunk, :].astype(F32)
            scale = lax.rsqrt(jnp.mean(h * h, axis=-1, keepdims=True) + NORM_EPS)
            a_buf[i % 2, r:r + chunk, :] = (h * scale * g_ref[...].astype(F32)).astype(BF16)

    def emit(i, head, part, cos_t, sin_t):
        kind, h = divmod(head, heads)
        cols = slice(h * HEAD_DIM, (h + 1) * HEAD_DIM)
        bias = (bq_ref, bk_ref, bv_ref)[kind][:, pl.ds(pl.multiple_of(col + h * HEAD_DIM, HEAD_DIM), HEAD_DIM)]
        part = part + bias.astype(F32)
        if kind < 2:
            (q_ref, k_ref)[kind][i, :, cols] = (part * cos_t + pltpu.roll(part, HEAD_DIM // 2, 1) * sin_t).astype(BF16)
        else:
            v_ref[i, cols, :] = jnp.transpose(part).astype(BF16)

    place_rows(0)
    norm_rows(0)
    for i in range(n):
        if i + 1 < n:
            for c in loads(i + 1):
                c.start()
            place_rows(i + 1)
            norm_rows(i + 1)
        if i == 0:
            for j in range(3):
                load_weight(j).wait()
        a = a_buf[i % 2]
        cos_t, sin_t = cos_ref[first + i], sin_ref[first + i]
        for head in range(0, 3 * heads, 2):
            span = min(2, 3 * heads - head)
            lin = dot32(a, w_buf[:, head * HEAD_DIM:(head + span) * HEAD_DIM])
            for d in range(span):
                emit(i, head + d, lin[:, d * HEAD_DIM:(d + 1) * HEAD_DIM], cos_t, sin_t)
    if near:
        for part in range(tok // block):
            gather_rows(chips - 1, part)
            at = slice(part * block, (part + 1) * block)
            far_ref[at, :] = acc_ref[...].astype(BF16)
            far_mask_ref[at, :] = jnp.broadcast_to(any_ref[:, :1], (block, 128)).astype(BF16)


def qkv(info, pieces, extra, cos_t, sin_t, norm, w_q, b_q, w_k, b_k, w_v, b_v, width, tok, near):
    hid = w_q.shape[0]
    chips = cos_t.shape[0]
    n = len(pieces)
    flat = [a for p in pieces for a in p]
    counts = tuple(len(p) for p in pieces)
    vm = pl.BlockSpec(memory_space=pltpu.VMEM)
    anyspec = pl.BlockSpec(memory_space=pl.ANY)
    out_shape = [jax.ShapeDtypeStruct((n, tok, width), BF16)] * 2 + [jax.ShapeDtypeStruct((n, width, tok), BF16)]
    scratch = [
        pltpu.VMEM((2, tok, hid), BF16),
        pltpu.VMEM((2, tok, hid), BF16),
        pltpu.VMEM((hid, 3 * width), BF16),
        pltpu.SemaphoreType.DMA((2, max(counts))),
        pltpu.SemaphoreType.DMA((3,)),
    ]
    if near:
        parts = extra[1:]
        extra_specs = [vm] + [anyspec] * len(parts)
        out_shape += [jax.ShapeDtypeStruct((tok, hid), BF16)] * 2 + [jax.ShapeDtypeStruct((tok, 128), BF16)]
        scratch += [
            pltpu.VMEM((sum(a.shape[0] for a in parts), hid), BF16),
            pltpu.VMEM((256, hid), F32),
            pltpu.VMEM((256, 128), F32),
            pltpu.SemaphoreType.DMA((len(parts),)),
        ]
    else:
        extra_specs = [vm, vm]
    return pl.pallas_call(
        functools.partial(qkv_kernel, near, len(extra) - 1, counts, chips),
        in_specs=[pl.BlockSpec(memory_space=pltpu.SMEM)] + [vm] * 6 + [anyspec] * (3 + len(flat)) + extra_specs,
        out_specs=[vm] * len(out_shape),
        out_shape=out_shape,
        scratch_shapes=scratch,
        compiler_params=params(),
        cost_estimate=cost(2 * n * tok * hid * 3 * width, 2 * hid * 3 * width + 4 * n * tok * hid),
        name="qkv",
    )(info, norm[None], cos_t, sin_t, b_q[None], b_k[None], b_v[None], w_q, w_k, w_v, *flat, *extra)


def attn_kernel(num_docs, chips, head0, info_ref, *refs):
    q_in, k_own_in, k_sib_in, v_own_in, v_sib_in = (refs[2 * g:2 * g + 2] for g in range(5))
    o_ref, q_buf, k_buf, v_buf, sems, m_ref, l_ref, acc_ref = refs[10:]
    head = pl.program_id(0)
    slot = lax.rem(head, 2)
    my_chip, core = info_ref[0], info_ref[1]
    tok = o_ref.shape[1]

    def copies(h, s):
        col = pl.multiple_of((head0 + h) * HEAD_DIM, HEAD_DIM)
        out = []
        lo = 0
        for g in range(2):
            n = q_in[g].shape[0]
            span = pl.ds(lo, n)
            lo += n
            cols = pl.ds(col, HEAD_DIM)
            out.append(pltpu.make_async_copy(q_in[g].at[:, :, cols], q_buf.at[s, span], sems.at[s, 5 * g]))
            out.append(pltpu.make_async_copy(k_own_in[g].at[:, :, cols], k_buf.at[s, 0, span], sems.at[s, 5 * g + 1]))
            out.append(pltpu.make_async_copy(k_sib_in[g].at[:, :, cols], k_buf.at[s, 1, span], sems.at[s, 5 * g + 2]))
            out.append(pltpu.make_async_copy(v_own_in[g].at[:, cols, :], v_buf.at[s, 0, span], sems.at[s, 5 * g + 3]))
            out.append(pltpu.make_async_copy(v_sib_in[g].at[:, cols, :], v_buf.at[s, 1, span], sems.at[s, 5 * g + 4]))
        return out

    @pl.when(head == 0)
    def _():
        for c in copies(0, 0):
            c.start()

    @pl.when(head + 1 < pl.num_programs(0))
    def _():
        for c in copies(head + 1, 1 - slot):
            c.start()

    for c in copies(head, slot):
        c.wait()

    def place_of(chip):
        delta = lax.rem(chip - my_chip + chips, chips)
        return jnp.where(delta == chips // 2, chips - 1, jnp.where(delta == chips - 1, chips - 2, delta))

    def doc_start(pos):
        start = jnp.zeros_like(pos)
        for d in range(1, num_docs):
            cut = info_ref[2 + d]
            start = jnp.where(pos >= cut, cut, start)
        return start

    factor = HEAD_DIM ** -0.5 * LOG2_E
    halves = 2
    half = tok // halves

    def queries(q_chip, carry):
        q_at = place_of(q_chip)
        q_base = tok * (CORES * q_chip + core)
        q = q_buf[slot, q_at]
        q_pos = q_base + lax.broadcasted_iota(jnp.int32, (1, tok), 1)
        starts = doc_start(q_pos)
        lo_start = doc_start(q_base)
        hi_start = doc_start(q_base + tok - 1)

        def block(j, masked, fresh):
            at = place_of(j)
            bases = (tok * (CORES * j + core), tok * (CORES * j + 1 - core))
            ks = [k_buf[slot, b, at] for b in range(2)]
            vs = jnp.concatenate([v_buf[slot, b, at] for b in range(2)], axis=1)
            scores = [[lax.dot_general(k, q[i * half:(i + 1) * half], (((1,), (1,)), ((), ())), preferred_element_type=F32) for k in ks] for i in range(halves)]
            for i in range(halves):
                lanes = slice(i * half, (i + 1) * half)
                pair = scores[i]
                if masked:
                    for b in range(2):
                        k_pos = bases[b] + lax.broadcasted_iota(jnp.int32, pair[b].shape, 0)
                        pair[b] = jnp.where((k_pos <= q_pos[:, lanes]) & (k_pos >= starts[:, lanes]), pair[b], NEG_BIG)
                top = jnp.maximum(jnp.max(pair[0], axis=0, keepdims=True), jnp.max(pair[1], axis=0, keepdims=True))
                if not fresh:
                    old = m_ref[:, lanes]
                    top = jnp.maximum(top, old)
                probs = [jnp.exp2((s - top) * factor) for s in pair]
                total = jnp.sum(probs[0], axis=0, keepdims=True) + jnp.sum(probs[1], axis=0, keepdims=True)
                out = dot32(vs, jnp.concatenate([p.astype(BF16) for p in probs], axis=0))
                if not fresh:
                    alpha = jnp.exp2((old - top) * factor)
                    total = total + l_ref[:, lanes] * alpha
                    out = out + acc_ref[:, lanes] * alpha
                m_ref[:, lanes] = top
                l_ref[:, lanes] = total
                acc_ref[:, lanes] = out

        block(q_chip, True, True)

        def body(t, inner):
            j = q_chip - 1 - t
            clear = tok * CORES * j >= hi_start

            @pl.when(clear)
            def _():
                block(j, False, False)

            @pl.when(jnp.logical_not(clear))
            def _():
                block(j, True, False)

            return inner

        lax.fori_loop(0, q_chip - lo_start // (tok * CORES), body, 0)
        o_ref[q_at] = jnp.transpose(acc_ref[...] / l_ref[...]).astype(BF16)
        return carry

    lax.fori_loop(0, chips, queries, 0)


def attention(info, qs, ks, k_sibs, vs, v_sibs, num_docs, chips, tok, head0, heads):
    grid_spec = pltpu.PrefetchScalarGridSpec(
        num_scalar_prefetch=1,
        grid=(heads,),
        in_specs=[pl.BlockSpec(memory_space=pl.ANY)] * 10,
        out_specs=pl.BlockSpec((chips, tok, HEAD_DIM), lambda h, s: (0, 0, h)),
        scratch_shapes=[
            pltpu.VMEM((2, chips, tok, HEAD_DIM), BF16),
            pltpu.VMEM((2, 2, chips, tok, HEAD_DIM), BF16),
            pltpu.VMEM((2, 2, chips, HEAD_DIM, tok), BF16),
            pltpu.SemaphoreType.DMA((2, 10)),
            pltpu.VMEM((1, tok), F32),
            pltpu.VMEM((1, tok), F32),
            pltpu.VMEM((HEAD_DIM, tok), F32),
        ],
    )
    width = heads * HEAD_DIM
    return pl.pallas_call(
        functools.partial(attn_kernel, num_docs, chips, head0),
        grid_spec=grid_spec,
        out_shape=jax.ShapeDtypeStruct((chips, tok, width), BF16),
        compiler_params=params(),
        cost_estimate=cost(2 * 2 * 20 * tok * tok * width, 2 * 5 * chips * tok * width),
        name="attend",
    )(info, *qs, *ks, *k_sibs, *vs, *v_sibs)


def oproj_kernel(shifts, info_ref, *refs):
    chips = len(shifts)
    n = 2 * chips
    o_refs = refs[:n]
    h_ref, g_ref, w_ref, h1_ref, b_ref, w_bufs, o_bufs, sems = refs[n], refs[n + 1], refs[n + 2], refs[n + 3], refs[n + 4], refs[n + 5:n + 7], refs[n + 7:n + 9], refs[n + 9]
    widths = [o_refs[0].shape[1], o_refs[chips].shape[1]]

    def copies(g, i):
        wide = widths[g]
        src = lax.rem(info_ref[0] + 2 * chips - shifts[i], chips)
        row = pl.multiple_of(src * sum(widths) + g * widths[0], HEAD_DIM)
        return (
            pltpu.make_async_copy(w_ref.at[pl.ds(row, wide), :], w_bufs[g].at[pl.ds(i * wide, wide), :], sems.at[g, i]),
            pltpu.make_async_copy(o_refs[g * chips + i], o_bufs[g].at[:, pl.ds(i * wide, wide)], sems.at[g, chips + i]),
        )

    for g in range(2):
        for i in range(chips):
            for c in copies(g, i):
                c.start()
    parts = []
    for g in range(2):
        for i in range(chips):
            for c in copies(g, i):
                c.wait()
        parts.append(dot32(o_bufs[g][...], w_bufs[g][...]))
    h1 = (h_ref[...].astype(F32) + (parts[0] + parts[1])).astype(BF16)
    h1_ref[...] = h1
    wide = h1.astype(F32)
    b_ref[...] = (wide * lax.rsqrt(jnp.mean(wide * wide, axis=-1, keepdims=True) + NORM_EPS) * g_ref[...].astype(F32)).astype(BF16)


def oproj(info, outs_a, outs_b, shifts, h_zero, norm, w_o):
    tok, hid = h_zero.shape
    wide_a, wide_b = outs_a[0].shape[1], outs_b[0].shape[1]
    chips = len(shifts)
    vm = pl.BlockSpec(memory_space=pltpu.VMEM)
    anyspec = pl.BlockSpec(memory_space=pl.ANY)
    return pl.pallas_call(
        functools.partial(oproj_kernel, shifts),
        in_specs=[pl.BlockSpec(memory_space=pltpu.SMEM)] + [anyspec] * (2 * chips) + [vm] * 2 + [anyspec],
        out_specs=[vm, vm],
        out_shape=[jax.ShapeDtypeStruct((tok, hid), BF16)] * 2,
        scratch_shapes=[
            pltpu.VMEM((chips * wide_a, hid), BF16),
            pltpu.VMEM((chips * wide_b, hid), BF16),
            pltpu.VMEM((tok, chips * wide_a), BF16),
            pltpu.VMEM((tok, chips * wide_b), BF16),
            pltpu.SemaphoreType.DMA((2, 2 * chips)),
        ],
        compiler_params=params(),
        cost_estimate=cost(2 * tok * hid * chips * (wide_a + wide_b), 2 * chips * (wide_a + wide_b) * hid),
        name="oproj",
    )(info, *outs_a, *outs_b, h_zero, norm[None], w_o)


def mlp_kernel(h_ref, b_ref, wg_ref, wu_ref, wd_ref, out_ref, acc_ref):
    step = pl.program_id(0)

    @pl.when(step == 0)
    def _():
        acc_ref[...] = h_ref[...].astype(F32)

    b = b_ref[...]
    gate = dot32(b, wg_ref[...])
    up = dot32(b, wu_ref[...])
    act = (jax.nn.silu(gate) * up).astype(BF16)
    acc_ref[...] += dot32(act, wd_ref[...])

    @pl.when(step == pl.num_programs(0) - 1)
    def _():
        out_ref[...] = acc_ref[...].astype(BF16)


def mlp(h_one, normed, w_gate, w_up, w_down):
    tok, hid = h_one.shape
    ffn = w_gate.shape[1]
    tile = 768
    whole = lambda i: (0, 0)
    return pl.pallas_call(
        mlp_kernel,
        grid=(ffn // tile,),
        in_specs=[
            pl.BlockSpec((tok, hid), whole),
            pl.BlockSpec((tok, hid), whole),
            pl.BlockSpec((hid, tile), lambda i: (0, i)),
            pl.BlockSpec((hid, tile), lambda i: (0, i)),
            pl.BlockSpec((tile, hid), lambda i: (i, 0)),
        ],
        out_specs=pl.BlockSpec((tok, hid), whole),
        out_shape=jax.ShapeDtypeStruct((tok, hid), BF16),
        scratch_shapes=[pltpu.VMEM((tok, hid), F32)],
        compiler_params=params(),
        cost_estimate=cost(6 * tok * hid * ffn, 6 * hid * ffn),
        name="mlp",
    )(h_one, normed, w_gate, w_up, w_down)


def rope_tables(rope_pos):
    half = HEAD_DIM // 2
    inv_freq = ROPE_THETA ** (-jnp.arange(0, HEAD_DIM, 2, dtype=F32) / HEAD_DIM)
    idx = jnp.arange(half)
    lo, hi = MROPE_SPLIT
    chosen = jnp.where(idx < lo, rope_pos[:, 0, :, None], jnp.where(idx < hi, rope_pos[:, 1, :, None], rope_pos[:, 2, :, None]))
    angles = chosen.astype(F32) * inv_freq
    cos_h, sin_h = jnp.cos(angles), jnp.sin(angles)
    return jnp.concatenate([cos_h, cos_h], axis=-1), jnp.concatenate([-sin_h, sin_h], axis=-1)


def solution(mesh):
    group = mesh.shape['sp']
    chips = group // CORES
    row_spec = P(('dp', 'sp'), None)
    sibling = [(i, CORES * (i // CORES) + (i + 1) % CORES) for i in range(group)]

    def hop(x, steps):
        return lax.ppermute(x, 'sp', [(i, (i + CORES * steps) % group) for i in range(group)])

    def swap(x):
        return lax.ppermute(x, 'sp', sibling)

    def step(patches, embeds, dest_slot, rope_pos, cu_doc, ln_w, ln_b, w_one, b_one, w_two, b_two, norm_attn, w_q, b_q, w_k, b_k, w_v, b_v, w_o, norm_mlp, w_gate, w_up, w_down):
        tok, _ = embeds.shape
        merged_dev = dest_slot.shape[0]
        num_docs = cu_doc.shape[0] - 1
        me = lax.axis_index('sp')
        chip, core = me // CORES, me % CORES
        width = w_q.shape[1] // chips
        half_m = merged_dev // 2
        half_t = tok // 2
        info = jnp.stack([chip, core]).astype(jnp.int32)

        e_prev = hop(embeds, 1)
        e_next = hop(embeds, -1)
        merged = merger(patches, ln_w, ln_b, w_one, b_one, w_two, b_two)
        m_prev = hop(merged, 1)
        m_next = hop(merged, -1)
        m_far_lo = hop(m_prev[:half_m], 1)
        m_far_hi = hop(m_next[half_m:], -1)
        mine = [merged, m_next, m_prev, m_far_lo, m_far_hi]
        theirs = [swap(m) for m in mine]
        e_far_lo = hop(e_prev[:half_t], 1)
        e_far_hi = hop(e_next[half_t:], -1)

        ints = jnp.concatenate([rope_pos, jnp.pad(dest_slot, (0, tok - merged_dev))[None]], axis=0)
        around = jnp.stack([ints, hop(ints, -1), hop(ints, 1), hop(ints, chips // 2)])
        slots_own = around[:, 3, :merged_dev]
        slots_sib = swap(slots_own)
        cos_t, sin_t = rope_tables(around[:, :3])
        slots = jnp.concatenate([slots_own, slots_sib], axis=0)
        shard_chip = (chip + jnp.array([0, 1, chips - 1, chips // 2], jnp.int32)) % chips
        base = tok * (CORES * shard_chip + core)
        starts = (base[:, None] + jnp.arange(0, tok, 256, dtype=jnp.int32)[None, :]).reshape(-1, 1, 1)
        counts = jnp.sum((slots[None] >= starts) & (slots[None] < starts + 256), axis=-1, dtype=jnp.int32)
        qkv_info = jnp.concatenate([info, counts.reshape(-1)])
        common = (cos_t, sin_t, norm_attn, w_q, b_q, w_k, b_k, w_v, b_v, width, tok)
        q_n, k_n, v_n, h_zero, far_rows, far_mask = qkv(qkv_info, [[embeds], [e_next], [e_prev]], [slots] + mine + theirs, *common, True)
        k_sib_n, v_sib_n = swap(k_n), swap(v_n)
        q_f, k_f, v_f = qkv(info, [[e_far_lo, e_far_hi]], [far_rows, far_mask], *common, False)
        k_sibs = [k_sib_n, swap(k_f)]
        v_sibs = [v_sib_n, swap(v_f)]

        att_info = jnp.concatenate([info, cu_doc]).astype(jnp.int32)
        heads = width // HEAD_DIM
        split = (heads + 1) // 2
        shifts = (0, 1, -1, chips // 2)
        parts = []
        for head0, n in ((0, split), (split, heads - split)):
            o = attention(att_info, (q_n, q_f), (k_n, k_f), k_sibs, (v_n, v_f), v_sibs, num_docs, chips, tok, head0, n)
            parts.append([o[0]] + [hop(o[i], shifts[i]) for i in range(1, chips)])
        h_one, normed = oproj(info, parts[0], parts[1], shifts, h_zero, norm_mlp, w_o)
        return mlp(h_one, normed, w_gate, w_up, w_down)

    in_specs = (row_spec, row_spec, P(('dp', 'sp')), P(None, ('dp', 'sp')), P('dp')) + (P(),) * 18
    return jax.shard_map(step, mesh=mesh, in_specs=in_specs, out_specs=row_spec, check_vma=False)
```

```python
import functools

import jax
import jax.numpy as jnp
from jax import lax
from jax.experimental import pallas as pl
from jax.experimental.pallas import tpu as pltpu
from jax.sharding import PartitionSpec as P


HEAD_DIM = 128
NORM_EPS = 1e-6
ROPE_THETA = 1000000.0
MROPE_SPLIT = (16, 40)
CORES = 2
NEG_BIG = -1e30
LOG2_E = 1.4426950408889634
F32 = jnp.float32
BF16 = jnp.bfloat16
VMEM_LIMIT = 60 * 1024 * 1024


def cost(flops, nbytes, trans=0):
    return pl.CostEstimate(flops=int(flops), bytes_accessed=int(nbytes), transcendentals=int(trans))


def params(limit=VMEM_LIMIT):
    return pltpu.CompilerParams(vmem_limit_bytes=limit)


def dot32(lhs, rhs):
    return jnp.dot(lhs, rhs, preferred_element_type=F32)


def merger_kernel(x_ref, lnw_ref, lnb_ref, w1_ref, b1_ref, w2_ref, b2_ref, out_ref, wide_ref, z_ref, acc_ref):
    step = pl.program_id(0)
    rows, feat = out_ref.shape[0], x_ref.shape[1]

    @pl.when(step == 0)
    def _():
        x = x_ref[...].astype(F32)
        cent = x - jnp.mean(x, axis=-1, keepdims=True)
        var = jnp.mean(cent * cent, axis=-1, keepdims=True)
        normed = cent * lax.rsqrt(var + NORM_EPS) * lnw_ref[...].astype(F32) + lnb_ref[...].astype(F32)
        for j in range(feat // 128):
            wide_ref[j] = normed[:, j * 128:(j + 1) * 128]
        for i in range(4):
            for j in range(feat // 128):
                col = i * feat + j * 128
                z_ref[:, col:col + 128] = wide_ref[j, pl.ds(i, rows, stride=4), :].astype(BF16)
        acc_ref[...] = jnp.zeros_like(acc_ref)

    pre = dot32(z_ref[...], w1_ref[...]) + b1_ref[...].astype(F32)
    inner = (0.5 * pre * (1.0 + lax.erf(pre * 2.0 ** -0.5))).astype(BF16)
    acc_ref[...] += dot32(inner, w2_ref[...])

    @pl.when(step == pl.num_programs(0) - 1)
    def _():
        out_ref[...] = (acc_ref[...] + b2_ref[...].astype(F32)).astype(BF16)


def merger(patches, ln_w, ln_b, w_one, b_one, w_two, b_two):
    total, feat = patches.shape
    rows = total // 4
    depth, mid = w_one.shape
    hid = w_two.shape[1]
    tile = 512
    whole = lambda i: (0, 0)
    return pl.pallas_call(
        merger_kernel,
        grid=(mid // tile,),
        in_specs=[
            pl.BlockSpec((total, feat), whole),
            pl.BlockSpec((1, feat), whole),
            pl.BlockSpec((1, feat), whole),
            pl.BlockSpec((depth, tile), lambda i: (0, i)),
            pl.BlockSpec((1, tile), lambda i: (0, i)),
            pl.BlockSpec((tile, hid), lambda i: (i, 0)),
            pl.BlockSpec((1, hid), whole),
        ],
        out_specs=pl.BlockSpec((rows, hid), whole),
        out_shape=jax.ShapeDtypeStruct((rows, hid), BF16),
        scratch_shapes=[
            pltpu.VMEM((feat // 128, total, 128), F32),
            pltpu.VMEM((rows, depth), BF16),
            pltpu.VMEM((rows, hid), F32),
        ],
        compiler_params=params(),
        cost_estimate=cost(2 * rows * mid * (depth + hid), 2 * mid * (depth + hid)),
        name="merger",
    )(patches, ln_w[None], ln_b[None], w_one, b_one[None], w_two, b_two[None])


def qkv_kernel(near, n_parts, e_counts, chips, info_ref, *refs):
    g_ref, cos_ref, sin_ref, bq_ref, bk_ref, bv_ref, wq_ref, wk_ref, wv_ref = refs[:9]
    n = len(e_counts)
    pos = 9
    e_refs = refs[pos:pos + sum(e_counts)]
    pos += len(e_refs)
    if near:
        slots_ref = refs[pos]
        m_refs = refs[pos + 1:pos + 1 + n_parts]
        pos += 1 + n_parts
        q_ref, k_ref, v_ref, h_ref, far_ref, far_mask_ref, e_buf, a_buf, w_buf, e_sems, w_sems, m_buf, acc_ref, any_ref, m_sems = refs[pos:]
    else:
        far_ref, far_mask_ref = refs[pos:pos + 2]
        q_ref, k_ref, v_ref, e_buf, a_buf, w_buf, e_sems, w_sems = refs[pos + 2:]
    first = 0 if near else chips - 1
    width = w_buf.shape[1] // 3
    heads = width // HEAD_DIM
    col = pl.multiple_of(info_ref[0] * width, width)
    tok, _ = a_buf.shape[1:]
    block = 256
    w_refs = (wq_ref, wk_ref, wv_ref)

    def load_weight(i):
        return pltpu.make_async_copy(w_refs[i].at[:, pl.ds(col, width)], w_buf.at[:, pl.ds(i * width, width)], w_sems.at[i])

    def loads(i):
        at = sum(e_counts[:i])
        row = 0
        out = []
        for j in range(e_counts[i]):
            rows = e_refs[at + j].shape[0]
            out.append(pltpu.make_async_copy(e_refs[at + j], e_buf.at[i % 2, pl.ds(row, rows), :], e_sems.at[i % 2, j]))
            row += rows
        return out

    if near:
        m_copies = []
        row = 0
        for j, m in enumerate(m_refs):
            m_copies.append(pltpu.make_async_copy(m, m_buf.at[pl.ds(row, m.shape[0]), :], m_sems.at[j]))
            row += m.shape[0]
        for c in m_copies:
            c.start()
    for c in loads(0):
        c.start()
    for i in range(3):
        load_weight(i).start()
    if near:
        for c in m_copies:
            c.wait()

    def gather_rows(shard, part):
        blocks = m_buf.shape[0] // block
        delta = chips // 2 if shard == chips - 1 else chips - 1 if shard == chips - 2 else shard
        chip = lax.rem(info_ref[0] + delta, chips)
        base = tok * (CORES * chip + info_ref[1]) + block * part
        acc_ref[...] = jnp.zeros_like(acc_ref)
        any_ref[...] = jnp.zeros_like(any_ref)

        def visit(j, carry):
            @pl.when(info_ref[2 + (shard * (tok // block) + part) * blocks + j] > 0)
            def _():
                token = base + lax.broadcasted_iota(jnp.int32, (block, block), 0)
                hit = (slots_ref[pl.ds(j, 1), :] == token).astype(F32)
                at = pl.ds(pl.multiple_of(j * block, block), block)
                acc_ref[...] += dot32(hit.astype(BF16), m_buf[at, :])
                any_ref[...] = jnp.maximum(any_ref[...], jnp.max(hit, axis=1, keepdims=True))

            return carry

        lax.fori_loop(0, blocks, visit, 0)

    chunk = 32

    def place_rows(i):
        for c in loads(i):
            c.wait()
        for part in range(tok // block):
            if near:
                gather_rows(i, part)
            for r in range(0, block, chunk):
                at = slice(part * block + r, part * block + r + chunk)
                if near:
                    hit, rows = any_ref[r:r + chunk, :1] > 0.5, acc_ref[r:r + chunk, :]
                else:
                    hit, rows = far_mask_ref[at, :1].astype(F32) > 0.5, far_ref[at, :].astype(F32)
                e_buf[i % 2, at, :] = jnp.where(hit, rows, e_buf[i % 2, at, :].astype(F32)).astype(BF16)
        if near and i == 0:
            h_ref[...] = e_buf[0]

    def norm_rows(i):
        for r in range(0, tok, chunk):
            h = e_buf[i % 2, r:r + chunk, :].astype(F32)
            scale = lax.rsqrt(jnp.mean(h * h, axis=-1, keepdims=True) + NORM_EPS)
            a_buf[i % 2, r:r + chunk, :] = (h * scale * g_ref[...].astype(F32)).astype(BF16)

    def emit(i, head, part, cos_t, sin_t):
        kind, h = divmod(head, heads)
        cols = slice(h * HEAD_DIM, (h + 1) * HEAD_DIM)
        bias = (bq_ref, bk_ref, bv_ref)[kind][:, pl.ds(pl.multiple_of(col + h * HEAD_DIM, HEAD_DIM), HEAD_DIM)]
        part = part + bias.astype(F32)
        if kind < 2:
            (q_ref, k_ref)[kind][i, :, cols] = (part * cos_t + pltpu.roll(part, HEAD_DIM // 2, 1) * sin_t).astype(BF16)
        else:
            v_ref[i, cols, :] = jnp.transpose(part).astype(BF16)

    place_rows(0)
    norm_rows(0)
    for i in range(n):
        if i + 1 < n:
            for c in loads(i + 1):
                c.start()
            place_rows(i + 1)
            norm_rows(i + 1)
        if i == 0:
            for j in range(3):
                load_weight(j).wait()
        a = a_buf[i % 2]
        cos_t, sin_t = cos_ref[first + i], sin_ref[first + i]
        for head in range(0, 3 * heads, 2):
            span = min(2, 3 * heads - head)
            lin = dot32(a, w_buf[:, head * HEAD_DIM:(head + span) * HEAD_DIM])
            for d in range(span):
                emit(i, head + d, lin[:, d * HEAD_DIM:(d + 1) * HEAD_DIM], cos_t, sin_t)
    if near:
        for part in range(tok // block):
            gather_rows(chips - 1, part)
            at = slice(part * block, (part + 1) * block)
            far_ref[at, :] = acc_ref[...].astype(BF16)
            far_mask_ref[at, :] = jnp.broadcast_to(any_ref[:, :1], (block, 128)).astype(BF16)


def qkv(info, pieces, extra, cos_t, sin_t, norm, w_q, b_q, w_k, b_k, w_v, b_v, width, tok, near):
    hid = w_q.shape[0]
    chips = cos_t.shape[0]
    n = len(pieces)
    flat = [a for p in pieces for a in p]
    counts = tuple(len(p) for p in pieces)
    vm = pl.BlockSpec(memory_space=pltpu.VMEM)
    anyspec = pl.BlockSpec(memory_space=pl.ANY)
    out_shape = [jax.ShapeDtypeStruct((n, tok, width), BF16)] * 2 + [jax.ShapeDtypeStruct((n, width, tok), BF16)]
    scratch = [
        pltpu.VMEM((2, tok, hid), BF16),
        pltpu.VMEM((2, tok, hid), BF16),
        pltpu.VMEM((hid, 3 * width), BF16),
        pltpu.SemaphoreType.DMA((2, max(counts))),
        pltpu.SemaphoreType.DMA((3,)),
    ]
    if near:
        parts = extra[1:]
        extra_specs = [vm] + [anyspec] * len(parts)
        out_shape += [jax.ShapeDtypeStruct((tok, hid), BF16)] * 2 + [jax.ShapeDtypeStruct((tok, 128), BF16)]
        scratch += [
            pltpu.VMEM((sum(a.shape[0] for a in parts), hid), BF16),
            pltpu.VMEM((256, hid), F32),
            pltpu.VMEM((256, 128), F32),
            pltpu.SemaphoreType.DMA((len(parts),)),
        ]
    else:
        extra_specs = [vm, vm]
    return pl.pallas_call(
        functools.partial(qkv_kernel, near, len(extra) - 1, counts, chips),
        in_specs=[pl.BlockSpec(memory_space=pltpu.SMEM)] + [vm] * 6 + [anyspec] * (3 + len(flat)) + extra_specs,
        out_specs=[vm] * len(out_shape),
        out_shape=out_shape,
        scratch_shapes=scratch,
        compiler_params=params(),
        cost_estimate=cost(2 * n * tok * hid * 3 * width, 2 * hid * 3 * width + 4 * n * tok * hid),
        name="qkv",
    )(info, norm[None], cos_t, sin_t, b_q[None], b_k[None], b_v[None], w_q, w_k, w_v, *flat, *extra)


def attn_kernel(num_docs, chips, head0, info_ref, *refs):
    q_in, k_own_in, k_sib_in, v_own_in, v_sib_in = (refs[2 * g:2 * g + 2] for g in range(5))
    o_ref, q_buf, k_buf, v_buf, sems, m_ref, l_ref, acc_ref = refs[10:]
    head = pl.program_id(0)
    slot = lax.rem(head, 2)
    my_chip, core = info_ref[0], info_ref[1]
    tok = o_ref.shape[1]

    def copies(h, s):
        col = pl.multiple_of((head0 + h) * HEAD_DIM, HEAD_DIM)
        out = []
        lo = 0
        for g in range(2):
            n = q_in[g].shape[0]
            span = pl.ds(lo, n)
            lo += n
            cols = pl.ds(col, HEAD_DIM)
            out.append(pltpu.make_async_copy(q_in[g].at[:, :, cols], q_buf.at[s, span], sems.at[s, 5 * g]))
            out.append(pltpu.make_async_copy(k_own_in[g].at[:, :, cols], k_buf.at[s, 0, span], sems.at[s, 5 * g + 1]))
            out.append(pltpu.make_async_copy(k_sib_in[g].at[:, :, cols], k_buf.at[s, 1, span], sems.at[s, 5 * g + 2]))
            out.append(pltpu.make_async_copy(v_own_in[g].at[:, cols, :], v_buf.at[s, 0, span], sems.at[s, 5 * g + 3]))
            out.append(pltpu.make_async_copy(v_sib_in[g].at[:, cols, :], v_buf.at[s, 1, span], sems.at[s, 5 * g + 4]))
        return out

    @pl.when(head == 0)
    def _():
        for c in copies(0, 0):
            c.start()

    @pl.when(head + 1 < pl.num_programs(0))
    def _():
        for c in copies(head + 1, 1 - slot):
            c.start()

    for c in copies(head, slot):
        c.wait()

    def place_of(chip):
        delta = lax.rem(chip - my_chip + chips, chips)
        return jnp.where(delta == chips // 2, chips - 1, jnp.where(delta == chips - 1, chips - 2, delta))

    def doc_start(pos):
        start = jnp.zeros_like(pos)
        for d in range(1, num_docs):
            cut = info_ref[2 + d]
            start = jnp.where(pos >= cut, cut, start)
        return start

    factor = HEAD_DIM ** -0.5 * LOG2_E
    halves = 2
    half = tok // halves

    def queries(q_chip, carry):
        q_at = place_of(q_chip)
        q_base = tok * (CORES * q_chip + core)
        q = q_buf[slot, q_at]
        q_pos = q_base + lax.broadcasted_iota(jnp.int32, (1, tok), 1)
        starts = doc_start(q_pos)
        lo_start = doc_start(q_base)
        hi_start = doc_start(q_base + tok - 1)

        def block(j, masked, fresh):
            at = place_of(j)
            bases = (tok * (CORES * j + core), tok * (CORES * j + 1 - core))
            ks = [k_buf[slot, b, at] for b in range(2)]
            vs = jnp.concatenate([v_buf[slot, b, at] for b in range(2)], axis=1)
            scores = [[lax.dot_general(k, q[i * half:(i + 1) * half], (((1,), (1,)), ((), ())), preferred_element_type=F32) for k in ks] for i in range(halves)]
            for i in range(halves):
                lanes = slice(i * half, (i + 1) * half)
                pair = scores[i]
                if masked:
                    for b in range(2):
                        k_pos = bases[b] + lax.broadcasted_iota(jnp.int32, pair[b].shape, 0)
                        pair[b] = jnp.where((k_pos <= q_pos[:, lanes]) & (k_pos >= starts[:, lanes]), pair[b], NEG_BIG)
                top = jnp.maximum(jnp.max(pair[0], axis=0, keepdims=True), jnp.max(pair[1], axis=0, keepdims=True))
                if not fresh:
                    old = m_ref[:, lanes]
                    top = jnp.maximum(top, old)
                probs = [jnp.exp2((s - top) * factor) for s in pair]
                total = jnp.sum(probs[0], axis=0, keepdims=True) + jnp.sum(probs[1], axis=0, keepdims=True)
                out = dot32(vs, jnp.concatenate([p.astype(BF16) for p in probs], axis=0))
                if not fresh:
                    alpha = jnp.exp2((old - top) * factor)
                    total = total + l_ref[:, lanes] * alpha
                    out = out + acc_ref[:, lanes] * alpha
                m_ref[:, lanes] = top
                l_ref[:, lanes] = total
                acc_ref[:, lanes] = out

        block(q_chip, True, True)

        def body(t, inner):
            j = q_chip - 1 - t
            clear = tok * CORES * j >= hi_start

            @pl.when(clear)
            def _():
                block(j, False, False)

            @pl.when(jnp.logical_not(clear))
            def _():
                block(j, True, False)

            return inner

        lax.fori_loop(0, q_chip - lo_start // (tok * CORES), body, 0)
        o_ref[q_at] = jnp.transpose(acc_ref[...] / l_ref[...]).astype(BF16)
        return carry

    lax.fori_loop(0, chips, queries, 0)


def attention(info, qs, ks, k_sibs, vs, v_sibs, num_docs, chips, tok, head0, heads):
    grid_spec = pltpu.PrefetchScalarGridSpec(
        num_scalar_prefetch=1,
        grid=(heads,),
        in_specs=[pl.BlockSpec(memory_space=pl.ANY)] * 10,
        out_specs=pl.BlockSpec((chips, tok, HEAD_DIM), lambda h, s: (0, 0, h)),
        scratch_shapes=[
            pltpu.VMEM((2, chips, tok, HEAD_DIM), BF16),
            pltpu.VMEM((2, 2, chips, tok, HEAD_DIM), BF16),
            pltpu.VMEM((2, 2, chips, HEAD_DIM, tok), BF16),
            pltpu.SemaphoreType.DMA((2, 10)),
            pltpu.VMEM((1, tok), F32),
            pltpu.VMEM((1, tok), F32),
            pltpu.VMEM((HEAD_DIM, tok), F32),
        ],
    )
    width = heads * HEAD_DIM
    return pl.pallas_call(
        functools.partial(attn_kernel, num_docs, chips, head0),
        grid_spec=grid_spec,
        out_shape=jax.ShapeDtypeStruct((chips, tok, width), BF16),
        compiler_params=params(),
        cost_estimate=cost(2 * 2 * 20 * tok * tok * width, 2 * 5 * chips * tok * width),
        name="attend",
    )(info, *qs, *ks, *k_sibs, *vs, *v_sibs)


def tail_kernel(shifts, tile, info_ref, *refs):
    chips = len(shifts)
    n = 2 * chips
    o_refs = refs[:n]
    h_ref, g_ref, wo_ref, wg_ref, wu_ref, wd_ref, out_ref = refs[n:n + 7]
    wo_bufs, o_bufs = refs[n + 7:n + 9], refs[n + 9:n + 11]
    wg_buf, wu_buf, wd_buf, act_buf, b_buf, acc_ref, o_sems, g_sems, u_sems, d_sems = refs[n + 11:]
    widths = [o_refs[0].shape[1], o_refs[chips].shape[1]]
    tok = acc_ref.shape[0]
    tiles = wg_ref.shape[1] // tile

    def o_copies(g, i):
        wide = widths[g]
        src = lax.rem(info_ref[0] + 2 * chips - shifts[i], chips)
        row = pl.multiple_of(src * sum(widths) + g * widths[0], HEAD_DIM)
        return (
            pltpu.make_async_copy(wo_ref.at[pl.ds(row, wide), :], wo_bufs[g].at[pl.ds(i * wide, wide), :], o_sems.at[g, i]),
            pltpu.make_async_copy(o_refs[g * chips + i], o_bufs[g].at[:, pl.ds(i * wide, wide)], o_sems.at[g, chips + i]),
        )

    def span(i):
        return pl.ds(pl.multiple_of(i * tile, tile), tile)

    def gate_copy(i, s):
        return pltpu.make_async_copy(wg_ref.at[:, span(i)], wg_buf.at[s], g_sems.at[s])

    def up_copy(i, s):
        return pltpu.make_async_copy(wu_ref.at[:, span(i)], wu_buf.at[s], u_sems.at[s])

    def down_copy(i, s):
        return pltpu.make_async_copy(wd_ref.at[span(i), :], wd_buf.at[s], d_sems.at[s])

    for g in range(2):
        for i in range(chips):
            for c in o_copies(g, i):
                c.start()
    for s in range(2):
        gate_copy(s, s).start()
        up_copy(s, s).start()
    down_copy(0, 0).start()

    for g in range(2):
        for i in range(chips):
            for c in o_copies(g, i):
                c.wait()
        part = dot32(o_bufs[g][...], wo_bufs[g][...])
        acc_ref[...] = part if g == 0 else acc_ref[...] + part
    chunk = 32
    for r in range(0, tok, chunk):
        h1 = (h_ref[r:r + chunk, :].astype(F32) + acc_ref[r:r + chunk, :]).astype(BF16).astype(F32)
        acc_ref[r:r + chunk, :] = h1
        scale = lax.rsqrt(jnp.mean(h1 * h1, axis=-1, keepdims=True) + NORM_EPS)
        b_buf[r:r + chunk, :] = (h1 * scale * g_ref[...].astype(F32)).astype(BF16)

    def front(s):
        b = b_buf[...]
        return (jax.nn.silu(dot32(b, wg_buf[s])) * dot32(b, wu_buf[s])).astype(BF16)

    gate_copy(0, 0).wait()
    up_copy(0, 0).wait()
    act_buf[...] = front(0)
    down_copy(1, 1).start()

    def body(i, carry):
        s = lax.rem(i, 2)
        p = 1 - s

        @pl.when(i + 1 < tiles)
        def _():
            gate_copy(i + 1, p).start()
            up_copy(i + 1, p).start()

        gate_copy(i, s).wait()
        up_copy(i, s).wait()
        down_copy(i - 1, p).wait()
        before = act_buf[...]
        act_buf[...] = front(s)
        acc_ref[...] += dot32(before, wd_buf[p])

        @pl.when(i + 1 < tiles)
        def _():
            down_copy(i + 1, p).start()

        return carry

    def first_body():
        gate_copy(1, 1).wait()
        up_copy(1, 1).wait()
        down_copy(0, 0).wait()
        gate_copy(2, 0).start()
        up_copy(2, 0).start()
        before = act_buf[...]
        act_buf[...] = front(1)
        acc_ref[...] += dot32(before, wd_buf[0])
        down_copy(2, 0).start()

    first_body()
    lax.fori_loop(2, tiles, body, 0)
    last = (tiles - 1) % 2
    down_copy(tiles - 1, last).wait()
    out_ref[...] = (acc_ref[...] + dot32(act_buf[...], wd_buf[last])).astype(BF16)


def tail(info, outs_a, outs_b, shifts, h_zero, norm, w_o, w_gate, w_up, w_down):
    tok, hid = h_zero.shape
    ffn = w_gate.shape[1]
    tile = 768
    wide_a, wide_b = outs_a[0].shape[1], outs_b[0].shape[1]
    chips = len(shifts)
    vm = pl.BlockSpec(memory_space=pltpu.VMEM)
    anyspec = pl.BlockSpec(memory_space=pl.ANY)
    return pl.pallas_call(
        functools.partial(tail_kernel, shifts, tile),
        in_specs=[pl.BlockSpec(memory_space=pltpu.SMEM)] + [anyspec] * (2 * chips) + [vm] * 2 + [anyspec] * 4,
        out_specs=vm,
        out_shape=jax.ShapeDtypeStruct((tok, hid), BF16),
        scratch_shapes=[
            pltpu.VMEM((chips * wide_a, hid), BF16),
            pltpu.VMEM((chips * wide_b, hid), BF16),
            pltpu.VMEM((tok, chips * wide_a), BF16),
            pltpu.VMEM((tok, chips * wide_b), BF16),
            pltpu.VMEM((2, hid, tile), BF16),
            pltpu.VMEM((2, hid, tile), BF16),
            pltpu.VMEM((2, tile, hid), BF16),
            pltpu.VMEM((tok, tile), BF16),
            pltpu.VMEM((tok, hid), BF16),
            pltpu.VMEM((tok, hid), F32),
            pltpu.SemaphoreType.DMA((2, 2 * chips)),
            pltpu.SemaphoreType.DMA((2,)),
            pltpu.SemaphoreType.DMA((2,)),
            pltpu.SemaphoreType.DMA((2,)),
        ],
        compiler_params=params(67043328),
        cost_estimate=cost(2 * tok * hid * (hid + 3 * ffn), 2 * hid * (hid + 3 * ffn)),
        name="tail",
    )(info, *outs_a, *outs_b, h_zero, norm[None], w_o, w_gate, w_up, w_down)


def rope_tables(rope_pos):
    half = HEAD_DIM // 2
    inv_freq = ROPE_THETA ** (-jnp.arange(0, HEAD_DIM, 2, dtype=F32) / HEAD_DIM)
    idx = jnp.arange(half)
    lo, hi = MROPE_SPLIT
    chosen = jnp.where(idx < lo, rope_pos[:, 0, :, None], jnp.where(idx < hi, rope_pos[:, 1, :, None], rope_pos[:, 2, :, None]))
    angles = chosen.astype(F32) * inv_freq
    cos_h, sin_h = jnp.cos(angles), jnp.sin(angles)
    return jnp.concatenate([cos_h, cos_h], axis=-1), jnp.concatenate([-sin_h, sin_h], axis=-1)


def solution(mesh):
    group = mesh.shape['sp']
    chips = group // CORES
    row_spec = P(('dp', 'sp'), None)
    sibling = [(i, CORES * (i // CORES) + (i + 1) % CORES) for i in range(group)]

    def hop(x, steps):
        return lax.ppermute(x, 'sp', [(i, (i + CORES * steps) % group) for i in range(group)])

    def swap(x):
        return lax.ppermute(x, 'sp', sibling)

    def step(patches, embeds, dest_slot, rope_pos, cu_doc, ln_w, ln_b, w_one, b_one, w_two, b_two, norm_attn, w_q, b_q, w_k, b_k, w_v, b_v, w_o, norm_mlp, w_gate, w_up, w_down):
        tok, _ = embeds.shape
        merged_dev = dest_slot.shape[0]
        num_docs = cu_doc.shape[0] - 1
        me = lax.axis_index('sp')
        chip, core = me // CORES, me % CORES
        width = w_q.shape[1] // chips
        half_m = merged_dev // 2
        half_t = tok // 2
        info = jnp.stack([chip, core]).astype(jnp.int32)

        cut = 3 * tok // 4
        e_a, e_b = embeds[:cut], embeds[cut:]
        a_prev = hop(e_a, 1)
        a_next = hop(e_a, -1)
        merged = merger(patches, ln_w, ln_b, w_one, b_one, w_two, b_two)
        m_prev = hop(merged, 1)
        m_next = hop(merged, -1)
        m_far_lo = hop(m_prev[:half_m], 1)
        m_far_hi = hop(m_next[half_m:], -1)
        mine = [merged, m_next, m_prev, m_far_lo, m_far_hi]
        theirs = [swap(m) for m in mine]
        b_prev = hop(e_b, 1)
        b_next = hop(e_b, -1)
        far = [hop(a_prev[:half_t], 1), hop(a_next[half_t:], -1)]
        far.append(hop(b_next, -1))

        ints = jnp.concatenate([rope_pos, jnp.pad(dest_slot, (0, tok - merged_dev))[None]], axis=0)
        around = jnp.stack([ints, hop(ints, -1), hop(ints, 1), hop(ints, chips // 2)])
        slots_own = around[:, 3, :merged_dev]
        slots_sib = swap(slots_own)
        cos_t, sin_t = rope_tables(around[:, :3])
        slots = jnp.concatenate([slots_own, slots_sib], axis=0)
        shard_chip = (chip + jnp.array([0, 1, chips - 1, chips // 2], jnp.int32)) % chips
        base = tok * (CORES * shard_chip + core)
        starts = (base[:, None] + jnp.arange(0, tok, 256, dtype=jnp.int32)[None, :]).reshape(-1, 1, 1)
        counts = jnp.sum((slots[None] >= starts) & (slots[None] < starts + 256), axis=-1, dtype=jnp.int32)
        qkv_info = jnp.concatenate([info, counts.reshape(-1)])
        common = (cos_t, sin_t, norm_attn, w_q, b_q, w_k, b_k, w_v, b_v, width, tok)
        q_n, k_n, v_n, h_zero, far_rows, far_mask = qkv(qkv_info, [[embeds], [a_next, b_next], [a_prev, b_prev]], [slots] + mine + theirs, *common, True)
        k_sib_n, v_sib_n = swap(k_n), swap(v_n)
        q_f, k_f, v_f = qkv(info, [far], [far_rows, far_mask], *common, False)
        k_sibs = [k_sib_n, swap(k_f)]
        v_sibs = [v_sib_n, swap(v_f)]

        att_info = jnp.concatenate([info, cu_doc]).astype(jnp.int32)
        heads = width // HEAD_DIM
        split = (heads + 1) // 2
        shifts = (0, 1, -1, chips // 2)
        parts = []
        for head0, n in ((0, split), (split, heads - split)):
            o = attention(att_info, (q_n, q_f), (k_n, k_f), k_sibs, (v_n, v_f), v_sibs, num_docs, chips, tok, head0, n)
            parts.append([o[0]] + [hop(o[i], shifts[i]) for i in range(1, chips)])
        return tail(info, parts[0], parts[1], shifts, h_zero, norm_mlp, w_o, w_gate, w_up, w_down)

    in_specs = (row_spec, row_spec, P(('dp', 'sp')), P(None, ('dp', 'sp')), P('dp')) + (P(),) * 18
    return jax.shard_map(step, mesh=mesh, in_specs=in_specs, out_specs=row_spec, check_vma=False)
```

```python
import functools

import jax
import jax.numpy as jnp
from jax import lax
from jax.experimental import pallas as pl
from jax.experimental.pallas import tpu as pltpu
from jax.sharding import PartitionSpec as P


HEAD_DIM = 128
NORM_EPS = 1e-6
ROPE_THETA = 1000000.0
MROPE_SPLIT = (16, 40)
CORES = 2
NEG_BIG = -1e30
LOG2_E = 1.4426950408889634
F32 = jnp.float32
BF16 = jnp.bfloat16
VMEM_LIMIT = 60 * 1024 * 1024


def cost(flops, nbytes, trans=0):
    return pl.CostEstimate(flops=int(flops), bytes_accessed=int(nbytes), transcendentals=int(trans))


def params(limit=VMEM_LIMIT):
    return pltpu.CompilerParams(vmem_limit_bytes=limit)


def dot32(lhs, rhs):
    return jnp.dot(lhs, rhs, preferred_element_type=F32)


def merger_kernel(x_ref, lnw_ref, lnb_ref, w1_ref, b1_ref, w2_ref, b2_ref, out_ref, wide_ref, z_ref, acc_ref):
    step = pl.program_id(0)
    rows, feat = out_ref.shape[0], x_ref.shape[1]

    @pl.when(step == 0)
    def _():
        x = x_ref[...].astype(F32)
        cent = x - jnp.mean(x, axis=-1, keepdims=True)
        var = jnp.mean(cent * cent, axis=-1, keepdims=True)
        normed = cent * lax.rsqrt(var + NORM_EPS) * lnw_ref[...].astype(F32) + lnb_ref[...].astype(F32)
        for j in range(feat // 128):
            wide_ref[j] = normed[:, j * 128:(j + 1) * 128]
        for i in range(4):
            for j in range(feat // 128):
                col = i * feat + j * 128
                z_ref[:, col:col + 128] = wide_ref[j, pl.ds(i, rows, stride=4), :].astype(BF16)
        acc_ref[...] = jnp.zeros_like(acc_ref)

    pre = dot32(z_ref[...], w1_ref[...]) + b1_ref[...].astype(F32)
    inner = (0.5 * pre * (1.0 + lax.erf(pre * 2.0 ** -0.5))).astype(BF16)
    acc_ref[...] += dot32(inner, w2_ref[...])

    @pl.when(step == pl.num_programs(0) - 1)
    def _():
        out_ref[...] = (acc_ref[...] + b2_ref[...].astype(F32)).astype(BF16)


def merger(patches, ln_w, ln_b, w_one, b_one, w_two, b_two):
    total, feat = patches.shape
    rows = total // 4
    depth, mid = w_one.shape
    hid = w_two.shape[1]
    tile = 512
    whole = lambda i: (0, 0)
    return pl.pallas_call(
        merger_kernel,
        grid=(mid // tile,),
        in_specs=[
            pl.BlockSpec((total, feat), whole),
            pl.BlockSpec((1, feat), whole),
            pl.BlockSpec((1, feat), whole),
            pl.BlockSpec((depth, tile), lambda i: (0, i)),
            pl.BlockSpec((1, tile), lambda i: (0, i)),
            pl.BlockSpec((tile, hid), lambda i: (i, 0)),
            pl.BlockSpec((1, hid), whole),
        ],
        out_specs=pl.BlockSpec((rows, hid), whole),
        out_shape=jax.ShapeDtypeStruct((rows, hid), BF16),
        scratch_shapes=[
            pltpu.VMEM((feat // 128, total, 128), F32),
            pltpu.VMEM((rows, depth), BF16),
            pltpu.VMEM((rows, hid), F32),
        ],
        compiler_params=params(),
        cost_estimate=cost(2 * rows * mid * (depth + hid), 2 * mid * (depth + hid)),
        name="merger",
    )(patches, ln_w[None], ln_b[None], w_one, b_one[None], w_two, b_two[None])


def qkv_kernel(near, n_parts, e_counts, chips, info_ref, *refs):
    g_ref, cos_ref, sin_ref, bq_ref, bk_ref, bv_ref, wq_ref, wk_ref, wv_ref = refs[:9]
    n = len(e_counts)
    pos = 9
    e_refs = refs[pos:pos + sum(e_counts)]
    pos += len(e_refs)
    if near:
        slots_ref = refs[pos]
        m_refs = refs[pos + 1:pos + 1 + n_parts]
        pos += 1 + n_parts
        q_ref, k_ref, v_ref, h_ref, far_ref, far_mask_ref, e_buf, a_buf, w_buf, e_sems, w_sems, m_buf, acc_ref, any_ref, m_sems = refs[pos:]
    else:
        far_ref, far_mask_ref = refs[pos:pos + 2]
        q_ref, k_ref, v_ref, e_buf, a_buf, w_buf, e_sems, w_sems = refs[pos + 2:]
    first = 0 if near else chips - 1
    width = w_buf.shape[1] // 3
    heads = width // HEAD_DIM
    col = pl.multiple_of(info_ref[0] * width, width)
    tok, _ = a_buf.shape[1:]
    block = 256
    w_refs = (wq_ref, wk_ref, wv_ref)

    def load_weight(i):
        return pltpu.make_async_copy(w_refs[i].at[:, pl.ds(col, width)], w_buf.at[:, pl.ds(i * width, width)], w_sems.at[i])

    def loads(i):
        at = sum(e_counts[:i])
        row = 0
        out = []
        for j in range(e_counts[i]):
            rows = e_refs[at + j].shape[0]
            out.append(pltpu.make_async_copy(e_refs[at + j], e_buf.at[i % 2, pl.ds(row, rows), :], e_sems.at[i % 2, j]))
            row += rows
        return out

    if near:
        m_copies = []
        row = 0
        for j, m in enumerate(m_refs):
            m_copies.append(pltpu.make_async_copy(m, m_buf.at[pl.ds(row, m.shape[0]), :], m_sems.at[j]))
            row += m.shape[0]
        for c in m_copies:
            c.start()
    for c in loads(0):
        c.start()
    for i in range(3):
        load_weight(i).start()
    if near:
        for c in m_copies:
            c.wait()

    def gather_rows(shard, part):
        blocks = m_buf.shape[0] // block
        delta = chips // 2 if shard == chips - 1 else chips - 1 if shard == chips - 2 else shard
        chip = lax.rem(info_ref[0] + delta, chips)
        base = tok * (CORES * chip + info_ref[1]) + block * part
        acc_ref[...] = jnp.zeros_like(acc_ref)
        any_ref[...] = jnp.zeros_like(any_ref)

        def visit(j, carry):
            @pl.when(info_ref[2 + (shard * (tok // block) + part) * blocks + j] > 0)
            def _():
                token = base + lax.broadcasted_iota(jnp.int32, (block, block), 0)
                hit = (slots_ref[pl.ds(j, 1), :] == token).astype(F32)
                at = pl.ds(pl.multiple_of(j * block, block), block)
                acc_ref[...] += dot32(hit.astype(BF16), m_buf[at, :])
                any_ref[...] = jnp.maximum(any_ref[...], jnp.max(hit, axis=1, keepdims=True))

            return carry

        lax.fori_loop(0, blocks, visit, 0)

    chunk = 32

    def place_rows(i):
        for c in loads(i):
            c.wait()
        for part in range(tok // block):
            if near:
                gather_rows(i, part)
            for r in range(0, block, chunk):
                at = slice(part * block + r, part * block + r + chunk)
                if near:
                    hit, rows = any_ref[r:r + chunk, :1] > 0.5, acc_ref[r:r + chunk, :]
                else:
                    hit, rows = far_mask_ref[at, :1].astype(F32) > 0.5, far_ref[at, :].astype(F32)
                e_buf[i % 2, at, :] = jnp.where(hit, rows, e_buf[i % 2, at, :].astype(F32)).astype(BF16)
        if near and i == 0:
            h_ref[...] = e_buf[0]

    def norm_rows(i):
        for r in range(0, tok, chunk):
            h = e_buf[i % 2, r:r + chunk, :].astype(F32)
            scale = lax.rsqrt(jnp.mean(h * h, axis=-1, keepdims=True) + NORM_EPS)
            a_buf[i % 2, r:r + chunk, :] = (h * scale * g_ref[...].astype(F32)).astype(BF16)

    def emit(i, head, part, cos_t, sin_t):
        kind, h = divmod(head, heads)
        cols = slice(h * HEAD_DIM, (h + 1) * HEAD_DIM)
        bias = (bq_ref, bk_ref, bv_ref)[kind][:, pl.ds(pl.multiple_of(col + h * HEAD_DIM, HEAD_DIM), HEAD_DIM)]
        part = part + bias.astype(F32)
        if kind < 2:
            (q_ref, k_ref)[kind][i, :, cols] = (part * cos_t + pltpu.roll(part, HEAD_DIM // 2, 1) * sin_t).astype(BF16)
        else:
            v_ref[i, cols, :] = jnp.transpose(part).astype(BF16)

    place_rows(0)
    norm_rows(0)
    for i in range(n):
        if i + 1 < n:
            for c in loads(i + 1):
                c.start()
            place_rows(i + 1)
            norm_rows(i + 1)
        if i == 0:
            for j in range(3):
                load_weight(j).wait()
        a = a_buf[i % 2]
        cos_t, sin_t = cos_ref[first + i], sin_ref[first + i]
        for head in range(0, 3 * heads, 2):
            span = min(2, 3 * heads - head)
            lin = dot32(a, w_buf[:, head * HEAD_DIM:(head + span) * HEAD_DIM])
            for d in range(span):
                emit(i, head + d, lin[:, d * HEAD_DIM:(d + 1) * HEAD_DIM], cos_t, sin_t)
    if near:
        for part in range(tok // block):
            gather_rows(chips - 1, part)
            at = slice(part * block, (part + 1) * block)
            far_ref[at, :] = acc_ref[...].astype(BF16)
            far_mask_ref[at, :] = jnp.broadcast_to(any_ref[:, :1], (block, 128)).astype(BF16)


def qkv(info, pieces, extra, cos_t, sin_t, norm, w_q, b_q, w_k, b_k, w_v, b_v, width, tok, near):
    hid = w_q.shape[0]
    chips = cos_t.shape[0]
    n = len(pieces)
    flat = [a for p in pieces for a in p]
    counts = tuple(len(p) for p in pieces)
    vm = pl.BlockSpec(memory_space=pltpu.VMEM)
    anyspec = pl.BlockSpec(memory_space=pl.ANY)
    out_shape = [jax.ShapeDtypeStruct((n, tok, width), BF16)] * 2 + [jax.ShapeDtypeStruct((n, width, tok), BF16)]
    scratch = [
        pltpu.VMEM((2, tok, hid), BF16),
        pltpu.VMEM((2, tok, hid), BF16),
        pltpu.VMEM((hid, 3 * width), BF16),
        pltpu.SemaphoreType.DMA((2, max(counts))),
        pltpu.SemaphoreType.DMA((3,)),
    ]
    if near:
        parts = extra[1:]
        extra_specs = [vm] + [anyspec] * len(parts)
        out_shape += [jax.ShapeDtypeStruct((tok, hid), BF16)] * 2 + [jax.ShapeDtypeStruct((tok, 128), BF16)]
        scratch += [
            pltpu.VMEM((sum(a.shape[0] for a in parts), hid), BF16),
            pltpu.VMEM((256, hid), F32),
            pltpu.VMEM((256, 128), F32),
            pltpu.SemaphoreType.DMA((len(parts),)),
        ]
    else:
        extra_specs = [vm, vm]
    return pl.pallas_call(
        functools.partial(qkv_kernel, near, len(extra) - 1, counts, chips),
        in_specs=[pl.BlockSpec(memory_space=pltpu.SMEM)] + [vm] * 6 + [anyspec] * (3 + len(flat)) + extra_specs,
        out_specs=[vm] * len(out_shape),
        out_shape=out_shape,
        scratch_shapes=scratch,
        compiler_params=params(),
        cost_estimate=cost(2 * n * tok * hid * 3 * width, 2 * hid * 3 * width + 4 * n * tok * hid),
        name="qkv",
    )(info, norm[None], cos_t, sin_t, b_q[None], b_k[None], b_v[None], w_q, w_k, w_v, *flat, *extra)


def attn_kernel(num_docs, chips, head0, info_ref, *refs):
    q_in, k_own_in, k_sib_in, v_own_in, v_sib_in = (refs[2 * g:2 * g + 2] for g in range(5))
    o_ref, q_buf, k_buf, v_buf, sems, m_ref, l_ref, acc_ref = refs[10:]
    head = pl.program_id(0)
    slot = lax.rem(head, 2)
    my_chip, core = info_ref[0], info_ref[1]
    tok = o_ref.shape[1]

    def copies(h, s):
        col = pl.multiple_of((head0 + h) * HEAD_DIM, HEAD_DIM)
        out = []
        lo = 0
        for g in range(2):
            n = q_in[g].shape[0]
            span = pl.ds(lo, n)
            lo += n
            cols = pl.ds(col, HEAD_DIM)
            out.append(pltpu.make_async_copy(q_in[g].at[:, :, cols], q_buf.at[s, span], sems.at[s, 5 * g]))
            out.append(pltpu.make_async_copy(k_own_in[g].at[:, :, cols], k_buf.at[s, 0, span], sems.at[s, 5 * g + 1]))
            out.append(pltpu.make_async_copy(k_sib_in[g].at[:, :, cols], k_buf.at[s, 1, span], sems.at[s, 5 * g + 2]))
            out.append(pltpu.make_async_copy(v_own_in[g].at[:, cols, :], v_buf.at[s, 0, span], sems.at[s, 5 * g + 3]))
            out.append(pltpu.make_async_copy(v_sib_in[g].at[:, cols, :], v_buf.at[s, 1, span], sems.at[s, 5 * g + 4]))
        return out

    @pl.when(head == 0)
    def _():
        for c in copies(0, 0):
            c.start()

    @pl.when(head + 1 < pl.num_programs(0))
    def _():
        for c in copies(head + 1, 1 - slot):
            c.start()

    for c in copies(head, slot):
        c.wait()

    def place_of(chip):
        delta = lax.rem(chip - my_chip + chips, chips)
        return jnp.where(delta == chips // 2, chips - 1, jnp.where(delta == chips - 1, chips - 2, delta))

    def doc_start(pos):
        start = jnp.zeros_like(pos)
        for d in range(1, num_docs):
            cut = info_ref[2 + d]
            start = jnp.where(pos >= cut, cut, start)
        return start

    factor = HEAD_DIM ** -0.5 * LOG2_E
    halves = 2
    half = tok // halves

    def queries(q_chip, carry):
        q_at = place_of(q_chip)
        q_base = tok * (CORES * q_chip + core)
        q = q_buf[slot, q_at]
        q_pos = q_base + lax.broadcasted_iota(jnp.int32, (1, tok), 1)
        starts = doc_start(q_pos)
        lo_start = doc_start(q_base)
        hi_start = doc_start(q_base + tok - 1)

        def block(j, masked, fresh):
            at = place_of(j)
            bases = (tok * (CORES * j + core), tok * (CORES * j + 1 - core))
            ks = [k_buf[slot, b, at] for b in range(2)]
            vs = jnp.concatenate([v_buf[slot, b, at] for b in range(2)], axis=1)
            scores = [[lax.dot_general(k, q[i * half:(i + 1) * half], (((1,), (1,)), ((), ())), preferred_element_type=F32) for k in ks] for i in range(halves)]
            for i in range(halves):
                lanes = slice(i * half, (i + 1) * half)
                pair = scores[i]
                if masked:
                    for b in range(2):
                        k_pos = bases[b] + lax.broadcasted_iota(jnp.int32, pair[b].shape, 0)
                        pair[b] = jnp.where((k_pos <= q_pos[:, lanes]) & (k_pos >= starts[:, lanes]), pair[b], NEG_BIG)
                top = jnp.maximum(jnp.max(pair[0], axis=0, keepdims=True), jnp.max(pair[1], axis=0, keepdims=True))
                if not fresh:
                    old = m_ref[:, lanes]
                    top = jnp.maximum(top, old)
                probs = [jnp.exp2((s - top) * factor) for s in pair]
                total = jnp.sum(probs[0], axis=0, keepdims=True) + jnp.sum(probs[1], axis=0, keepdims=True)
                out = dot32(vs, jnp.concatenate([p.astype(BF16) for p in probs], axis=0))
                if not fresh:
                    alpha = jnp.exp2((old - top) * factor)
                    total = total + l_ref[:, lanes] * alpha
                    out = out + acc_ref[:, lanes] * alpha
                m_ref[:, lanes] = top
                l_ref[:, lanes] = total
                acc_ref[:, lanes] = out

        block(q_chip, True, True)

        def body(t, inner):
            j = q_chip - 1 - t
            clear = tok * CORES * j >= hi_start

            @pl.when(clear)
            def _():
                block(j, False, False)

            @pl.when(jnp.logical_not(clear))
            def _():
                block(j, True, False)

            return inner

        lax.fori_loop(0, q_chip - lo_start // (tok * CORES), body, 0)
        o_ref[q_at] = jnp.transpose(acc_ref[...] / l_ref[...]).astype(BF16)
        return carry

    lax.fori_loop(0, chips, queries, 0)


def attention(info, qs, ks, k_sibs, vs, v_sibs, num_docs, chips, tok, head0, heads):
    grid_spec = pltpu.PrefetchScalarGridSpec(
        num_scalar_prefetch=1,
        grid=(heads,),
        in_specs=[pl.BlockSpec(memory_space=pl.ANY)] * 10,
        out_specs=pl.BlockSpec((chips, tok, HEAD_DIM), lambda h, s: (0, 0, h)),
        scratch_shapes=[
            pltpu.VMEM((2, chips, tok, HEAD_DIM), BF16),
            pltpu.VMEM((2, 2, chips, tok, HEAD_DIM), BF16),
            pltpu.VMEM((2, 2, chips, HEAD_DIM, tok), BF16),
            pltpu.SemaphoreType.DMA((2, 10)),
            pltpu.VMEM((1, tok), F32),
            pltpu.VMEM((1, tok), F32),
            pltpu.VMEM((HEAD_DIM, tok), F32),
        ],
    )
    width = heads * HEAD_DIM
    return pl.pallas_call(
        functools.partial(attn_kernel, num_docs, chips, head0),
        grid_spec=grid_spec,
        out_shape=jax.ShapeDtypeStruct((chips, tok, width), BF16),
        compiler_params=params(),
        cost_estimate=cost(2 * 2 * 20 * tok * tok * width, 2 * 5 * chips * tok * width),
        name="attend",
    )(info, *qs, *ks, *k_sibs, *vs, *v_sibs)


def half_oproj_copies(shifts, group, head0, info_ref, w_ref, o_refs, w_buf, o_buf, sems):
    chips = len(shifts)
    wide = o_refs[0].shape[1]
    out = []
    for i in range(chips):
        src = lax.rem(info_ref[0] + 2 * chips - shifts[i], chips)
        row = pl.multiple_of(src * group + head0 * HEAD_DIM, HEAD_DIM)
        out.append(pltpu.make_async_copy(w_ref.at[pl.ds(row, wide), :], w_buf.at[pl.ds(i * wide, wide), :], sems.at[i]))
        out.append(pltpu.make_async_copy(o_refs[i], o_buf.at[:, pl.ds(i * wide, wide)], sems.at[chips + i]))
    return out


def oproj_kernel(shifts, group, info_ref, *refs):
    chips = len(shifts)
    h_ref, w_ref, out_ref, w_buf, o_buf, sems = refs[chips:]
    copies = half_oproj_copies(shifts, group, 0, info_ref, w_ref, refs[:chips], w_buf, o_buf, sems)
    for c in copies:
        c.start()
    for c in copies:
        c.wait()
    out_ref[...] = h_ref[...].astype(F32) + dot32(o_buf[...], w_buf[...])


def oproj(info, outs, shifts, group, h_zero, w_o):
    tok, hid = h_zero.shape
    wide = outs[0].shape[1]
    chips = len(shifts)
    vm = pl.BlockSpec(memory_space=pltpu.VMEM)
    anyspec = pl.BlockSpec(memory_space=pl.ANY)
    return pl.pallas_call(
        functools.partial(oproj_kernel, shifts, group),
        in_specs=[pl.BlockSpec(memory_space=pltpu.SMEM)] + [anyspec] * chips + [vm, anyspec],
        out_specs=vm,
        out_shape=jax.ShapeDtypeStruct((tok, hid), F32),
        scratch_shapes=[
            pltpu.VMEM((chips * wide, hid), BF16),
            pltpu.VMEM((tok, chips * wide), BF16),
            pltpu.SemaphoreType.DMA((2 * chips,)),
        ],
        compiler_params=params(),
        cost_estimate=cost(2 * tok * hid * chips * wide, 2 * chips * wide * hid),
        name="oproj",
    )(info, *outs, h_zero, w_o)


def tail_kernel(shifts, tile, group, head0, info_ref, *refs):
    chips = len(shifts)
    h_ref, g_ref, wo_ref, wg_ref, wu_ref, wd_ref, out_ref = refs[chips:chips + 7]
    wo_buf, o_buf, wg_buf, wu_buf, wd_buf, act_buf, b_buf, acc_ref, o_sems, g_sems, u_sems, d_sems = refs[chips + 7:]
    tok = acc_ref.shape[0]
    tiles = wg_ref.shape[1] // tile

    def span(i):
        return pl.ds(pl.multiple_of(i * tile, tile), tile)

    def gate_copy(i, s):
        return pltpu.make_async_copy(wg_ref.at[:, span(i)], wg_buf.at[s], g_sems.at[s])

    def up_copy(i, s):
        return pltpu.make_async_copy(wu_ref.at[:, span(i)], wu_buf.at[s], u_sems.at[s])

    def down_copy(i, s):
        return pltpu.make_async_copy(wd_ref.at[span(i), :], wd_buf.at[s], d_sems.at[s])

    copies = half_oproj_copies(shifts, group, head0, info_ref, wo_ref, refs[:chips], wo_buf, o_buf, o_sems)
    copies.append(pltpu.make_async_copy(h_ref, acc_ref, o_sems.at[2 * chips]))
    for c in copies:
        c.start()
    for s in range(2):
        gate_copy(s, s).start()
        up_copy(s, s).start()
    down_copy(0, 0).start()
    for c in copies:
        c.wait()
    acc_ref[...] += dot32(o_buf[...], wo_buf[...])
    chunk = 32
    for r in range(0, tok, chunk):
        h1 = acc_ref[r:r + chunk, :].astype(BF16).astype(F32)
        acc_ref[r:r + chunk, :] = h1
        scale = lax.rsqrt(jnp.mean(h1 * h1, axis=-1, keepdims=True) + NORM_EPS)
        b_buf[r:r + chunk, :] = (h1 * scale * g_ref[...].astype(F32)).astype(BF16)

    def front(s):
        b = b_buf[...]
        return (jax.nn.silu(dot32(b, wg_buf[s])) * dot32(b, wu_buf[s])).astype(BF16)

    gate_copy(0, 0).wait()
    up_copy(0, 0).wait()
    act_buf[...] = front(0)
    down_copy(1, 1).start()

    def body(i, carry):
        s = lax.rem(i, 2)
        p = 1 - s

        @pl.when(i + 1 < tiles)
        def _():
            gate_copy(i + 1, p).start()
            up_copy(i + 1, p).start()

        gate_copy(i, s).wait()
        up_copy(i, s).wait()
        down_copy(i - 1, p).wait()
        before = act_buf[...]
        act_buf[...] = front(s)
        acc_ref[...] += dot32(before, wd_buf[p])

        @pl.when(i + 1 < tiles)
        def _():
            down_copy(i + 1, p).start()

        return carry

    def first_body():
        gate_copy(1, 1).wait()
        up_copy(1, 1).wait()
        down_copy(0, 0).wait()
        gate_copy(2, 0).start()
        up_copy(2, 0).start()
        before = act_buf[...]
        act_buf[...] = front(1)
        acc_ref[...] += dot32(before, wd_buf[0])
        down_copy(2, 0).start()

    first_body()
    lax.fori_loop(2, tiles, body, 0)
    last = (tiles - 1) % 2
    down_copy(tiles - 1, last).wait()
    out_ref[...] = (acc_ref[...] + dot32(act_buf[...], wd_buf[last])).astype(BF16)


def tail(info, outs, shifts, group, head0, partial, norm, w_o, w_gate, w_up, w_down):
    tok, hid = partial.shape
    ffn = w_gate.shape[1]
    tile = 768
    wide = outs[0].shape[1]
    chips = len(shifts)
    vm = pl.BlockSpec(memory_space=pltpu.VMEM)
    anyspec = pl.BlockSpec(memory_space=pl.ANY)
    return pl.pallas_call(
        functools.partial(tail_kernel, shifts, tile, group, head0),
        in_specs=[pl.BlockSpec(memory_space=pltpu.SMEM)] + [anyspec] * (chips + 1) + [vm] + [anyspec] * 4,
        out_specs=vm,
        out_shape=jax.ShapeDtypeStruct((tok, hid), BF16),
        scratch_shapes=[
            pltpu.VMEM((chips * wide, hid), BF16),
            pltpu.VMEM((tok, chips * wide), BF16),
            pltpu.VMEM((2, hid, tile), BF16),
            pltpu.VMEM((2, hid, tile), BF16),
            pltpu.VMEM((2, tile, hid), BF16),
            pltpu.VMEM((tok, tile), BF16),
            pltpu.VMEM((tok, hid), BF16),
            pltpu.VMEM((tok, hid), F32),
            pltpu.SemaphoreType.DMA((2 * chips + 1,)),
            pltpu.SemaphoreType.DMA((2,)),
            pltpu.SemaphoreType.DMA((2,)),
            pltpu.SemaphoreType.DMA((2,)),
        ],
        compiler_params=params(67043328),
        cost_estimate=cost(2 * tok * hid * (chips * wide + 3 * ffn), 2 * hid * (chips * wide + 3 * ffn)),
        name="tail",
    )(info, *outs, partial, norm[None], w_o, w_gate, w_up, w_down)


def rope_tables(rope_pos):
    half = HEAD_DIM // 2
    inv_freq = ROPE_THETA ** (-jnp.arange(0, HEAD_DIM, 2, dtype=F32) / HEAD_DIM)
    idx = jnp.arange(half)
    lo, hi = MROPE_SPLIT
    chosen = jnp.where(idx < lo, rope_pos[:, 0, :, None], jnp.where(idx < hi, rope_pos[:, 1, :, None], rope_pos[:, 2, :, None]))
    angles = chosen.astype(F32) * inv_freq
    cos_h, sin_h = jnp.cos(angles), jnp.sin(angles)
    return jnp.concatenate([cos_h, cos_h], axis=-1), jnp.concatenate([-sin_h, sin_h], axis=-1)


def solution(mesh):
    group = mesh.shape['sp']
    chips = group // CORES
    row_spec = P(('dp', 'sp'), None)
    sibling = [(i, CORES * (i // CORES) + (i + 1) % CORES) for i in range(group)]

    def hop(x, steps):
        return lax.ppermute(x, 'sp', [(i, (i + CORES * steps) % group) for i in range(group)])

    def swap(x):
        return lax.ppermute(x, 'sp', sibling)

    def step(patches, embeds, dest_slot, rope_pos, cu_doc, ln_w, ln_b, w_one, b_one, w_two, b_two, norm_attn, w_q, b_q, w_k, b_k, w_v, b_v, w_o, norm_mlp, w_gate, w_up, w_down):
        tok, _ = embeds.shape
        merged_dev = dest_slot.shape[0]
        num_docs = cu_doc.shape[0] - 1
        me = lax.axis_index('sp')
        chip, core = me // CORES, me % CORES
        width = w_q.shape[1] // chips
        half_m = merged_dev // 2
        half_t = tok // 2
        info = jnp.stack([chip, core]).astype(jnp.int32)

        e_prev = hop(embeds, 1)
        e_next = hop(embeds, -1)
        ints = jnp.concatenate([rope_pos, jnp.pad(dest_slot, (0, tok - merged_dev))[None]], axis=0)
        around = [ints, hop(ints, -1), hop(ints, 1), hop(ints, chips // 2)]
        merged = merger(patches, ln_w, ln_b, w_one, b_one, w_two, b_two)
        m_prev = hop(merged, 1)
        m_next = hop(merged, -1)
        m_far_lo = hop(m_prev[:half_m], 1)
        m_far_hi = hop(m_next[half_m:], -1)
        mine = [merged, m_next, m_prev, m_far_lo, m_far_hi]
        theirs = [swap(m) for m in mine[:-2]]
        theirs += [swap(m) for m in mine[-2:]]
        far = [hop(e_prev[:half_t], 1), hop(e_next[half_t:], -1)]

        around = jnp.stack(around)
        slots_own = around[:, 3, :merged_dev]
        slots_sib = swap(slots_own)
        cos_t, sin_t = rope_tables(around[:, :3])
        slots = jnp.concatenate([slots_own, slots_sib], axis=0)
        shard_chip = (chip + jnp.array([0, 1, chips - 1, chips // 2], jnp.int32)) % chips
        base = tok * (CORES * shard_chip + core)
        starts = (base[:, None] + jnp.arange(0, tok, 256, dtype=jnp.int32)[None, :]).reshape(-1, 1, 1)
        counts = jnp.sum((slots[None] >= starts) & (slots[None] < starts + 256), axis=-1, dtype=jnp.int32)
        qkv_info = jnp.concatenate([info, counts.reshape(-1)])
        common = (cos_t, sin_t, norm_attn, w_q, b_q, w_k, b_k, w_v, b_v, width, tok)
        q_n, k_n, v_n, h_zero, far_rows, far_mask = qkv(qkv_info, [[embeds], [e_next], [e_prev]], [slots] + mine + theirs, *common, True)
        k_sib_n, v_sib_n = swap(k_n), swap(v_n)
        q_f, k_f, v_f = qkv(info, [far], [far_rows, far_mask], *common, False)
        k_sibs = [k_sib_n, swap(k_f)]
        v_sibs = [v_sib_n, swap(v_f)]

        att_info = jnp.concatenate([info, cu_doc]).astype(jnp.int32)
        heads = width // HEAD_DIM
        split = (heads + 1) // 2
        shifts = (0, 1, -1, chips // 2)
        parts = []
        for head0, n in ((0, split), (split, heads - split)):
            o = attention(att_info, (q_n, q_f), (k_n, k_f), k_sibs, (v_n, v_f), v_sibs, num_docs, chips, tok, head0, n)
            parts.append([o[0]] + [hop(o[i], shifts[i]) for i in range(1, chips)])
        partial = oproj(info, parts[0], shifts, width, h_zero, w_o)
        return tail(info, parts[1], shifts, width, split, partial, norm_mlp, w_o, w_gate, w_up, w_down)

    in_specs = (row_spec, row_spec, P(('dp', 'sp')), P(None, ('dp', 'sp')), P('dp')) + (P(),) * 18
    return jax.shard_map(step, mesh=mesh, in_specs=in_specs, out_specs=row_spec, check_vma=False)
```

```python
import functools

import jax
import jax.numpy as jnp
from jax import lax
from jax.experimental import pallas as pl
from jax.experimental.pallas import tpu as pltpu
from jax.sharding import PartitionSpec as P


HEAD_DIM = 128
NORM_EPS = 1e-6
ROPE_THETA = 1000000.0
MROPE_SPLIT = (16, 40)
CORES = 2
NEG_BIG = -1e30
LOG2_E = 1.4426950408889634
F32 = jnp.float32
BF16 = jnp.bfloat16
VMEM_LIMIT = 60 * 1024 * 1024


def cost(flops, nbytes, trans=0):
    return pl.CostEstimate(flops=int(flops), bytes_accessed=int(nbytes), transcendentals=int(trans))


def params(limit=VMEM_LIMIT):
    return pltpu.CompilerParams(vmem_limit_bytes=limit)


def dot32(lhs, rhs):
    return jnp.dot(lhs, rhs, preferred_element_type=F32)


def merger_kernel(x_ref, vec_ref, w1_ref, w2_ref, out_ref, wide_ref, z_ref, acc_ref):
    step = pl.program_id(0)
    rows, feat = out_ref.shape[0], x_ref.shape[1]
    _, tile = w1_ref.shape
    lnw_ref, lnb_ref, b2_ref = vec_ref.at[:, :feat], vec_ref.at[:, feat:2 * feat], vec_ref.at[:, vec_ref.shape[1] - w2_ref.shape[1]:]
    b1_ref = vec_ref.at[:, pl.ds(pl.multiple_of(2 * feat + step * tile, 128), tile)]

    @pl.when(step == 0)
    def _():
        x = x_ref[...].astype(F32)
        cent = x - jnp.mean(x, axis=-1, keepdims=True)
        var = jnp.mean(cent * cent, axis=-1, keepdims=True)
        normed = cent * lax.rsqrt(var + NORM_EPS) * lnw_ref[...].astype(F32) + lnb_ref[...].astype(F32)
        for j in range(feat // 128):
            wide_ref[j] = normed[:, j * 128:(j + 1) * 128]
        for i in range(4):
            for j in range(feat // 128):
                col = i * feat + j * 128
                z_ref[:, col:col + 128] = wide_ref[j, pl.ds(i, rows, stride=4), :].astype(BF16)
        acc_ref[...] = jnp.zeros_like(acc_ref)

    pre = dot32(z_ref[...], w1_ref[...]) + b1_ref[...].astype(F32)
    inner = (0.5 * pre * (1.0 + lax.erf(pre * 2.0 ** -0.5))).astype(BF16)
    acc_ref[...] += dot32(inner, w2_ref[...])

    @pl.when(step == pl.num_programs(0) - 1)
    def _():
        out_ref[...] = (acc_ref[...] + b2_ref[...].astype(F32)).astype(BF16)


def merger(patches, ln_w, ln_b, w_one, b_one, w_two, b_two):
    total, feat = patches.shape
    rows = total // 4
    depth, mid = w_one.shape
    hid = w_two.shape[1]
    tile = 512
    whole = lambda i: (0, 0)
    return pl.pallas_call(
        merger_kernel,
        grid=(mid // tile,),
        in_specs=[
            pl.BlockSpec((total, feat), whole),
            pl.BlockSpec((1, 2 * feat + mid + hid), whole),
            pl.BlockSpec((depth, tile), lambda i: (0, i)),
            pl.BlockSpec((tile, hid), lambda i: (i, 0)),
        ],
        out_specs=pl.BlockSpec((rows, hid), whole),
        out_shape=jax.ShapeDtypeStruct((rows, hid), BF16),
        scratch_shapes=[
            pltpu.VMEM((feat // 128, total, 128), F32),
            pltpu.VMEM((rows, depth), BF16),
            pltpu.VMEM((rows, hid), F32),
        ],
        compiler_params=params(),
        cost_estimate=cost(2 * rows * mid * (depth + hid), 2 * mid * (depth + hid)),
        name="merger",
    )(patches, jnp.concatenate([ln_w, ln_b, b_one, b_two])[None], w_one, w_two)


def qkv_kernel(near, n_parts, e_counts, chips, info_ref, *refs):
    g_ref, cos_ref, sin_ref, bq_ref, bk_ref, bv_ref, wq_ref, wk_ref, wv_ref = refs[:9]
    n = len(e_counts)
    pos = 9
    e_refs = refs[pos:pos + sum(e_counts)]
    pos += len(e_refs)
    if near:
        slots_ref = refs[pos]
        m_refs = refs[pos + 1:pos + 1 + n_parts]
        pos += 1 + n_parts
        q_ref, k_ref, v_ref, h_ref, far_ref, far_mask_ref, e_buf, a_buf, w_buf, e_sems, w_sems, m_buf, acc_ref, any_ref, m_sems = refs[pos:]
    else:
        far_ref, far_mask_ref = refs[pos:pos + 2]
        q_ref, k_ref, v_ref, e_buf, a_buf, w_buf, e_sems, w_sems = refs[pos + 2:]
    first = 0 if near else chips - 1
    width = w_buf.shape[1] // 3
    heads = width // HEAD_DIM
    col = pl.multiple_of(info_ref[0] * width, width)
    tok, _ = a_buf.shape[1:]
    block = 256
    w_refs = (wq_ref, wk_ref, wv_ref)

    def load_weight(i):
        return pltpu.make_async_copy(w_refs[i].at[:, pl.ds(col, width)], w_buf.at[:, pl.ds(i * width, width)], w_sems.at[i])

    def loads(i):
        at = sum(e_counts[:i])
        row = 0
        out = []
        for j in range(e_counts[i]):
            rows = e_refs[at + j].shape[0]
            out.append(pltpu.make_async_copy(e_refs[at + j], e_buf.at[i % 2, pl.ds(row, rows), :], e_sems.at[i % 2, j]))
            row += rows
        return out

    if near:
        m_copies = []
        row = 0
        for j, m in enumerate(m_refs):
            m_copies.append(pltpu.make_async_copy(m, m_buf.at[pl.ds(row, m.shape[0]), :], m_sems.at[j]))
            row += m.shape[0]
        for c in m_copies:
            c.start()
    for c in loads(0):
        c.start()
    for i in range(3):
        load_weight(i).start()
    if near:
        for c in m_copies:
            c.wait()

    def gather_rows(shard, part):
        blocks = m_buf.shape[0] // block
        delta = chips // 2 if shard == chips - 1 else chips - 1 if shard == chips - 2 else shard
        chip = lax.rem(info_ref[0] + delta, chips)
        base = tok * (CORES * chip + info_ref[1]) + block * part
        acc_ref[...] = jnp.zeros_like(acc_ref)
        any_ref[...] = jnp.zeros_like(any_ref)

        def visit(j, carry):
            @pl.when(info_ref[2 + (shard * (tok // block) + part) * blocks + j] > 0)
            def _():
                token = base + lax.broadcasted_iota(jnp.int32, (block, block), 0)
                hit = (slots_ref[pl.ds(j, 1), :] == token).astype(F32)
                at = pl.ds(pl.multiple_of(j * block, block), block)
                acc_ref[...] += dot32(hit.astype(BF16), m_buf[at, :])
                any_ref[...] = jnp.maximum(any_ref[...], jnp.max(hit, axis=1, keepdims=True))

            return carry

        lax.fori_loop(0, blocks, visit, 0)

    chunk = 32

    def place_rows(i):
        for c in loads(i):
            c.wait()
        for part in range(tok // block):
            if near:
                gather_rows(i, part)
            for r in range(0, block, chunk):
                at = slice(part * block + r, part * block + r + chunk)
                if near:
                    hit, rows = any_ref[r:r + chunk, :1] > 0.5, acc_ref[r:r + chunk, :]
                else:
                    hit, rows = far_mask_ref[at, :1].astype(F32) > 0.5, far_ref[at, :].astype(F32)
                e_buf[i % 2, at, :] = jnp.where(hit, rows, e_buf[i % 2, at, :].astype(F32)).astype(BF16)
        if near and i == 0:
            h_ref[...] = e_buf[0]

    def norm_rows(i):
        for r in range(0, tok, chunk):
            h = e_buf[i % 2, r:r + chunk, :].astype(F32)
            scale = lax.rsqrt(jnp.mean(h * h, axis=-1, keepdims=True) + NORM_EPS)
            a_buf[i % 2, r:r + chunk, :] = (h * scale * g_ref[...].astype(F32)).astype(BF16)

    def emit(i, head, part, cos_t, sin_t):
        kind, h = divmod(head, heads)
        cols = slice(h * HEAD_DIM, (h + 1) * HEAD_DIM)
        bias = (bq_ref, bk_ref, bv_ref)[kind][:, pl.ds(pl.multiple_of(col + h * HEAD_DIM, HEAD_DIM), HEAD_DIM)]
        part = part + bias.astype(F32)
        if kind < 2:
            (q_ref, k_ref)[kind][i, :, cols] = (part * cos_t + pltpu.roll(part, HEAD_DIM // 2, 1) * sin_t).astype(BF16)
        else:
            v_ref[i, cols, :] = jnp.transpose(part).astype(BF16)

    place_rows(0)
    norm_rows(0)
    for i in range(n):
        if i + 1 < n:
            for c in loads(i + 1):
                c.start()
            place_rows(i + 1)
            norm_rows(i + 1)
        if i == 0:
            for j in range(3):
                load_weight(j).wait()
        a = a_buf[i % 2]
        cos_t, sin_t = cos_ref[first + i], sin_ref[first + i]
        for head in range(0, 3 * heads, 2):
            span = min(2, 3 * heads - head)
            lin = dot32(a, w_buf[:, head * HEAD_DIM:(head + span) * HEAD_DIM])
            for d in range(span):
                emit(i, head + d, lin[:, d * HEAD_DIM:(d + 1) * HEAD_DIM], cos_t, sin_t)
    if near:
        for part in range(tok // block):
            gather_rows(chips - 1, part)
            at = slice(part * block, (part + 1) * block)
            far_ref[at, :] = acc_ref[...].astype(BF16)
            far_mask_ref[at, :] = jnp.broadcast_to(any_ref[:, :1], (block, 128)).astype(BF16)


def qkv(info, pieces, extra, cos_t, sin_t, norm, w_q, b_q, w_k, b_k, w_v, b_v, width, tok, near):
    hid = w_q.shape[0]
    chips = cos_t.shape[0]
    n = len(pieces)
    flat = [a for p in pieces for a in p]
    counts = tuple(len(p) for p in pieces)
    vm = pl.BlockSpec(memory_space=pltpu.VMEM)
    anyspec = pl.BlockSpec(memory_space=pl.ANY)
    out_shape = [jax.ShapeDtypeStruct((n, tok, width), BF16)] * 2 + [jax.ShapeDtypeStruct((n, width, tok), BF16)]
    scratch = [
        pltpu.VMEM((2, tok, hid), BF16),
        pltpu.VMEM((2, tok, hid), BF16),
        pltpu.VMEM((hid, 3 * width), BF16),
        pltpu.SemaphoreType.DMA((2, max(counts))),
        pltpu.SemaphoreType.DMA((3,)),
    ]
    if near:
        parts = extra[1:]
        extra_specs = [vm] + [anyspec] * len(parts)
        out_shape += [jax.ShapeDtypeStruct((tok, hid), BF16)] * 2 + [jax.ShapeDtypeStruct((tok, 128), BF16)]
        scratch += [
            pltpu.VMEM((sum(a.shape[0] for a in parts), hid), BF16),
            pltpu.VMEM((256, hid), F32),
            pltpu.VMEM((256, 128), F32),
            pltpu.SemaphoreType.DMA((len(parts),)),
        ]
    else:
        extra_specs = [vm, vm]
    return pl.pallas_call(
        functools.partial(qkv_kernel, near, len(extra) - 1, counts, chips),
        in_specs=[pl.BlockSpec(memory_space=pltpu.SMEM)] + [vm] * 6 + [anyspec] * (3 + len(flat)) + extra_specs,
        out_specs=[vm] * len(out_shape),
        out_shape=out_shape,
        scratch_shapes=scratch,
        compiler_params=params(),
        cost_estimate=cost(2 * n * tok * hid * 3 * width, 2 * hid * 3 * width + 4 * n * tok * hid),
        name="qkv",
    )(info, norm[None], cos_t, sin_t, b_q[None], b_k[None], b_v[None], w_q, w_k, w_v, *flat, *extra)


def attn_kernel(num_docs, chips, head0, info_ref, *refs):
    q_in, k_own_in, k_sib_in, v_own_in, v_sib_in = (refs[2 * g:2 * g + 2] for g in range(5))
    o_refs = refs[10:10 + chips]
    q_buf, k_buf, v_buf, sems, m_ref, l_ref, acc_ref = refs[10 + chips:]
    head = pl.program_id(0)
    slot = lax.rem(head, 2)
    my_chip, core = info_ref[0], info_ref[1]
    tok = o_refs[0].shape[0]

    def copies(h, s):
        col = pl.multiple_of((head0 + h) * HEAD_DIM, HEAD_DIM)
        out = []
        lo = 0
        for g in range(2):
            n = q_in[g].shape[0]
            span = pl.ds(lo, n)
            lo += n
            cols = pl.ds(col, HEAD_DIM)
            out.append(pltpu.make_async_copy(q_in[g].at[:, :, cols], q_buf.at[s, span], sems.at[s, 5 * g]))
            out.append(pltpu.make_async_copy(k_own_in[g].at[:, :, cols], k_buf.at[s, 0, span], sems.at[s, 5 * g + 1]))
            out.append(pltpu.make_async_copy(k_sib_in[g].at[:, :, cols], k_buf.at[s, 1, span], sems.at[s, 5 * g + 2]))
            out.append(pltpu.make_async_copy(v_own_in[g].at[:, cols, :], v_buf.at[s, 0, span], sems.at[s, 5 * g + 3]))
            out.append(pltpu.make_async_copy(v_sib_in[g].at[:, cols, :], v_buf.at[s, 1, span], sems.at[s, 5 * g + 4]))
        return out

    @pl.when(head == 0)
    def _():
        for c in copies(0, 0):
            c.start()

    @pl.when(head + 1 < pl.num_programs(0))
    def _():
        for c in copies(head + 1, 1 - slot):
            c.start()

    for c in copies(head, slot):
        c.wait()

    def place_of(chip):
        delta = lax.rem(chip - my_chip + chips, chips)
        return jnp.where(delta == chips // 2, chips - 1, jnp.where(delta == chips - 1, chips - 2, delta))

    def doc_start(pos):
        start = jnp.zeros_like(pos)
        for d in range(1, num_docs):
            cut = info_ref[2 + d]
            start = jnp.where(pos >= cut, cut, start)
        return start

    factor = HEAD_DIM ** -0.5 * LOG2_E
    halves = 2
    half = tok // halves

    def queries(q_chip, carry):
        q_at = place_of(q_chip)
        q_base = tok * (CORES * q_chip + core)
        q = q_buf[slot, q_at]
        q_pos = q_base + lax.broadcasted_iota(jnp.int32, (1, tok), 1)
        starts = doc_start(q_pos)
        lo_start = doc_start(q_base)
        hi_start = doc_start(q_base + tok - 1)

        def block(j, masked, fresh):
            at = place_of(j)
            bases = (tok * (CORES * j + core), tok * (CORES * j + 1 - core))
            ks = [k_buf[slot, b, at] for b in range(2)]
            vs = jnp.concatenate([v_buf[slot, b, at] for b in range(2)], axis=1)
            scores = [[lax.dot_general(k, q[i * half:(i + 1) * half], (((1,), (1,)), ((), ())), preferred_element_type=F32) for k in ks] for i in range(halves)]
            for i in range(halves):
                lanes = slice(i * half, (i + 1) * half)
                pair = scores[i]
                if masked:
                    for b in range(2):
                        k_pos = bases[b] + lax.broadcasted_iota(jnp.int32, pair[b].shape, 0)
                        pair[b] = jnp.where((k_pos <= q_pos[:, lanes]) & (k_pos >= starts[:, lanes]), pair[b], NEG_BIG)
                top = jnp.maximum(jnp.max(pair[0], axis=0, keepdims=True), jnp.max(pair[1], axis=0, keepdims=True))
                if not fresh:
                    old = m_ref[:, lanes]
                    top = jnp.maximum(top, old)
                probs = [jnp.exp2((s - top) * factor) for s in pair]
                total = jnp.sum(probs[0], axis=0, keepdims=True) + jnp.sum(probs[1], axis=0, keepdims=True)
                out = dot32(vs, jnp.concatenate([p.astype(BF16) for p in probs], axis=0))
                if not fresh:
                    alpha = jnp.exp2((old - top) * factor)
                    total = total + l_ref[:, lanes] * alpha
                    out = out + acc_ref[:, lanes] * alpha
                m_ref[:, lanes] = top
                l_ref[:, lanes] = total
                acc_ref[:, lanes] = out

        block(q_chip, True, True)

        def body(t, inner):
            j = q_chip - 1 - t
            clear = tok * CORES * j >= hi_start

            @pl.when(clear)
            def _():
                block(j, False, False)

            @pl.when(jnp.logical_not(clear))
            def _():
                block(j, True, False)

            return inner

        lax.fori_loop(0, q_chip - lo_start // (tok * CORES), body, 0)
        out = jnp.transpose(acc_ref[...] / l_ref[...]).astype(BF16)
        for i in range(chips):
            @pl.when(q_at == i)
            def _():
                o_refs[i][...] = out

        return carry

    lax.fori_loop(0, chips, queries, 0)


def attention(info, qs, ks, k_sibs, vs, v_sibs, num_docs, chips, tok, head0, heads):
    grid_spec = pltpu.PrefetchScalarGridSpec(
        num_scalar_prefetch=1,
        grid=(heads,),
        in_specs=[pl.BlockSpec(memory_space=pl.ANY)] * 10,
        out_specs=[pl.BlockSpec((tok, HEAD_DIM), lambda h, s: (0, h))] * chips,
        scratch_shapes=[
            pltpu.VMEM((2, chips, tok, HEAD_DIM), BF16),
            pltpu.VMEM((2, 2, chips, tok, HEAD_DIM), BF16),
            pltpu.VMEM((2, 2, chips, HEAD_DIM, tok), BF16),
            pltpu.SemaphoreType.DMA((2, 10)),
            pltpu.VMEM((1, tok), F32),
            pltpu.VMEM((1, tok), F32),
            pltpu.VMEM((HEAD_DIM, tok), F32),
        ],
    )
    width = heads * HEAD_DIM
    return pl.pallas_call(
        functools.partial(attn_kernel, num_docs, chips, head0),
        grid_spec=grid_spec,
        out_shape=[jax.ShapeDtypeStruct((tok, width), BF16)] * chips,
        compiler_params=params(),
        cost_estimate=cost(2 * 2 * 20 * tok * tok * width, 2 * 5 * chips * tok * width),
        name="attend",
    )(info, *qs, *ks, *k_sibs, *vs, *v_sibs)


def half_oproj_copies(shifts, group, head0, info_ref, w_ref, o_refs, w_buf, o_buf, sems):
    chips = len(shifts)
    wide = o_refs[0].shape[1]
    out = []
    for i in range(chips):
        src = lax.rem(info_ref[0] + 2 * chips - shifts[i], chips)
        row = pl.multiple_of(src * group + head0 * HEAD_DIM, HEAD_DIM)
        out.append(pltpu.make_async_copy(w_ref.at[pl.ds(row, wide), :], w_buf.at[pl.ds(i * wide, wide), :], sems.at[i]))
        out.append(pltpu.make_async_copy(o_refs[i], o_buf.at[:, pl.ds(i * wide, wide)], sems.at[chips + i]))
    return out


def oproj_kernel(shifts, group, info_ref, *refs):
    chips = len(shifts)
    h_ref, w_ref, out_ref, w_buf, o_buf, sems = refs[chips:]
    copies = half_oproj_copies(shifts, group, 0, info_ref, w_ref, refs[:chips], w_buf, o_buf, sems)
    for c in copies:
        c.start()
    for c in copies:
        c.wait()
    out_ref[...] = h_ref[...].astype(F32) + dot32(o_buf[...], w_buf[...])


def oproj(info, outs, shifts, group, h_zero, w_o):
    tok, hid = h_zero.shape
    wide = outs[0].shape[1]
    chips = len(shifts)
    vm = pl.BlockSpec(memory_space=pltpu.VMEM)
    anyspec = pl.BlockSpec(memory_space=pl.ANY)
    return pl.pallas_call(
        functools.partial(oproj_kernel, shifts, group),
        in_specs=[pl.BlockSpec(memory_space=pltpu.SMEM)] + [anyspec] * chips + [vm, anyspec],
        out_specs=vm,
        out_shape=jax.ShapeDtypeStruct((tok, hid), F32),
        scratch_shapes=[
            pltpu.VMEM((chips * wide, hid), BF16),
            pltpu.VMEM((tok, chips * wide), BF16),
            pltpu.SemaphoreType.DMA((2 * chips,)),
        ],
        compiler_params=params(),
        cost_estimate=cost(2 * tok * hid * chips * wide, 2 * chips * wide * hid),
        name="oproj",
    )(info, *outs, h_zero, w_o)


def tail_kernel(shifts, tile, group, head0, info_ref, *refs):
    chips = len(shifts)
    h_ref, g_ref, wo_ref, wg_ref, wu_ref, wd_ref, out_ref = refs[chips:chips + 7]
    wo_buf, o_buf, wg_buf, wu_buf, wd_buf, act_buf, b_buf, acc_ref, o_sems, g_sems, u_sems, d_sems = refs[chips + 7:]
    tok = acc_ref.shape[0]
    tiles = wg_ref.shape[1] // tile

    def span(i):
        return pl.ds(pl.multiple_of(i * tile, tile), tile)

    def gate_copy(i, s):
        return pltpu.make_async_copy(wg_ref.at[:, span(i)], wg_buf.at[s], g_sems.at[s])

    def up_copy(i, s):
        return pltpu.make_async_copy(wu_ref.at[:, span(i)], wu_buf.at[s], u_sems.at[s])

    def down_copy(i, s):
        return pltpu.make_async_copy(wd_ref.at[span(i), :], wd_buf.at[s], d_sems.at[s])

    copies = half_oproj_copies(shifts, group, head0, info_ref, wo_ref, refs[:chips], wo_buf, o_buf, o_sems)
    copies.append(pltpu.make_async_copy(h_ref, acc_ref, o_sems.at[2 * chips]))
    for c in copies:
        c.start()
    for s in range(2):
        gate_copy(s, s).start()
        up_copy(s, s).start()
    down_copy(0, 0).start()
    for c in copies:
        c.wait()
    acc_ref[...] += dot32(o_buf[...], wo_buf[...])
    chunk = 32
    for r in range(0, tok, chunk):
        h1 = acc_ref[r:r + chunk, :].astype(BF16).astype(F32)
        acc_ref[r:r + chunk, :] = h1
        scale = lax.rsqrt(jnp.mean(h1 * h1, axis=-1, keepdims=True) + NORM_EPS)
        b_buf[r:r + chunk, :] = (h1 * scale * g_ref[...].astype(F32)).astype(BF16)

    def front(s):
        b = b_buf[...]
        return (jax.nn.silu(dot32(b, wg_buf[s])) * dot32(b, wu_buf[s])).astype(BF16)

    gate_copy(0, 0).wait()
    up_copy(0, 0).wait()
    act_buf[...] = front(0)
    down_copy(1, 1).start()

    def body(i, carry):
        s = lax.rem(i, 2)
        p = 1 - s

        @pl.when(i + 1 < tiles)
        def _():
            gate_copy(i + 1, p).start()
            up_copy(i + 1, p).start()

        gate_copy(i, s).wait()
        up_copy(i, s).wait()
        down_copy(i - 1, p).wait()
        before = act_buf[...]
        act_buf[...] = front(s)
        acc_ref[...] += dot32(before, wd_buf[p])

        @pl.when(i + 1 < tiles)
        def _():
            down_copy(i + 1, p).start()

        return carry

    def first_body():
        gate_copy(1, 1).wait()
        up_copy(1, 1).wait()
        down_copy(0, 0).wait()
        gate_copy(2, 0).start()
        up_copy(2, 0).start()
        before = act_buf[...]
        act_buf[...] = front(1)
        acc_ref[...] += dot32(before, wd_buf[0])
        down_copy(2, 0).start()

    first_body()
    lax.fori_loop(2, tiles, body, 0)
    last = (tiles - 1) % 2
    down_copy(tiles - 1, last).wait()
    out_ref[...] = (acc_ref[...] + dot32(act_buf[...], wd_buf[last])).astype(BF16)


def tail(info, outs, shifts, group, head0, partial, norm, w_o, w_gate, w_up, w_down):
    tok, hid = partial.shape
    ffn = w_gate.shape[1]
    tile = 768
    wide = outs[0].shape[1]
    chips = len(shifts)
    vm = pl.BlockSpec(memory_space=pltpu.VMEM)
    anyspec = pl.BlockSpec(memory_space=pl.ANY)
    return pl.pallas_call(
        functools.partial(tail_kernel, shifts, tile, group, head0),
        in_specs=[pl.BlockSpec(memory_space=pltpu.SMEM)] + [anyspec] * (chips + 1) + [vm] + [anyspec] * 4,
        out_specs=vm,
        out_shape=jax.ShapeDtypeStruct((tok, hid), BF16),
        scratch_shapes=[
            pltpu.VMEM((chips * wide, hid), BF16),
            pltpu.VMEM((tok, chips * wide), BF16),
            pltpu.VMEM((2, hid, tile), BF16),
            pltpu.VMEM((2, hid, tile), BF16),
            pltpu.VMEM((2, tile, hid), BF16),
            pltpu.VMEM((tok, tile), BF16),
            pltpu.VMEM((tok, hid), BF16),
            pltpu.VMEM((tok, hid), F32),
            pltpu.SemaphoreType.DMA((2 * chips + 1,)),
            pltpu.SemaphoreType.DMA((2,)),
            pltpu.SemaphoreType.DMA((2,)),
            pltpu.SemaphoreType.DMA((2,)),
        ],
        compiler_params=params(67043328),
        cost_estimate=cost(2 * tok * hid * (chips * wide + 3 * ffn), 2 * hid * (chips * wide + 3 * ffn)),
        name="tail",
    )(info, *outs, partial, norm[None], w_o, w_gate, w_up, w_down)


def rope_tables(rope_pos):
    half = HEAD_DIM // 2
    inv_freq = ROPE_THETA ** (-jnp.arange(0, HEAD_DIM, 2, dtype=F32) / HEAD_DIM)
    idx = jnp.arange(half)
    lo, hi = MROPE_SPLIT
    chosen = jnp.where(idx < lo, rope_pos[:, 0, :, None], jnp.where(idx < hi, rope_pos[:, 1, :, None], rope_pos[:, 2, :, None]))
    angles = chosen.astype(F32) * inv_freq
    cos_h, sin_h = jnp.cos(angles), jnp.sin(angles)
    return jnp.concatenate([cos_h, cos_h], axis=-1), jnp.concatenate([-sin_h, sin_h], axis=-1)


def solution(mesh):
    group = mesh.shape['sp']
    chips = group // CORES
    row_spec = P(('dp', 'sp'), None)
    sibling = [(i, CORES * (i // CORES) + (i + 1) % CORES) for i in range(group)]

    def hop(x, steps):
        return lax.ppermute(x, 'sp', [(i, (i + CORES * steps) % group) for i in range(group)])

    def swap(x):
        return lax.ppermute(x, 'sp', sibling)

    def step(patches, embeds, dest_slot, rope_pos, cu_doc, ln_w, ln_b, w_one, b_one, w_two, b_two, norm_attn, w_q, b_q, w_k, b_k, w_v, b_v, w_o, norm_mlp, w_gate, w_up, w_down):
        tok, _ = embeds.shape
        merged_dev = dest_slot.shape[0]
        num_docs = cu_doc.shape[0] - 1
        me = lax.axis_index('sp')
        chip, core = me // CORES, me % CORES
        width = w_q.shape[1] // chips
        half_m = merged_dev // 2
        half_t = tok // 2
        info = jnp.stack([chip, core]).astype(jnp.int32)

        cut = 7 * tok // 8
        e_a, e_b = embeds[:cut], embeds[cut:]
        a_prev = hop(e_a, 1)
        a_next = hop(e_a, -1)
        ints = jnp.concatenate([rope_pos, jnp.pad(dest_slot, (0, tok - merged_dev))[None]], axis=0)
        around = [ints, hop(ints, -1), hop(ints, 1), hop(ints, chips // 2)]
        merged = merger(patches, ln_w, ln_b, w_one, b_one, w_two, b_two)
        m_prev = hop(merged, 1)
        m_next = hop(merged, -1)
        m_far_lo = hop(m_prev[:half_m], 1)
        m_far_hi = hop(m_next[half_m:], -1)
        mine = [merged, m_next, m_prev, m_far_lo, m_far_hi]
        theirs = [swap(m) for m in mine[:-2]]
        theirs += [swap(m) for m in mine[-2:]]
        b_prev = hop(e_b, 1)
        b_next = hop(e_b, -1)
        far = [hop(a_prev[:half_t], 1), hop(a_next[half_t:], -1), hop(b_next, -1)]

        around = jnp.stack(around)
        slots_own = around[:, 3, :merged_dev]
        slots_sib = swap(slots_own)
        cos_t, sin_t = rope_tables(around[:, :3])
        slots = jnp.concatenate([slots_own, slots_sib], axis=0)
        shard_chip = (chip + jnp.array([0, 1, chips - 1, chips // 2], jnp.int32)) % chips
        base = tok * (CORES * shard_chip + core)
        starts = (base[:, None] + jnp.arange(0, tok, 256, dtype=jnp.int32)[None, :]).reshape(-1, 1, 1)
        counts = jnp.sum((slots[None] >= starts) & (slots[None] < starts + 256), axis=-1, dtype=jnp.int32)
        qkv_info = jnp.concatenate([info, counts.reshape(-1)])
        common = (cos_t, sin_t, norm_attn, w_q, b_q, w_k, b_k, w_v, b_v, width, tok)
        q_n, k_n, v_n, h_zero, far_rows, far_mask = qkv(qkv_info, [[embeds], [a_next, b_next], [a_prev, b_prev]], [slots] + mine + theirs, *common, True)
        k_sib_n, v_sib_n = swap(k_n), swap(v_n)
        q_f, k_f, v_f = qkv(info, [far], [far_rows, far_mask], *common, False)
        k_sibs = [k_sib_n, swap(k_f)]
        v_sibs = [v_sib_n, swap(v_f)]

        att_info = jnp.concatenate([info, cu_doc]).astype(jnp.int32)
        heads = width // HEAD_DIM
        split = (heads + 1) // 2
        shifts = (0, 1, -1, chips // 2)
        parts = []
        for head0, n in ((0, split), (split, heads - split)):
            o = attention(att_info, (q_n, q_f), (k_n, k_f), k_sibs, (v_n, v_f), v_sibs, num_docs, chips, tok, head0, n)
            parts.append([o[0]] + [hop(o[i], shifts[i]) for i in range(1, chips)])
        partial = oproj(info, parts[0], shifts, width, h_zero, w_o)
        return tail(info, parts[1], shifts, width, split, partial, norm_mlp, w_o, w_gate, w_up, w_down)

    in_specs = (row_spec, row_spec, P(('dp', 'sp')), P(None, ('dp', 'sp')), P('dp')) + (P(),) * 18
    return jax.shard_map(step, mesh=mesh, in_specs=in_specs, out_specs=row_spec, check_vma=False)
```

```python
import functools

import jax
import jax.numpy as jnp
from jax import lax
from jax.experimental import pallas as pl
from jax.experimental.pallas import tpu as pltpu
from jax.sharding import PartitionSpec as P


HEAD_DIM = 128
NORM_EPS = 1e-6
ROPE_THETA = 1000000.0
MROPE_SPLIT = (16, 40)
CORES = 2
NEG_BIG = -1e30
LOG2_E = 1.4426950408889634
F32 = jnp.float32
BF16 = jnp.bfloat16
VMEM_LIMIT = 60 * 1024 * 1024


def cost(flops, nbytes, trans=0):
    return pl.CostEstimate(flops=int(flops), bytes_accessed=int(nbytes), transcendentals=int(trans))


def params(limit=VMEM_LIMIT):
    return pltpu.CompilerParams(vmem_limit_bytes=limit)


def dot32(lhs, rhs):
    return jnp.dot(lhs, rhs, preferred_element_type=F32)


def merger_kernel(x_ref, vec_ref, w1_ref, w2_ref, lo_ref, hi_ref, wide_ref, z_ref, acc_ref):
    step = pl.program_id(0)
    half = lo_ref.shape[0]
    rows, feat = 2 * half, x_ref.shape[1]
    _, tile = w1_ref.shape
    lnw_ref, lnb_ref, b2_ref = vec_ref.at[:, :feat], vec_ref.at[:, feat:2 * feat], vec_ref.at[:, vec_ref.shape[1] - w2_ref.shape[1]:]
    b1_ref = vec_ref.at[:, pl.ds(pl.multiple_of(2 * feat + step * tile, 128), tile)]

    @pl.when(step == 0)
    def _():
        x = x_ref[...].astype(F32)
        cent = x - jnp.mean(x, axis=-1, keepdims=True)
        var = jnp.mean(cent * cent, axis=-1, keepdims=True)
        normed = cent * lax.rsqrt(var + NORM_EPS) * lnw_ref[...].astype(F32) + lnb_ref[...].astype(F32)
        for j in range(feat // 128):
            wide_ref[j] = normed[:, j * 128:(j + 1) * 128]
        for i in range(4):
            for j in range(feat // 128):
                col = i * feat + j * 128
                z_ref[:, col:col + 128] = wide_ref[j, pl.ds(i, rows, stride=4), :].astype(BF16)
        acc_ref[...] = jnp.zeros_like(acc_ref)

    pre = dot32(z_ref[...], w1_ref[...]) + b1_ref[...].astype(F32)
    inner = (0.5 * pre * (1.0 + lax.erf(pre * 2.0 ** -0.5))).astype(BF16)
    acc_ref[...] += dot32(inner, w2_ref[...])

    @pl.when(step == pl.num_programs(0) - 1)
    def _():
        out = (acc_ref[...] + b2_ref[...].astype(F32)).astype(BF16)
        lo_ref[...] = out[:half]
        hi_ref[...] = out[half:]


def merger(patches, ln_w, ln_b, w_one, b_one, w_two, b_two):
    total, feat = patches.shape
    rows = total // 4
    depth, mid = w_one.shape
    hid = w_two.shape[1]
    tile = 512
    whole = lambda i: (0, 0)
    return pl.pallas_call(
        merger_kernel,
        grid=(mid // tile,),
        in_specs=[
            pl.BlockSpec((total, feat), whole),
            pl.BlockSpec((1, 2 * feat + mid + hid), whole),
            pl.BlockSpec((depth, tile), lambda i: (0, i)),
            pl.BlockSpec((tile, hid), lambda i: (i, 0)),
        ],
        out_specs=[pl.BlockSpec((rows // 2, hid), whole)] * 2,
        out_shape=[jax.ShapeDtypeStruct((rows // 2, hid), BF16)] * 2,
        scratch_shapes=[
            pltpu.VMEM((feat // 128, total, 128), F32),
            pltpu.VMEM((rows, depth), BF16),
            pltpu.VMEM((rows, hid), F32),
        ],
        compiler_params=params(),
        cost_estimate=cost(2 * rows * mid * (depth + hid), 2 * mid * (depth + hid)),
        name="merger",
    )(patches, jnp.concatenate([ln_w, ln_b, b_one, b_two])[None], w_one, w_two)


def qkv_kernel(near, n_parts, e_counts, chips, info_ref, *refs):
    g_ref, cos_ref, sin_ref, bq_ref, bk_ref, bv_ref, wq_ref, wk_ref, wv_ref = refs[:9]
    n = len(e_counts)
    pos = 9
    e_refs = refs[pos:pos + sum(e_counts)]
    pos += len(e_refs)
    if near:
        slots_ref = refs[pos]
        m_refs = refs[pos + 1:pos + 1 + n_parts]
        pos += 1 + n_parts
        q_ref, k_ref, v_ref, h_ref, far_ref, far_mask_ref, e_buf, a_buf, w_buf, e_sems, w_sems, m_buf, acc_ref, any_ref, m_sems = refs[pos:]
    else:
        far_ref, far_mask_ref = refs[pos:pos + 2]
        q_ref, k_ref, v_ref, e_buf, a_buf, w_buf, e_sems, w_sems = refs[pos + 2:]
    first = 0 if near else chips - 1
    width = w_buf.shape[1] // 3
    heads = width // HEAD_DIM
    col = pl.multiple_of(info_ref[0] * width, width)
    tok, _ = a_buf.shape[1:]
    block = 256
    w_refs = (wq_ref, wk_ref, wv_ref)

    def load_weight(i):
        return pltpu.make_async_copy(w_refs[i].at[:, pl.ds(col, width)], w_buf.at[:, pl.ds(i * width, width)], w_sems.at[i])

    def loads(i):
        at = sum(e_counts[:i])
        row = 0
        out = []
        for j in range(e_counts[i]):
            rows = e_refs[at + j].shape[0]
            out.append(pltpu.make_async_copy(e_refs[at + j], e_buf.at[i % 2, pl.ds(row, rows), :], e_sems.at[i % 2, j]))
            row += rows
        return out

    if near:
        m_copies = []
        row = 0
        for j, m in enumerate(m_refs):
            m_copies.append(pltpu.make_async_copy(m, m_buf.at[pl.ds(row, m.shape[0]), :], m_sems.at[j]))
            row += m.shape[0]
        for c in m_copies:
            c.start()
    for c in loads(0):
        c.start()
    for i in range(3):
        load_weight(i).start()
    if near:
        for c in m_copies:
            c.wait()

    def gather_rows(shard, part):
        blocks = m_buf.shape[0] // block
        delta = chips // 2 if shard == chips - 1 else chips - 1 if shard == chips - 2 else shard
        chip = lax.rem(info_ref[0] + delta, chips)
        base = tok * (CORES * chip + info_ref[1]) + block * part
        acc_ref[...] = jnp.zeros_like(acc_ref)
        any_ref[...] = jnp.zeros_like(any_ref)

        def visit(j, carry):
            @pl.when(info_ref[2 + (shard * (tok // block) + part) * blocks + j] > 0)
            def _():
                token = base + lax.broadcasted_iota(jnp.int32, (block, block), 0)
                hit = (slots_ref[pl.ds(j, 1), :] == token).astype(F32)
                at = pl.ds(pl.multiple_of(j * block, block), block)
                acc_ref[...] += dot32(hit.astype(BF16), m_buf[at, :])
                any_ref[...] = jnp.maximum(any_ref[...], jnp.max(hit, axis=1, keepdims=True))

            return carry

        lax.fori_loop(0, blocks, visit, 0)

    chunk = 32

    def place_rows(i):
        for c in loads(i):
            c.wait()
        for part in range(tok // block):
            if near:
                gather_rows(i, part)
            for r in range(0, block, chunk):
                at = slice(part * block + r, part * block + r + chunk)
                if near:
                    hit, rows = any_ref[r:r + chunk, :1] > 0.5, acc_ref[r:r + chunk, :]
                else:
                    hit, rows = far_mask_ref[at, :1].astype(F32) > 0.5, far_ref[at, :].astype(F32)
                e_buf[i % 2, at, :] = jnp.where(hit, rows, e_buf[i % 2, at, :].astype(F32)).astype(BF16)
        if near and i == 0:
            h_ref[...] = e_buf[0]

    def norm_rows(i):
        for r in range(0, tok, chunk):
            h = e_buf[i % 2, r:r + chunk, :].astype(F32)
            scale = lax.rsqrt(jnp.mean(h * h, axis=-1, keepdims=True) + NORM_EPS)
            a_buf[i % 2, r:r + chunk, :] = (h * scale * g_ref[...].astype(F32)).astype(BF16)

    def emit(i, head, part, cos_t, sin_t):
        kind, h = divmod(head, heads)
        cols = slice(h * HEAD_DIM, (h + 1) * HEAD_DIM)
        bias = (bq_ref, bk_ref, bv_ref)[kind][:, pl.ds(pl.multiple_of(col + h * HEAD_DIM, HEAD_DIM), HEAD_DIM)]
        part = part + bias.astype(F32)
        if kind < 2:
            (q_ref, k_ref)[kind][i, :, cols] = (part * cos_t + pltpu.roll(part, HEAD_DIM // 2, 1) * sin_t).astype(BF16)
        else:
            v_ref[i, cols, :] = jnp.transpose(part).astype(BF16)

    place_rows(0)
    norm_rows(0)
    for i in range(n):
        if i + 1 < n:
            for c in loads(i + 1):
                c.start()
            place_rows(i + 1)
            norm_rows(i + 1)
        if i == 0:
            for j in range(3):
                load_weight(j).wait()
        a = a_buf[i % 2]
        cos_t, sin_t = cos_ref[first + i], sin_ref[first + i]
        for head in range(0, 3 * heads, 2):
            span = min(2, 3 * heads - head)
            lin = dot32(a, w_buf[:, head * HEAD_DIM:(head + span) * HEAD_DIM])
            for d in range(span):
                emit(i, head + d, lin[:, d * HEAD_DIM:(d + 1) * HEAD_DIM], cos_t, sin_t)
    if near:
        for part in range(tok // block):
            gather_rows(chips - 1, part)
            at = slice(part * block, (part + 1) * block)
            far_ref[at, :] = acc_ref[...].astype(BF16)
            far_mask_ref[at, :] = jnp.broadcast_to(any_ref[:, :1], (block, 128)).astype(BF16)


def qkv(info, pieces, extra, cos_t, sin_t, norm, w_q, b_q, w_k, b_k, w_v, b_v, width, tok, near):
    hid = w_q.shape[0]
    chips = cos_t.shape[0]
    n = len(pieces)
    flat = [a for p in pieces for a in p]
    counts = tuple(len(p) for p in pieces)
    vm = pl.BlockSpec(memory_space=pltpu.VMEM)
    anyspec = pl.BlockSpec(memory_space=pl.ANY)
    out_shape = [jax.ShapeDtypeStruct((n, tok, width), BF16)] * 2 + [jax.ShapeDtypeStruct((n, width, tok), BF16)]
    scratch = [
        pltpu.VMEM((2, tok, hid), BF16),
        pltpu.VMEM((2, tok, hid), BF16),
        pltpu.VMEM((hid, 3 * width), BF16),
        pltpu.SemaphoreType.DMA((2, max(counts))),
        pltpu.SemaphoreType.DMA((3,)),
    ]
    if near:
        parts = extra[1:]
        extra_specs = [vm] + [anyspec] * len(parts)
        out_shape += [jax.ShapeDtypeStruct((tok, hid), BF16)] * 2 + [jax.ShapeDtypeStruct((tok, 128), BF16)]
        scratch += [
            pltpu.VMEM((sum(a.shape[0] for a in parts), hid), BF16),
            pltpu.VMEM((256, hid), F32),
            pltpu.VMEM((256, 128), F32),
            pltpu.SemaphoreType.DMA((len(parts),)),
        ]
    else:
        extra_specs = [vm, vm]
    return pl.pallas_call(
        functools.partial(qkv_kernel, near, len(extra) - 1, counts, chips),
        in_specs=[pl.BlockSpec(memory_space=pltpu.SMEM)] + [vm] * 6 + [anyspec] * (3 + len(flat)) + extra_specs,
        out_specs=[vm] * len(out_shape),
        out_shape=out_shape,
        scratch_shapes=scratch,
        compiler_params=params(),
        cost_estimate=cost(2 * n * tok * hid * 3 * width, 2 * hid * 3 * width + 4 * n * tok * hid),
        name="qkv",
    )(info, norm[None], cos_t, sin_t, b_q[None], b_k[None], b_v[None], w_q, w_k, w_v, *flat, *extra)


def attn_kernel(num_docs, chips, head0, info_ref, *refs):
    q_in, k_own_in, k_sib_in, v_own_in, v_sib_in = (refs[2 * g:2 * g + 2] for g in range(5))
    o_refs = refs[10:10 + chips]
    q_buf, k_buf, v_buf, sems, m_ref, l_ref, acc_ref = refs[10 + chips:]
    head = pl.program_id(0)
    slot = lax.rem(head, 2)
    my_chip, core = info_ref[0], info_ref[1]
    tok = o_refs[0].shape[0]

    def copies(h, s):
        col = pl.multiple_of((head0 + h) * HEAD_DIM, HEAD_DIM)
        out = []
        lo = 0
        for g in range(2):
            n = q_in[g].shape[0]
            span = pl.ds(lo, n)
            lo += n
            cols = pl.ds(col, HEAD_DIM)
            out.append(pltpu.make_async_copy(q_in[g].at[:, :, cols], q_buf.at[s, span], sems.at[s, 5 * g]))
            out.append(pltpu.make_async_copy(k_own_in[g].at[:, :, cols], k_buf.at[s, 0, span], sems.at[s, 5 * g + 1]))
            out.append(pltpu.make_async_copy(k_sib_in[g].at[:, :, cols], k_buf.at[s, 1, span], sems.at[s, 5 * g + 2]))
            out.append(pltpu.make_async_copy(v_own_in[g].at[:, cols, :], v_buf.at[s, 0, span], sems.at[s, 5 * g + 3]))
            out.append(pltpu.make_async_copy(v_sib_in[g].at[:, cols, :], v_buf.at[s, 1, span], sems.at[s, 5 * g + 4]))
        return out

    @pl.when(head == 0)
    def _():
        for c in copies(0, 0):
            c.start()

    @pl.when(head + 1 < pl.num_programs(0))
    def _():
        for c in copies(head + 1, 1 - slot):
            c.start()

    for c in copies(head, slot):
        c.wait()

    def place_of(chip):
        delta = lax.rem(chip - my_chip + chips, chips)
        return jnp.where(delta == chips // 2, chips - 1, jnp.where(delta == chips - 1, chips - 2, delta))

    def doc_start(pos):
        start = jnp.zeros_like(pos)
        for d in range(1, num_docs):
            cut = info_ref[2 + d]
            start = jnp.where(pos >= cut, cut, start)
        return start

    factor = HEAD_DIM ** -0.5 * LOG2_E
    halves = 2
    half = tok // halves

    def queries(q_chip, carry):
        q_at = place_of(q_chip)
        q_base = tok * (CORES * q_chip + core)
        q = q_buf[slot, q_at]
        q_pos = q_base + lax.broadcasted_iota(jnp.int32, (1, tok), 1)
        starts = doc_start(q_pos)
        lo_start = doc_start(q_base)
        hi_start = doc_start(q_base + tok - 1)

        def block(j, masked, fresh):
            at = place_of(j)
            bases = (tok * (CORES * j + core), tok * (CORES * j + 1 - core))
            ks = [k_buf[slot, b, at] for b in range(2)]
            vs = jnp.concatenate([v_buf[slot, b, at] for b in range(2)], axis=1)
            scores = [[lax.dot_general(k, q[i * half:(i + 1) * half], (((1,), (1,)), ((), ())), preferred_element_type=F32) for k in ks] for i in range(halves)]
            for i in range(halves):
                lanes = slice(i * half, (i + 1) * half)
                pair = scores[i]
                if masked:
                    for b in range(2):
                        k_pos = bases[b] + lax.broadcasted_iota(jnp.int32, pair[b].shape, 0)
                        pair[b] = jnp.where((k_pos <= q_pos[:, lanes]) & (k_pos >= starts[:, lanes]), pair[b], NEG_BIG)
                top = jnp.maximum(jnp.max(pair[0], axis=0, keepdims=True), jnp.max(pair[1], axis=0, keepdims=True))
                if not fresh:
                    old = m_ref[:, lanes]
                    top = jnp.maximum(top, old)
                probs = [jnp.exp2((s - top) * factor) for s in pair]
                total = jnp.sum(probs[0], axis=0, keepdims=True) + jnp.sum(probs[1], axis=0, keepdims=True)
                out = dot32(vs, jnp.concatenate([p.astype(BF16) for p in probs], axis=0))
                if not fresh:
                    alpha = jnp.exp2((old - top) * factor)
                    total = total + l_ref[:, lanes] * alpha
                    out = out + acc_ref[:, lanes] * alpha
                m_ref[:, lanes] = top
                l_ref[:, lanes] = total
                acc_ref[:, lanes] = out

        block(q_chip, True, True)

        def body(t, inner):
            j = q_chip - 1 - t
            clear = tok * CORES * j >= hi_start

            @pl.when(clear)
            def _():
                block(j, False, False)

            @pl.when(jnp.logical_not(clear))
            def _():
                block(j, True, False)

            return inner

        lax.fori_loop(0, q_chip - lo_start // (tok * CORES), body, 0)
        out = jnp.transpose(acc_ref[...] / l_ref[...]).astype(BF16)
        for i in range(chips):
            @pl.when(q_at == i)
            def _():
                o_refs[i][...] = out

        return carry

    lax.fori_loop(0, chips, queries, 0)


def attention(info, qs, ks, k_sibs, vs, v_sibs, num_docs, chips, tok, head0, heads):
    grid_spec = pltpu.PrefetchScalarGridSpec(
        num_scalar_prefetch=1,
        grid=(heads,),
        in_specs=[pl.BlockSpec(memory_space=pl.ANY)] * 10,
        out_specs=[pl.BlockSpec((tok, HEAD_DIM), lambda h, s: (0, h))] * chips,
        scratch_shapes=[
            pltpu.VMEM((2, chips, tok, HEAD_DIM), BF16),
            pltpu.VMEM((2, 2, chips, tok, HEAD_DIM), BF16),
            pltpu.VMEM((2, 2, chips, HEAD_DIM, tok), BF16),
            pltpu.SemaphoreType.DMA((2, 10)),
            pltpu.VMEM((1, tok), F32),
            pltpu.VMEM((1, tok), F32),
            pltpu.VMEM((HEAD_DIM, tok), F32),
        ],
    )
    width = heads * HEAD_DIM
    return pl.pallas_call(
        functools.partial(attn_kernel, num_docs, chips, head0),
        grid_spec=grid_spec,
        out_shape=[jax.ShapeDtypeStruct((tok, width), BF16)] * chips,
        compiler_params=params(),
        cost_estimate=cost(2 * 2 * 20 * tok * tok * width, 2 * 5 * chips * tok * width),
        name="attend",
    )(info, *qs, *ks, *k_sibs, *vs, *v_sibs)


def half_oproj_copies(shifts, group, head0, info_ref, w_ref, o_refs, w_buf, o_buf, sems):
    chips = len(shifts)
    wide = o_refs[0].shape[1]
    out = []
    for i in range(chips):
        src = lax.rem(info_ref[0] + 2 * chips - shifts[i], chips)
        row = pl.multiple_of(src * group + head0 * HEAD_DIM, HEAD_DIM)
        out.append(pltpu.make_async_copy(w_ref.at[pl.ds(row, wide), :], w_buf.at[pl.ds(i * wide, wide), :], sems.at[i]))
        out.append(pltpu.make_async_copy(o_refs[i], o_buf.at[:, pl.ds(i * wide, wide)], sems.at[chips + i]))
    return out


def oproj_kernel(shifts, group, info_ref, *refs):
    chips = len(shifts)
    h_ref, w_ref, out_ref, w_buf, o_buf, sems = refs[chips:]
    copies = half_oproj_copies(shifts, group, 0, info_ref, w_ref, refs[:chips], w_buf, o_buf, sems)
    for c in copies:
        c.start()
    for c in copies:
        c.wait()
    out_ref[...] = h_ref[...].astype(F32) + dot32(o_buf[...], w_buf[...])


def oproj(info, outs, shifts, group, h_zero, w_o):
    tok, hid = h_zero.shape
    wide = outs[0].shape[1]
    chips = len(shifts)
    vm = pl.BlockSpec(memory_space=pltpu.VMEM)
    anyspec = pl.BlockSpec(memory_space=pl.ANY)
    return pl.pallas_call(
        functools.partial(oproj_kernel, shifts, group),
        in_specs=[pl.BlockSpec(memory_space=pltpu.SMEM)] + [anyspec] * chips + [vm, anyspec],
        out_specs=vm,
        out_shape=jax.ShapeDtypeStruct((tok, hid), F32),
        scratch_shapes=[
            pltpu.VMEM((chips * wide, hid), BF16),
            pltpu.VMEM((tok, chips * wide), BF16),
            pltpu.SemaphoreType.DMA((2 * chips,)),
        ],
        compiler_params=params(),
        cost_estimate=cost(2 * tok * hid * chips * wide, 2 * chips * wide * hid),
        name="oproj",
    )(info, *outs, h_zero, w_o)


def tail_kernel(shifts, tile, group, head0, info_ref, *refs):
    chips = len(shifts)
    h_ref, g_ref, wo_ref, wg_ref, wu_ref, wd_ref, out_ref = refs[chips:chips + 7]
    wo_buf, o_buf, wg_buf, wu_buf, wd_buf, act_buf, b_buf, acc_ref, o_sems, g_sems, u_sems, d_sems = refs[chips + 7:]
    tok = acc_ref.shape[0]
    tiles = wg_ref.shape[1] // tile

    def span(i):
        return pl.ds(pl.multiple_of(i * tile, tile), tile)

    def gate_copy(i, s):
        return pltpu.make_async_copy(wg_ref.at[:, span(i)], wg_buf.at[s], g_sems.at[s])

    def up_copy(i, s):
        return pltpu.make_async_copy(wu_ref.at[:, span(i)], wu_buf.at[s], u_sems.at[s])

    def down_copy(i, s):
        return pltpu.make_async_copy(wd_ref.at[span(i), :], wd_buf.at[s], d_sems.at[s])

    copies = half_oproj_copies(shifts, group, head0, info_ref, wo_ref, refs[:chips], wo_buf, o_buf, o_sems)
    copies.append(pltpu.make_async_copy(h_ref, acc_ref, o_sems.at[2 * chips]))
    for c in copies:
        c.start()
    for s in range(2):
        gate_copy(s, s).start()
        up_copy(s, s).start()
    down_copy(0, 0).start()
    for c in copies:
        c.wait()
    acc_ref[...] += dot32(o_buf[...], wo_buf[...])
    chunk = 32
    for r in range(0, tok, chunk):
        h1 = acc_ref[r:r + chunk, :].astype(BF16).astype(F32)
        acc_ref[r:r + chunk, :] = h1
        scale = lax.rsqrt(jnp.mean(h1 * h1, axis=-1, keepdims=True) + NORM_EPS)
        b_buf[r:r + chunk, :] = (h1 * scale * g_ref[...].astype(F32)).astype(BF16)

    def front(s):
        b = b_buf[...]
        return (jax.nn.silu(dot32(b, wg_buf[s])) * dot32(b, wu_buf[s])).astype(BF16)

    gate_copy(0, 0).wait()
    up_copy(0, 0).wait()
    act_buf[...] = front(0)
    down_copy(1, 1).start()

    def body(i, carry):
        s = lax.rem(i, 2)
        p = 1 - s

        @pl.when(i + 1 < tiles)
        def _():
            gate_copy(i + 1, p).start()
            up_copy(i + 1, p).start()

        gate_copy(i, s).wait()
        up_copy(i, s).wait()
        down_copy(i - 1, p).wait()
        before = act_buf[...]
        act_buf[...] = front(s)
        acc_ref[...] += dot32(before, wd_buf[p])

        @pl.when(i + 1 < tiles)
        def _():
            down_copy(i + 1, p).start()

        return carry

    def first_body():
        gate_copy(1, 1).wait()
        up_copy(1, 1).wait()
        down_copy(0, 0).wait()
        gate_copy(2, 0).start()
        up_copy(2, 0).start()
        before = act_buf[...]
        act_buf[...] = front(1)
        acc_ref[...] += dot32(before, wd_buf[0])
        down_copy(2, 0).start()

    first_body()
    lax.fori_loop(2, tiles, body, 0)
    last = (tiles - 1) % 2
    down_copy(tiles - 1, last).wait()
    out_ref[...] = (acc_ref[...] + dot32(act_buf[...], wd_buf[last])).astype(BF16)


def tail(info, outs, shifts, group, head0, partial, norm, w_o, w_gate, w_up, w_down):
    tok, hid = partial.shape
    ffn = w_gate.shape[1]
    tile = 768
    wide = outs[0].shape[1]
    chips = len(shifts)
    vm = pl.BlockSpec(memory_space=pltpu.VMEM)
    anyspec = pl.BlockSpec(memory_space=pl.ANY)
    return pl.pallas_call(
        functools.partial(tail_kernel, shifts, tile, group, head0),
        in_specs=[pl.BlockSpec(memory_space=pltpu.SMEM)] + [anyspec] * (chips + 1) + [vm] + [anyspec] * 4,
        out_specs=vm,
        out_shape=jax.ShapeDtypeStruct((tok, hid), BF16),
        scratch_shapes=[
            pltpu.VMEM((chips * wide, hid), BF16),
            pltpu.VMEM((tok, chips * wide), BF16),
            pltpu.VMEM((2, hid, tile), BF16),
            pltpu.VMEM((2, hid, tile), BF16),
            pltpu.VMEM((2, tile, hid), BF16),
            pltpu.VMEM((tok, tile), BF16),
            pltpu.VMEM((tok, hid), BF16),
            pltpu.VMEM((tok, hid), F32),
            pltpu.SemaphoreType.DMA((2 * chips + 1,)),
            pltpu.SemaphoreType.DMA((2,)),
            pltpu.SemaphoreType.DMA((2,)),
            pltpu.SemaphoreType.DMA((2,)),
        ],
        compiler_params=params(67043328),
        cost_estimate=cost(2 * tok * hid * (chips * wide + 3 * ffn), 2 * hid * (chips * wide + 3 * ffn)),
        name="tail",
    )(info, *outs, partial, norm[None], w_o, w_gate, w_up, w_down)


def rope_tables(rope_pos):
    half = HEAD_DIM // 2
    inv_freq = ROPE_THETA ** (-jnp.arange(0, HEAD_DIM, 2, dtype=F32) / HEAD_DIM)
    idx = jnp.arange(half)
    lo, hi = MROPE_SPLIT
    chosen = jnp.where(idx < lo, rope_pos[:, 0, :, None], jnp.where(idx < hi, rope_pos[:, 1, :, None], rope_pos[:, 2, :, None]))
    angles = chosen.astype(F32) * inv_freq
    cos_h, sin_h = jnp.cos(angles), jnp.sin(angles)
    return jnp.concatenate([cos_h, cos_h], axis=-1), jnp.concatenate([-sin_h, sin_h], axis=-1)


def solution(mesh):
    group = mesh.shape['sp']
    chips = group // CORES
    row_spec = P(('dp', 'sp'), None)
    sibling = [(i, CORES * (i // CORES) + (i + 1) % CORES) for i in range(group)]

    def hop(x, steps):
        return lax.ppermute(x, 'sp', [(i, (i + CORES * steps) % group) for i in range(group)])

    def swap(x):
        return lax.ppermute(x, 'sp', sibling)

    def step(patches, embeds, dest_slot, rope_pos, cu_doc, ln_w, ln_b, w_one, b_one, w_two, b_two, norm_attn, w_q, b_q, w_k, b_k, w_v, b_v, w_o, norm_mlp, w_gate, w_up, w_down):
        tok, _ = embeds.shape
        merged_dev = dest_slot.shape[0]
        num_docs = cu_doc.shape[0] - 1
        me = lax.axis_index('sp')
        chip, core = me // CORES, me % CORES
        width = w_q.shape[1] // chips
        half_t = tok // 2
        info = jnp.stack([chip, core]).astype(jnp.int32)

        cut = 7 * tok // 8
        e_a, e_b = embeds[:cut], embeds[cut:]
        a_prev = hop(e_a, 1)
        a_next = hop(e_a, -1)
        ints = jnp.concatenate([rope_pos, jnp.pad(dest_slot, (0, tok - merged_dev))[None]], axis=0)
        around = [ints, hop(ints, -1), hop(ints, 1), hop(ints, chips // 2)]
        m_lo, m_hi = merger(patches, ln_w, ln_b, w_one, b_one, w_two, b_two)
        prev_lo, next_hi = hop(m_lo, 1), hop(m_hi, -1)
        prev_hi, next_lo = hop(m_hi, 1), hop(m_lo, -1)
        far_lo, far_hi = hop(prev_lo, 1), hop(next_hi, -1)
        mine = [m_lo, m_hi, next_lo, next_hi, prev_lo, prev_hi, far_lo, far_hi]
        theirs = [swap(m) for m in mine[:2]]
        theirs += [swap(m) for m in mine[2:-2]]
        theirs += [swap(m) for m in mine[-2:]]
        b_prev = hop(e_b, 1)
        b_next = hop(e_b, -1)
        far = [hop(a_prev[:half_t], 1), hop(a_next[half_t:], -1), hop(b_next, -1)]

        around = jnp.stack(around)
        slots_own = around[:, 3, :merged_dev]
        slots_sib = swap(slots_own)
        cos_t, sin_t = rope_tables(around[:, :3])
        slots = jnp.concatenate([slots_own, slots_sib], axis=0)
        shard_chip = (chip + jnp.array([0, 1, chips - 1, chips // 2], jnp.int32)) % chips
        base = tok * (CORES * shard_chip + core)
        starts = (base[:, None] + jnp.arange(0, tok, 256, dtype=jnp.int32)[None, :]).reshape(-1, 1, 1)
        counts = jnp.sum((slots[None] >= starts) & (slots[None] < starts + 256), axis=-1, dtype=jnp.int32)
        qkv_info = jnp.concatenate([info, counts.reshape(-1)])
        common = (cos_t, sin_t, norm_attn, w_q, b_q, w_k, b_k, w_v, b_v, width, tok)
        q_n, k_n, v_n, h_zero, far_rows, far_mask = qkv(qkv_info, [[embeds], [a_next, b_next], [a_prev, b_prev]], [slots] + mine + theirs, *common, True)
        k_sib_n, v_sib_n = swap(k_n), swap(v_n)
        q_f, k_f, v_f = qkv(info, [far], [far_rows, far_mask], *common, False)
        k_sibs = [k_sib_n, swap(k_f)]
        v_sibs = [v_sib_n, swap(v_f)]

        att_info = jnp.concatenate([info, cu_doc]).astype(jnp.int32)
        heads = width // HEAD_DIM
        split = (heads + 1) // 2
        shifts = (0, 1, -1, chips // 2)
        parts = []
        for head0, n in ((0, split), (split, heads - split)):
            o = attention(att_info, (q_n, q_f), (k_n, k_f), k_sibs, (v_n, v_f), v_sibs, num_docs, chips, tok, head0, n)
            parts.append([o[0]] + [hop(o[i], shifts[i]) for i in range(1, chips)])
        partial = oproj(info, parts[0], shifts, width, h_zero, w_o)
        return tail(info, parts[1], shifts, width, split, partial, norm_mlp, w_o, w_gate, w_up, w_down)

    in_specs = (row_spec, row_spec, P(('dp', 'sp')), P(None, ('dp', 'sp')), P('dp')) + (P(),) * 18
    return jax.shard_map(step, mesh=mesh, in_specs=in_specs, out_specs=row_spec, check_vma=False)
```
